32 devices in a mesh: dom: 8 (over y, x, core), tp: 4 (over z).
Axes of the slice: x: 2, y: 2, z: 4, core: 2. Of those that a mesh axis runs over, the one named last changes fastest.
Arguments:
- activations: bfloat16 [4, 128, 4096], P(None, 'dom', 'tp'), may hold values from -6 to 6
- norm_gain: float32 [4096], replicated, may hold values from 0.5 to 1.5
- w_query: bfloat16 [4096, 4096], P(None, 'tp'), may hold values from -0.09375 to 0.09375
- w_key: bfloat16 [4096, 1024], P(None, 'tp'), may hold values from -0.09375 to 0.09375
- value_weight: bfloat16 [4096, 1024], P(None, 'tp'), may hold values from -0.5 to 0.5
- w_output: bfloat16 [4096, 4096], P('tp'), may hold values from -0.09375 to 0.09375
- cache_keys: bfloat16 [128, 128, 1024], P('dom', None, 'tp'), may hold values from -740 to 740
- cache_values: bfloat16 [128, 128, 1024], P('dom', None, 'tp'), may hold values from -48 to 48
- tokens: int32 [4, 128], P(None, 'dom'), may hold values from 0 to 128255
- twisting_table: bfloat16 [128256], replicated, may hold values from -6 to 6
- twist_vec: float32 [4096], P('tp'), may hold values from -0.09375 to 0.09375
- previous_log_weights: float32 [128], P('dom'), may hold values from -300 to 0
- copy_counts: int32 [128], P('dom'), may hold values from 0 to 4, as said below
Outputs:
- attn_out: bfloat16 [4, 128, 4096], P(None, 'dom', 'tp')
- new_keys: bfloat16 [128, 132, 1024], P('dom', None, 'tp')
- new_values: bfloat16 [128, 132, 1024], P('dom', None, 'tp')
- out_logw: float32 [128], P('dom')
The draws below stay inside these ranges and needn't reach their ends.
Inputs may be any that keep to these rules, and one draw needn't show every extreme that they name: copy_counts sum to 128; the particles of one index of dom have together at most 64 copies, and one index has exactly that many.
All inputs are finite; a program needn't handle non-finite values.
Results may differ from the reference program's by a relative error of at most 0.012.
The reference program's roundings to bfloat16 on the way (of `normed`, `queries`, `fresh_keys`, `fresh_values`, `key_rows`, `weights` and `context`) count: a program that leaves them out, or rounds other values in their place, can miss the bound.
Values may be sent and summed in bfloat16 or wider, within the bound.
A program may use at most 128 MiB of HBM per device.

```python
import math
import jax
import jax.numpy as jnp
import numpy as np
from jax import lax

D = 4096
QH = 32
KVH = 8
HD = 128
VOCAB = 128256
STEPS = 4
PART_DEV = 16
L = 128
PARTICLES = 128
N_DOM = 8


def draw_cache_keys(key, part):
    base_key = jax.random.fold_in(jax.random.fold_in(key, 11), 0)
    width = KVH * HD
    result = jnp.clip(jax.random.normal(base_key, (PARTICLES, L, width), jnp.float32), -4.5, 4.5)
    return result.astype(jnp.bfloat16)


def draw_previous_log_weights(key, part):
    result = jax.random.uniform(jax.random.fold_in(key, 23), (PARTICLES,), jnp.float32, -8.0, 0.0)
    return result


def draw_copy_counts(key, part):
    first_key, second_key = jax.random.split(jax.random.fold_in(key, 37), 2)
    devices = PARTICLES // PART_DEV
    slots_all = 4 * PARTICLES
    heavy_device = jax.random.randint(first_key, (), 0, devices)
    shuffle = jax.random.permutation(second_key, slots_all)
    owner_device = jnp.arange(slots_all, dtype=jnp.int32) // (4 * PART_DEV)
    lighter = (owner_device[shuffle] != heavy_device).astype(jnp.int32)
    running = jnp.cumsum(lighter)
    needed = (devices - 4) * PART_DEV
    picked_order = ((lighter == 1) & (running <= needed)).astype(jnp.int32)
    picked = jnp.zeros((slots_all,), jnp.int32).at[shuffle].set(picked_order)
    picked = jnp.maximum(picked, (owner_device == heavy_device).astype(jnp.int32))
    return jnp.sum(picked.reshape(PARTICLES, 4), 1).astype(jnp.int32)


def set_ends(values, stream_key, smallest, top_value):
    dims = values.shape
    place = [jax.random.randint(jax.random.fold_in(stream_key, axis), (), 0, dims[axis]) for axis in range(len(dims))]
    values = values.at[tuple(place)].set(smallest)
    longest = dims.index(max(dims))
    place[longest] = (place[longest] + 1) % dims[longest]
    return values.at[tuple(place)].set(top_value)


def block_levels(key, extent, cuts, smallest, top_value):
    gain = 1.0
    for dim, shards_of in cuts:
        heights = jax.random.uniform(jax.random.fold_in(jax.random.fold_in(key, 6), dim), (shards_of,), jnp.float32, smallest / len(cuts), top_value / len(cuts))
        gain = gain * jnp.repeat(jnp.exp(heights), extent[dim] // shards_of).reshape((-1,) + (1,) * (len(extent) - 1 - dim))
    return gain


def wide_ids(own_key, shape, number_of, lean):
    loads = [min(1 << octave, number_of + 1 - (1 << octave)) * (1 << 20) // math.isqrt((1 << octave) ** lean) + 1 for octave in range((number_of + 1).bit_length()) if 1 << octave <= number_of]
    scale = 1 + sum(loads) // (1 << 30)
    listing = np.cumsum(np.array([max(1, weight // scale) for weight in loads]))
    lot = jax.random.randint(jax.random.fold_in(own_key, 1), shape, 0, int(listing[len(loads) - 1]))
    start = jnp.left_shift(1, jnp.searchsorted(jnp.asarray(listing, jnp.int32), lot, side="right").astype(jnp.int32))
    rank = start - 1 + jax.random.randint(jax.random.fold_in(own_key, 4), shape, 0, 1 << 30) % jnp.minimum(start, number_of + 1 - start)
    return jax.random.permutation(jax.random.fold_in(own_key, 2), number_of)[rank].astype(jnp.int32)


def normal_values(key, shape, scale, reach, cuts=(), kind=jnp.bfloat16):
    values = jax.random.normal(key, shape, jnp.float32) * scale
    if len(cuts) > 0:
        values = block_levels(key, shape, cuts, -0.22, 0.18) * values
    return jnp.clip(values, min=-reach, max=reach).astype(kind)


def setup_inputs(seed: int = 0) -> dict:
    keys = jax.random.split(jax.random.key(seed), 14)
    return {
        "activations": normal_values(keys[0], (STEPS, PARTICLES, D), 1.0, 6.0, ((1, 8), (2, 4))),
        "norm_gain": jnp.clip(1.0 + 0.1 * jax.random.normal(keys[1], (D,), jnp.float32), 0.5, 1.5),
        "w_query": normal_values(keys[2], (D, QH * HD), D ** -0.5, 0.09375, ((1, 4),)),
        "w_key": normal_values(keys[3], (D, KVH * HD), D ** -0.5, 0.09375, ((1, 4),)),
        "value_weight": normal_values(keys[4], (D, KVH * HD), (D // 32) ** -0.5, 0.5, ((1, 4),)),
        "w_output": normal_values(keys[5], (QH * HD, D), (QH * HD) ** -0.5, 0.09375, ((0, 4),)),
        "cache_keys": draw_cache_keys(jax.random.fold_in(keys[13], 71), 0),
        "cache_values": normal_values(keys[7], (PARTICLES, L, KVH * HD), 8.0, 48.0, ((0, 8), (2, 4))),
        "tokens": set_ends(wide_ids(keys[8], (STEPS, PARTICLES), VOCAB, 2), jax.random.fold_in(keys[8], 3), 0, VOCAB - 1).astype(jnp.int32),
        "twisting_table": normal_values(keys[9], (VOCAB,), 1.0, 6.0),
        "twist_vec": normal_values(keys[10], (D,), D ** -0.5, 0.09375, ((0, 4),), jnp.float32),
        "previous_log_weights": draw_previous_log_weights(jax.random.fold_in(keys[13], 71), 0),
        "copy_counts": draw_copy_counts(jax.random.fold_in(keys[13], 71), 0),
    }


def rotate(tensor, positions):
    middle = tensor.shape[-1] // 2
    frequency = 500000.0 ** (-2.0 * jnp.arange(middle, dtype=jnp.float32) / tensor.shape[-1])
    angles = positions[:, None] * frequency[None, :]
    cosine = jnp.cos(angles)[:, None, None, :]
    sine_part = jnp.sin(angles)[:, None, None, :]
    lower_half = tensor[..., :middle]
    upper_half = tensor[..., middle:]
    return jnp.concatenate([lower_half * cosine - upper_half * sine_part, upper_half * cosine + lower_half * sine_part], -1)

def reference(activations, norm_gain, w_query, w_key, value_weight, w_output, cache_keys, cache_values, tokens, twisting_table, twist_vec, previous_log_weights, copy_counts):
    inputs = activations.astype(jnp.float32)
    normed = (inputs * lax.rsqrt(lax.optimization_barrier(jnp.mean(inputs * inputs, -1, keepdims=True)) + 1e-05) * norm_gain).astype(jnp.bfloat16)
    flat_rows = normed.reshape(STEPS * PARTICLES, D)
    positions = (L + jnp.arange(STEPS, dtype=jnp.int32)).astype(jnp.float32)
    queries = jnp.dot(flat_rows, w_query, preferred_element_type=jnp.float32).reshape(STEPS, PARTICLES, QH, HD)
    queries = rotate(queries, positions).astype(jnp.bfloat16)
    fresh_keys = jnp.dot(flat_rows, w_key, preferred_element_type=jnp.float32).reshape(STEPS, PARTICLES, KVH, HD)
    fresh_keys = rotate(fresh_keys, positions).astype(jnp.bfloat16).reshape(STEPS, PARTICLES, KVH * HD)
    fresh_values = jnp.dot(flat_rows, value_weight, preferred_element_type=jnp.float32).astype(jnp.bfloat16).reshape(STEPS, PARTICLES, KVH * HD)
    key_rows = jnp.concatenate([cache_keys, jnp.transpose(fresh_keys, (1, 0, 2))], 1)
    value_rows = jnp.concatenate([cache_values, jnp.transpose(fresh_values, (1, 0, 2))], 1)
    key_span = L + STEPS
    group_size = QH // KVH
    query_heads = queries.reshape(STEPS, PARTICLES, KVH, group_size, HD).astype(jnp.float32)
    key_heads = key_rows.reshape(PARTICLES, key_span, KVH, HD).astype(jnp.float32)
    value_heads = value_rows.reshape(PARTICLES, key_span, KVH, HD).astype(jnp.float32)
    scores = jnp.einsum('snkgd,nlkd->snkgl', query_heads, key_heads) / HD ** 0.5
    allowed = jnp.arange(key_span, dtype=jnp.int32)[None, :] <= (L + jnp.arange(STEPS, dtype=jnp.int32))[:, None]
    allowed = allowed[:, None, None, None, :]
    masked = jnp.where(allowed, scores, -jnp.inf)
    highest = lax.optimization_barrier(jnp.max(masked, -1, keepdims=True))
    exponent = jnp.exp(masked - highest)
    weights = (exponent / lax.optimization_barrier(jnp.sum(exponent, -1, keepdims=True))).astype(jnp.bfloat16)
    context = jnp.einsum('snkgl,nlkd->snkgd', weights.astype(jnp.float32), value_heads).astype(jnp.bfloat16)
    context = context.reshape(STEPS * PARTICLES, QH * HD)
    head_mix = jnp.dot(context, w_output, preferred_element_type=jnp.float32).reshape(STEPS, PARTICLES, D)
    attn_out = head_mix.astype(jnp.bfloat16)
    summed = inputs + head_mix
    twisting_score = lax.optimization_barrier(jnp.sum(summed * twist_vec, -1)) / jnp.sqrt(lax.optimization_barrier(jnp.mean(summed * summed, -1)) + 1e-06)
    token_reward = twisting_table[tokens].astype(jnp.float32)
    particle_log_weight = previous_log_weights + lax.optimization_barrier(jnp.sum(token_reward + twisting_score, 0))
    largest = jnp.max(particle_log_weight)
    out_logw = particle_log_weight - (largest + jnp.log(jnp.sum(jnp.exp(particle_log_weight - largest))))
    copy_ends = jnp.cumsum(copy_counts).astype(jnp.int32)
    new_slot = jnp.arange(PARTICLES, dtype=jnp.int32)
    owner_index = new_slot // PART_DEV
    local_slot = new_slot % PART_DEV
    copy_rank = local_slot * N_DOM + owner_index
    ancestor = lax.optimization_barrier(jnp.sum((copy_ends[None, :] <= copy_rank[:, None]).astype(jnp.int32), 1)).astype(jnp.int32)
    new_keys = key_rows[ancestor]
    new_values = value_rows[ancestor]
    return (attn_out, new_keys, new_values, out_logw)
```

```python
import functools

import jax
import jax.numpy as jnp
import numpy as np
from jax import lax
from jax.experimental import pallas as pl
from jax.experimental.pallas import tpu as pltpu
from jax.sharding import PartitionSpec as P

D = 4096
HD = 128
CAP = 8


def rotate(tensor, positions):
    middle = tensor.shape[-1] // 2
    frequency = 500000.0 ** (-2.0 * jnp.arange(middle, dtype=jnp.float32) / tensor.shape[-1])
    angles = positions[:, None] * frequency[None, :]
    cosine = jnp.cos(angles)[:, None, None, :]
    sine_part = jnp.sin(angles)[:, None, None, :]
    lower_half = tensor[..., :middle]
    upper_half = tensor[..., middle:]
    return jnp.concatenate(
        [
            lower_half * cosine - upper_half * sine_part,
            upper_half * cosine + lower_half * sine_part,
        ],
        -1,
    )


def local(
    activations,
    norm_gain,
    w_query,
    w_key,
    value_weight,
    w_output,
    cache_keys,
    cache_values,
    tokens,
    twisting_table,
    twist_vec,
    previous_log_weights,
    copy_counts,
):
    step_count = activations.shape[0]
    particle_count = activations.shape[1]
    span_old = cache_keys.shape[1]
    dom_size = lax.axis_size("dom")
    kv_local = w_key.shape[1] // HD
    q_local = w_query.shape[1] // HD
    group_size = q_local // kv_local
    all_counts = lax.all_gather(copy_counts, "dom", axis=0, tiled=True)
    copy_ends = jnp.cumsum(all_counts)
    ranks = jnp.arange(particle_count, dtype=jnp.int32) * dom_size + lax.axis_index("dom")
    ancestor = jnp.sum((copy_ends[None, :] <= ranks[:, None]).astype(jnp.int32), 1)
    all_keys = lax.all_gather(cache_keys, "dom", axis=0, tiled=True)
    all_values = lax.all_gather(cache_values, "dom", axis=0, tiled=True)

    gathered = lax.all_gather(activations, "tp", axis=2, tiled=True)
    inputs = gathered.astype(jnp.float32)
    normed = (
        inputs * lax.rsqrt(jnp.mean(inputs * inputs, -1, keepdims=True) + 1e-05) * norm_gain
    ).astype(jnp.bfloat16)
    flat_rows = normed.reshape(step_count * particle_count, D)
    positions = (span_old + jnp.arange(step_count, dtype=jnp.int32)).astype(jnp.float32)
    queries = jnp.dot(flat_rows, w_query, preferred_element_type=jnp.float32).reshape(
        step_count, particle_count, q_local, HD
    )
    queries = rotate(queries, positions).astype(jnp.bfloat16)
    fresh_keys = jnp.dot(flat_rows, w_key, preferred_element_type=jnp.float32).reshape(
        step_count, particle_count, kv_local, HD
    )
    fresh_keys = (
        rotate(fresh_keys, positions)
        .astype(jnp.bfloat16)
        .reshape(step_count, particle_count, kv_local * HD)
    )
    fresh_values = jnp.dot(flat_rows, value_weight, preferred_element_type=jnp.float32).astype(
        jnp.bfloat16
    )
    fresh_values = fresh_values.reshape(step_count, particle_count, kv_local * HD)
    fresh_keys = jnp.transpose(fresh_keys, (1, 0, 2))
    fresh_values = jnp.transpose(fresh_values, (1, 0, 2))
    key_rows = jnp.concatenate([cache_keys, fresh_keys], 1)
    value_rows = jnp.concatenate([cache_values, fresh_values], 1)
    key_span = span_old + step_count
    query_heads = queries.reshape(step_count, particle_count, kv_local, group_size, HD)
    key_heads = key_rows.reshape(particle_count, key_span, kv_local, HD)
    value_heads = value_rows.reshape(particle_count, key_span, kv_local, HD)
    scores = (
        jnp.einsum("snkgd,nlkd->snkgl", query_heads, key_heads, preferred_element_type=jnp.float32)
        / HD**0.5
    )
    allowed = (
        jnp.arange(key_span, dtype=jnp.int32)[None, :]
        <= (span_old + jnp.arange(step_count, dtype=jnp.int32))[:, None]
    )
    allowed = allowed[:, None, None, None, :]
    masked = jnp.where(allowed, scores, -jnp.inf)
    highest = jnp.max(masked, -1, keepdims=True)
    exponent = jnp.exp(masked - highest)
    weights = (exponent / jnp.sum(exponent, -1, keepdims=True)).astype(jnp.bfloat16)
    context = jnp.einsum(
        "snkgl,nlkd->snkgd", weights, value_heads, preferred_element_type=jnp.float32
    ).astype(jnp.bfloat16)
    context = context.reshape(step_count * particle_count, q_local * HD)
    partial_value = jnp.dot(context, w_output, preferred_element_type=jnp.float32).reshape(
        step_count, particle_count, D
    )
    head_mix = lax.psum_scatter(partial_value, "tp", scatter_dimension=2, tiled=True)
    attn_out = head_mix.astype(jnp.bfloat16)
    summed = activations.astype(jnp.float32) + head_mix
    aligned, energy = lax.psum(
        (jnp.sum(summed * twist_vec, -1), jnp.sum(summed * summed, -1)), "tp"
    )
    twisting_score = aligned / jnp.sqrt(energy / D + 1e-06)
    token_reward = twisting_table[tokens].astype(jnp.float32)
    particle_log_weight = previous_log_weights + jnp.sum(token_reward + twisting_score, 0)
    largest = lax.pmax(jnp.max(particle_log_weight), "dom")
    mass_total = lax.psum(jnp.sum(jnp.exp(particle_log_weight - largest)), "dom")
    out_logw = particle_log_weight - (largest + jnp.log(mass_total))
    fresh = lax.all_gather(
        jnp.concatenate([fresh_keys, fresh_values], 2), "dom", axis=0, tiled=True
    )[ancestor]
    width = fresh_keys.shape[2]
    new_keys = jnp.concatenate([all_keys[ancestor], fresh[..., :width]], 1)
    new_values = jnp.concatenate([all_values[ancestor], fresh[..., width:]], 1)
    return (attn_out, new_keys, new_values, out_logw)


MESH = pl.DeviceIdType.MESH


def layer_kernel(
    steps, parts, doms, tps,
    act, gain, wq, wk, wv, wo, ck, cv, twist, aux, cosine, sine,
    attn_out, all_k, all_v, fresh_sel, out_lw, anc_out,
    act_all, wq_v, wk_v, wv_v, wo_v, ck_v, cv_v, qs, cx, sc1, ctx_b, fresh, fresh_all,
    rs_send, rs_recv, sc_all, lw_all, cnt_all,
    loc, tp_send, tp_recv, dom_send, dom_recv, blk_send, blk_recv,
):
    f32, bf16 = jnp.float32, jnp.bfloat16
    me_d = lax.axis_index("dom")
    me_t = lax.axis_index("tp")
    rows, width = act.shape
    half = parts // 2
    kvw = wk.shape[1]
    groups = kvw // HD
    per = wq.shape[1] // kvw
    pack = steps * per
    c = me_d % 2
    x = (me_d // 2) % 2
    y = me_d // 4
    sib = me_d + 1 - 2 * c
    xn = me_d + 2 - 4 * x
    yn = me_d + 4 - 8 * y
    dn = xn + 4 - 8 * y

    barrier = pltpu.get_barrier_semaphore()
    for k in range(1, tps):
        pl.semaphore_signal(
            barrier, inc=1, device_id=(me_d, (me_t + k) % tps), device_id_type=MESH
        )
    for k in range(1, doms):
        pl.semaphore_signal(
            barrier, inc=1, device_id=((me_d + k) % doms, me_t), device_id_type=MESH
        )

    def fetch(i, src, dst):
        copy = pltpu.make_async_copy(src, dst, loc.at[i])
        copy.start()
        return copy

    own_act = fetch(0, act, act_all.at[me_t])
    load_q = fetch(1, wq, wq_v)
    load_k = fetch(2, wk, wk_v)
    load_v = fetch(3, wv, wv_v)
    load_ck = fetch(4, ck, ck_v)
    load_cv = fetch(5, cv, cv_v)
    load_o = fetch(6, wo, wo_v)

    cnt_all[me_d] = jnp.broadcast_to(aux[:, 1:], cnt_all.shape[1:])
    pl.semaphore_wait(barrier, tps + doms - 2)

    def tp_push(base, k, src, dst):
        copy = pltpu.make_async_remote_copy(
            src_ref=src, dst_ref=dst, send_sem=tp_send.at[base + k - 1],
            recv_sem=tp_recv.at[base + k - 1],
            device_id=(me_d, (me_t + k) % tps), device_id_type=MESH,
        )
        copy.start()
        return copy

    def dom_push(base, k, src, dst):
        copy = pltpu.make_async_remote_copy(
            src_ref=src, dst_ref=dst, send_sem=dom_send.at[base + k - 1],
            recv_sem=dom_recv.at[base + k - 1],
            device_id=((me_d + k) % doms, me_t), device_id_type=MESH,
        )
        copy.start()
        return copy

    acts = [tp_push(0, k, act, act_all.at[me_t]) for k in range(1, tps)]

    def piece(kind, to, which, h, slot, own):
        dst = (all_k, all_v)[which].at[slot, pl.ds(h * half, half)]
        src = (ck, cv)[which].at[pl.ds(h * half, half)] if own else dst
        i = kind * 4 + h * 2 + which
        copy = pltpu.make_async_remote_copy(
            src_ref=src, dst_ref=dst, send_sem=blk_send.at[i], recv_sem=blk_recv.at[i],
            device_id=(to, me_t), device_id_type=MESH,
        )
        copy.start()
        return copy

    moves = {}
    for h, kind, to in ((0, 0, xn), (1, 1, yn), (1, 0, xn), (0, 1, yn)):
        for which in range(2):
            moves[kind, h, which] = piece(kind, to, which, h, me_d, True)
    cnts = [dom_push(0, k, cnt_all.at[me_d], cnt_all.at[me_d]) for k in range(1, doms)]
    for h in range(2):
        for which in range(2):
            moves[3, h, which] = piece(3, sib, which, h, me_d, True)

    own_act.wait()
    for copy in acts:
        copy.wait()
    square = jnp.zeros((rows, 1), f32)
    for t in range(tps):
        u = act_all[t].astype(f32)
        square = square + jnp.sum(u * u, -1, keepdims=True)
    inv = lax.rsqrt(square / (width * tps) + 1e-05)
    normed = []
    for t in range(tps):
        u = act_all[t].astype(f32)
        normed.append((u * inv * gain[:, t * width : (t + 1) * width]).astype(bf16))

    def project(w):
        total = None
        for t in range(tps):
            part = jnp.dot(
                normed[t], w[t * width : (t + 1) * width, :], preferred_element_type=f32
            )
            total = part if total is None else total + part
        return total

    cos_t, sin_t = cosine[...], sine[...]

    def turn(u):
        return u * cos_t + pltpu.roll(u, HD // 2, 1) * sin_t

    load_k.wait()
    load_v.wait()
    keys = project(wk_v)
    for g in range(groups):
        fresh[:, g * HD : (g + 1) * HD] = turn(keys[:, g * HD : (g + 1) * HD]).astype(bf16)
    fresh[:, kvw:] = project(wv_v).astype(bf16)
    fresh_all[me_d] = fresh[...]
    news = [dom_push(doms - 1, k, fresh, fresh_all.at[me_d]) for k in range(1, doms)]
    load_q.wait()
    query = project(wq_v)
    for h in range(groups * per):
        g, j = h // per, h % per
        turned = turn(query[:, h * HD : (h + 1) * HD])
        for s in range(steps):
            qs[g, :, s * per + j, :] = turned[s * parts : (s + 1) * parts]
    load_ck.wait()
    load_cv.wait()
    put_k = fetch(7, ck_v, all_k.at[me_d])
    put_v = fetch(8, cv_v, all_v.at[me_d])

    lines = parts * pack
    row = lax.broadcasted_iota(jnp.int32, (lines, rows), 0)
    col = lax.broadcasted_iota(jnp.int32, (lines, rows), 1)
    allowed = (row // pack == col % parts) & (col // parts <= (row % pack) // per)
    scale = HD**0.5
    for g in range(groups):
        lanes = slice(g * HD, (g + 1) * HD)
        qg = qs[g].reshape(lines, HD).astype(bf16)
        for n in range(parts):
            sc1[g, n * pack : (n + 1) * pack, :] = lax.dot_general(
                qg[n * pack : (n + 1) * pack], ck_v[n, :, lanes],
                (((1,), (1,)), ((), ())), preferred_element_type=f32,
            )
        near = lax.dot_general(
            qg, fresh[:, lanes], (((1,), (1,)), ((), ())), preferred_element_type=f32
        )
        near = jnp.where(allowed, near / scale, -jnp.inf)
        far = sc1[g] / scale
        top = jnp.maximum(
            jnp.max(far, -1, keepdims=True), jnp.max(near, -1, keepdims=True)
        )
        far = jnp.exp(far - top)
        near = jnp.exp(near - top)
        mass = jnp.sum(far, -1, keepdims=True) + jnp.sum(near, -1, keepdims=True)
        far = (far / mass).astype(bf16)
        near = (near / mass).astype(bf16)
        extra = jnp.dot(
            near, fresh[:, kvw + g * HD : kvw + (g + 1) * HD], preferred_element_type=f32
        )
        for n in range(parts):
            span = slice(n * pack, (n + 1) * pack)
            cx[g, n] = extra[span] + jnp.dot(
                far[span], cv_v[n, :, lanes], preferred_element_type=f32
            )
    for h in range(groups * per):
        g, j = h // per, h % per
        for s in range(steps):
            ctx_b[s * parts : (s + 1) * parts, h * HD : (h + 1) * HD] = cx[
                g, :, s * per + j, :
            ].astype(bf16)
    load_o.wait()

    def mix(p):
        return jnp.dot(
            ctx_b[...], wo_v[:, pl.ds(pl.multiple_of(p * width, HD), width)],
            preferred_element_type=f32,
        )

    sums = []
    for k in range(1, tps):
        rs_send[k - 1] = mix((me_t + k) % tps)
        sums.append(tp_push(tps - 1, k, rs_send.at[k - 1], rs_recv.at[k - 1]))
    head = mix(me_t)

    def done(kind, h):
        for which in range(2):
            moves[kind, h, which].wait_recv()

    def relay(kind, to, h, slot):
        for which in range(2):
            moves[kind, h, which] = piece(kind, to, which, h, slot, False)

    done(0, 0)
    relay(2, yn, 0, xn)
    relay(4, sib, 0, xn)
    done(1, 1)
    relay(6, xn, 1, yn)
    relay(5, sib, 1, yn)
    for k in range(1, tps):
        sums[k - 1].wait()
        head = head + rs_recv[k - 1]
    attn_out[...] = head.astype(bf16)
    summed = act_all[me_t].astype(f32) + head
    along = jnp.sum(summed * twist[...], -1, keepdims=True)
    energy = jnp.sum(summed * summed, -1, keepdims=True)
    lane = lax.broadcasted_iota(jnp.int32, (rows, HD), 1)
    sc_all[me_t] = jnp.where(lane < HD // 2, along, energy)
    scores = [
        tp_push(2 * (tps - 1), k, sc_all.at[me_t], sc_all.at[me_t]) for k in range(1, tps)
    ]
    for copy in scores:
        copy.wait()
    both = sc_all[0]
    for t in range(1, tps):
        both = both + sc_all[t]
    score = both[:, :1] / jnp.sqrt(both[:, HD - 1 :] / (width * tps) + 1e-06)
    total = score[:parts]
    for s in range(1, steps):
        total = total + score[s * parts : (s + 1) * parts]
    mine = jnp.broadcast_to(aux[:, :1] + total, (parts, HD))
    lw_all[me_d] = mine
    lws = [
        dom_push(2 * (doms - 1), k, lw_all.at[me_d], lw_all.at[me_d]) for k in range(1, doms)
    ]

    done(0, 1)
    relay(4, sib, 1, xn)
    done(1, 0)
    relay(5, sib, 0, yn)

    for copy in cnts:
        copy.wait()
    for copy in news:
        copy.wait()
    whole = parts * doms
    number = cnt_all[...].reshape(whole, HD).astype(bf16)
    lower = lax.broadcasted_iota(jnp.int32, (whole, whole), 0)
    upper = lax.broadcasted_iota(jnp.int32, (whole, whole), 1)
    ends = jnp.dot(
        (upper <= lower).astype(f32).astype(bf16), number, preferred_element_type=f32
    )
    slot = lax.broadcasted_iota(jnp.int32, (whole, HD), 1)

    def ancestor(place):
        rank = (place * doms + me_d).astype(f32)
        return jnp.sum((ends <= rank).astype(f32), 0, keepdims=True).astype(jnp.int32)

    anc_out[...] = jnp.broadcast_to(ancestor(slot), anc_out.shape)
    lanes = lax.broadcasted_iota(jnp.int32, (1, HD), 1)
    wide = ancestor(slot // 8)
    target = (wide // parts) * rows + (lanes % 8) * parts + wide % parts
    target = jnp.where(lanes % 8 < steps, target, -1)
    index = lax.broadcasted_iota(jnp.int32, (doms * rows, HD), 0)
    pick = (index == target).astype(f32).astype(bf16)
    fresh_sel[...] = lax.dot_general(
        pick, fresh_all[...].reshape(doms * rows, 2 * kvw),
        (((0,), (0,)), ((), ())), preferred_element_type=f32,
    ).astype(bf16)

    for copy in lws:
        copy.wait()
    largest = jnp.max(lw_all[...], (0, 1), keepdims=True)[0]
    mass = jnp.sum(jnp.exp(lw_all[...] - largest[None]), (0, 1), keepdims=True)[0]
    out_lw[...] = mine - (largest + jnp.log(mass))

    done(2, 0)
    relay_d0 = [piece(7, sib, which, 0, dn, False) for which in range(2)]
    done(6, 1)
    relay_d1 = [piece(7, sib, which, 1, dn, False) for which in range(2)]
    for kind in (3, 4, 5):
        for h in range(2):
            done(kind, h)
    for copy in moves.values():
        copy.wait_send()
    for copy in relay_d0 + relay_d1:
        copy.wait()
    put_k.wait()
    put_v.wait()


def select_kernel(parts, steps, anc, fresh_sel, all_k, all_v, new_k, new_v, sem):
    span = all_k.shape[2]
    width = all_k.shape[3]
    copies = []
    for i in range(parts):
        a = anc[0, i]
        d, n = a // parts, a % parts
        for which, (src, dst) in enumerate(((all_k, new_k), (all_v, new_v))):
            copy = pltpu.make_async_copy(
                src.at[d, n], dst.at[i, pl.ds(0, span)], sem.at[2 * i + which]
            )
            copy.start()
            copies.append(copy)
    for i in range(parts):
        new_k[i, span:, :] = fresh_sel[i * 8 : i * 8 + steps, :width]
        new_v[i, span:, :] = fresh_sel[i * 8 : i * 8 + steps, width:]
    for copy in copies:
        copy.wait()


def all_rows(
    steps, parts, act, gain, wq, wk, wv, wo, ck, cv, twist, aux, cosine, sine,
):
    f32, bf16 = jnp.float32, jnp.bfloat16
    rows, width = act.shape
    span = ck.shape[1]
    kvw = wk.shape[1]
    qw = wq.shape[1]
    groups = kvw // HD
    pack = steps * (qw // kvw)
    doms = lax.axis_size("dom")
    tps = lax.axis_size("tp")
    vmem = pl.BlockSpec(memory_space=pltpu.VMEM)
    hbm = pl.BlockSpec(memory_space=pl.ANY)
    block = jax.ShapeDtypeStruct((doms,) + ck.shape, bf16)
    attn, all_k, all_v, fresh_sel, out_lw, anc = pl.pallas_call(
        functools.partial(layer_kernel, steps, parts, doms, tps),
        out_shape=(
            jax.ShapeDtypeStruct((rows, width), bf16), block, block,
            jax.ShapeDtypeStruct((HD, 2 * kvw), bf16),
            jax.ShapeDtypeStruct((parts, HD), f32),
            jax.ShapeDtypeStruct((8, HD), jnp.int32),
        ),
        in_specs=[hbm, vmem] + [hbm] * 6 + [vmem] * 4,
        out_specs=(vmem, hbm, hbm, vmem, vmem, vmem),
        scratch_shapes=[
            pltpu.VMEM((tps, rows, width), bf16),
            pltpu.VMEM(wq.shape, bf16),
            pltpu.VMEM(wk.shape, bf16),
            pltpu.VMEM(wv.shape, bf16),
            pltpu.VMEM(wo.shape, bf16),
            pltpu.VMEM(ck.shape, bf16),
            pltpu.VMEM(cv.shape, bf16),
            pltpu.VMEM((groups, parts, pack, HD), f32),
            pltpu.VMEM((groups, parts, pack, HD), f32),
            pltpu.VMEM((groups, parts * pack, span), f32),
            pltpu.VMEM((rows, qw), bf16),
            pltpu.VMEM((rows, 2 * kvw), bf16),
            pltpu.VMEM((doms, rows, 2 * kvw), bf16),
            pltpu.VMEM((tps - 1, rows, width), f32),
            pltpu.VMEM((tps - 1, rows, width), f32),
            pltpu.VMEM((tps, rows, HD), f32),
            pltpu.VMEM((doms, parts, HD), f32),
            pltpu.VMEM((doms, parts, HD), f32),
            pltpu.SemaphoreType.DMA((9,)),
            pltpu.SemaphoreType.DMA((3 * (tps - 1),)),
            pltpu.SemaphoreType.DMA((3 * (tps - 1),)),
            pltpu.SemaphoreType.DMA((3 * (doms - 1),)),
            pltpu.SemaphoreType.DMA((3 * (doms - 1),)),
            pltpu.SemaphoreType.DMA((32,)),
            pltpu.SemaphoreType.DMA((32,)),
        ],
        compiler_params=pltpu.CompilerParams(
            collective_id=4, has_side_effects=True, vmem_limit_bytes=56 << 20
        ),
        name="layer",
    )(act, gain, wq, wk, wv, wo, ck, cv, twist, aux, cosine, sine)
    result = jax.ShapeDtypeStruct((parts, span + steps, kvw), bf16)
    new_k, new_v = pl.pallas_call(
        functools.partial(select_kernel, parts, steps),
        out_shape=(result, result),
        in_specs=[pl.BlockSpec(memory_space=pltpu.SMEM), vmem, hbm, hbm],
        out_specs=(vmem, vmem),
        scratch_shapes=[pltpu.SemaphoreType.DMA((2 * parts,))],
        name="select",
    )(anc, fresh_sel, all_k, all_v)
    return attn, new_k, new_v, out_lw


def plan_kernel(parts, doms, cap, steps, rows, cnt, tab, cnt_all, send, recv):
    f32, bf16, i32 = jnp.float32, jnp.bfloat16, jnp.int32
    me_d = lax.axis_index("dom")
    me_t = lax.axis_index("tp")
    core = me_d % 2
    x = (me_d // 2) % 2
    y = me_d // 4
    chip = me_d // 2
    barrier = pltpu.get_barrier_semaphore()
    for k in range(1, doms):
        pl.semaphore_signal(
            barrier, inc=1, device_id=((me_d + k) % doms, me_t), device_id_type=MESH
        )
    cnt_all[me_d] = jnp.zeros(cnt_all.shape[1:], f32)
    cnt_all[me_d, :, :parts] = jnp.broadcast_to(cnt[...].astype(f32), (8, parts))
    pl.semaphore_wait(barrier, doms - 1)
    copies = []
    for k in range(1, doms):
        copy = pltpu.make_async_remote_copy(
            src_ref=cnt_all.at[me_d], dst_ref=cnt_all.at[me_d],
            send_sem=send.at[k - 1], recv_sem=recv.at[k - 1],
            device_id=((me_d + k) % doms, me_t), device_id_type=MESH,
        )
        copy.start()
        copies.append(copy)
    for copy in copies:
        copy.wait()
    whole = parts * doms
    j = lax.broadcasted_iota(i32, (whole, HD), 0)
    lane = lax.broadcasted_iota(i32, (whole, HD), 1)
    spread = jnp.concatenate([cnt_all[d] for d in range(doms) for _ in range(parts // 8)], 0)
    column = jnp.sum(jnp.where(lane == j % parts, spread, 0.0), -1, keepdims=True)
    number = jnp.broadcast_to(column, (whole, HD))
    first = lax.broadcasted_iota(i32, (whole, whole), 0)
    second = lax.broadcasted_iota(i32, (whole, whole), 1)

    def total(mask, values):
        return jnp.dot(
            mask.astype(f32).astype(bf16), values.astype(bf16), preferred_element_type=f32
        )

    ends = total(second <= first, number)
    loads = total(second // parts == first // parts, number)
    number = number.astype(i32)
    ends = ends.astype(i32)
    starts = ends - number
    top = jnp.max(loads, (0, 1), keepdims=True)
    owner = j // parts
    heavy = jnp.min(jnp.where(loads == top, owner, doms).astype(f32), (0, 1), keepdims=True)
    heavy = heavy.astype(i32)
    light = owner != heavy
    home = j // (2 * parts)

    def needs(to):
        hit = None
        for m in range(4):
            one = (m < number) & (((starts + m) % doms) // 2 == to)
            hit = one if hit is None else hit | one
        return hit & light & (home != to)

    kind = (lane // cap) % 4
    there_x = x + kind % 2 - 2 * x * (kind % 2)
    there_y = y + kind // 2 - 2 * y * (kind // 2)
    need_send = needs(2 * there_y + there_x)
    need_here = needs(jnp.broadcast_to(chip, (whole, HD)))
    need_any = needs(lane % 4)
    before = (second < first) & (second // (2 * parts) == first // (2 * parts))
    places = total(
        before,
        jnp.concatenate([u.astype(f32) for u in (need_send, need_here, need_any)], 1),
    ).astype(i32)
    place_send = places[:, :HD]
    place_here = places[:, HD : 2 * HD]
    place_any = places[:, 2 * HD :]
    local_row = j % parts + parts * (owner % 2 + core - 2 * core * (owner % 2))
    picked = need_send & (place_send == lane % cap) & (home == chip)
    sources = jnp.sum(jnp.where(picked, local_row, 0).astype(f32), 0, keepdims=True)
    hx, hy = home % 2, home // 2
    away = (hx + x - 2 * x * hx) + 2 * (hy + y - 2 * y * hy)
    value = jnp.where(
        away == 0,
        local_row,
        jnp.where(light, 3 * parts + (away - 1) * cap + place_here, 2 * parts + j % parts),
    )
    rank = lane * doms + me_d
    mine = (starts <= rank) & (rank < ends)
    index = jnp.sum(jnp.where(mine, value, 0).astype(f32), 0, keepdims=True)
    wide = (lane // 8) * doms + me_d
    old = jnp.sum((ends <= wide).astype(f32), 0, keepdims=True).astype(i32)
    row = lax.broadcasted_iota(i32, (1, HD), 1)
    target = (old // parts) * rows + (row % 8) * parts + old % parts
    target = jnp.where(row % 8 < steps, target, -1)
    longest = jnp.max(
        jnp.where(need_any, place_any + 1, 0).astype(f32), (0, 1), keepdims=True
    ).astype(i32)
    base = parts * (heavy % 2 + core - 2 * core * (heavy % 2))
    branch = jnp.where(longest <= cap, heavy // 2, 4)
    tab[0:1, :] = sources.astype(i32)
    tab[1:2, :] = index.astype(i32)
    tab[2:3, :] = jnp.broadcast_to(base, (1, HD))
    tab[3:4, :] = target
    tab[4:5, :] = jnp.broadcast_to(branch, (1, HD))
    tab[5:8, :] = jnp.zeros((3, HD), i32)


def main_kernel(
    steps, parts, doms, tps, cap, hot,
    act, gain, wq, wk, wv, wo, ck, cv, twist, aux, cosine, sine, tab, tabv,
    attn_out, new_k, new_v, out_lw,
    act_all, wq_v, wk_v, wv_v, wo_v, chip_k, chip_v, all_k, all_v, send_k, send_v,
    qs, cx, sc1, ctx_b, fresh_all, rs_send, rs_recv, sc_all, lw_all,
    loc, tp_send, tp_recv, lw_send, lw_recv, sib_send, sib_recv,
    hv_send, hv_recv, li_send, li_recv, fr_send, fr_recv,
):
    f32, bf16 = jnp.float32, jnp.bfloat16
    me_d = lax.axis_index("dom")
    me_t = lax.axis_index("tp")
    rows, width = act.shape
    kvw = wk.shape[1]
    groups = kvw // HD
    per = wq.shape[1] // kvw
    pack = steps * per
    span = ck.shape[1]
    c = me_d % 2
    x = (me_d // 2) % 2
    y = me_d // 4
    sib = me_d + 1 - 2 * c
    xn = me_d + 2 - 4 * x
    yn = me_d + 4 - 8 * y
    dn = xn + 4 - 8 * y
    rx = x if hot % 2 == 0 else 1 - x
    ry = y if hot // 2 == 0 else 1 - y
    pos = (1 - c) * (3 * ry + rx * (1 - 2 * ry)) + c * (3 * rx + ry * (1 - 2 * rx))
    turn_y = (pos + c) % 2
    onward = xn + turn_y * (yn - xn)

    barrier = pltpu.get_barrier_semaphore()
    for k in range(1, tps):
        pl.semaphore_signal(
            barrier, inc=1, device_id=(me_d, (me_t + k) % tps), device_id_type=MESH
        )
    for k in range(1, doms):
        pl.semaphore_signal(
            barrier, inc=1, device_id=((me_d + k) % doms, me_t), device_id_type=MESH
        )

    def fetch(i, src, dst):
        copy = pltpu.make_async_copy(src, dst, loc.at[i])
        copy.start()
        return copy

    own_act = fetch(0, act, act_all.at[me_t])
    load_ck = fetch(4, ck, chip_k.at[pl.ds(0, parts)])
    load_cv = fetch(5, cv, chip_v.at[pl.ds(0, parts)])
    load_k = fetch(2, wk, wk_v)
    load_v = fetch(3, wv, wv_v)
    load_q = fetch(1, wq, wq_v)
    load_o = fetch(6, wo, wo_v)
    pl.semaphore_wait(barrier, tps + doms - 2)

    def push(src, dst, ssem, rsem, to_d, to_t):
        return pltpu.make_async_remote_copy(
            src_ref=src, dst_ref=dst, send_sem=ssem, recv_sem=rsem,
            device_id=(to_d, to_t), device_id_type=MESH,
        )

    def tp_push(base, k, src, dst):
        copy = push(
            src, dst, tp_send.at[base + k - 1], tp_recv.at[base + k - 1],
            me_d, (me_t + k) % tps,
        )
        copy.start()
        return copy

    acts = [tp_push(0, k, act, act_all.at[me_t]) for k in range(1, tps)]
    swaps = []
    for i, (src, dst) in enumerate(((ck, chip_k), (cv, chip_v))):
        copy = push(src, dst.at[pl.ds(parts, parts)], sib_send.at[i], sib_recv.at[i], sib, me_t)
        copy.start()
        swaps.append(copy)

    lane_rows = cap // 2
    hot_rows = parts // 2
    chunk = hot_rows // 4

    def hot_copy(q, which, to, base):
        ref = (all_k, all_v)[which]
        area = ref.at[pl.ds(2 * parts + hot_rows * c + q * chunk, chunk)]
        i = base + q * 2 + which
        return push(area, area, hv_send.at[i], hv_recv.at[i], to, me_t)

    def forward(q, which):
        return hot_copy(q, which, onward, 0)

    def mirror(q, which):
        return hot_copy(q, which, sib, 8)

    def light_area(ref, k):
        return ref.at[pl.ds(3 * parts + (k - 1) * cap + lane_rows * c, lane_rows)]

    def light(k, which):
        i = (k - 1) * 2 + which
        return push(
            (send_k, send_v)[which].at[k - 1], light_area((all_k, all_v)[which], k),
            li_send.at[i], li_recv.at[i], (xn, yn, dn)[k - 1], me_t,
        )

    def light_mirror(k, which):
        i = 6 + (k - 1) * 2 + which
        area = light_area((all_k, all_v)[which], k)
        return push(area, area, li_send.at[i], li_recv.at[i], sib, me_t)

    load_ck.wait()
    load_cv.wait()
    for copy in swaps:
        copy.wait()
    both_k = fetch(7, chip_k, all_k.at[pl.ds(0, 2 * parts)])
    both_v = fetch(8, chip_v, all_v.at[pl.ds(0, 2 * parts)])

    @pl.when(pos == 0)
    def _():
        for i in range(hot_rows):
            at = tab[2, 0] + hot_rows * c + i
            all_k[2 * parts + hot_rows * c + i] = chip_k[at]
            all_v[2 * parts + hot_rows * c + i] = chip_v[at]
            if i % chunk == chunk - 1:
                for which in range(2):
                    forward(i // chunk, which).start()

    for k in (3, 1, 2):
        for t in range(lane_rows):
            at = tab[0, k * cap + lane_rows * c + t]
            send_k[k - 1, t] = chip_k[at]
            send_v[k - 1, t] = chip_v[at]
        for which in range(2):
            light(k, which).start()

    def relay(*list_of):
        for where, q in list_of:

            @pl.when(pos == where)
            def _():
                for which in range(2):
                    forward(q, which).wait_recv()
                    if where < 3:
                        forward(q, which).start()
                    mirror(q, which).start()

    own_act.wait()
    for copy in acts:
        copy.wait()
    square = jnp.zeros((rows, 1), f32)
    for t in range(tps):
        u = act_all[t].astype(f32)
        square = square + jnp.sum(u * u, -1, keepdims=True)
    inv = lax.rsqrt(square / (width * tps) + 1e-05)
    normed = []
    for t in range(tps):
        u = act_all[t].astype(f32)
        normed.append((u * inv * gain[:, t * width : (t + 1) * width]).astype(bf16))

    def project(w):
        total = None
        for t in range(tps):
            part = jnp.dot(
                normed[t], w[t * width : (t + 1) * width, :], preferred_element_type=f32
            )
            total = part if total is None else total + part
        return total

    cos_t, sin_t = cosine[...], sine[...]

    def turn(u):
        return u * cos_t + pltpu.roll(u, HD // 2, 1) * sin_t

    load_k.wait()
    load_v.wait()
    keys = project(wk_v)
    fresh = fresh_all.at[me_d]
    for g in range(groups):
        fresh[:, g * HD : (g + 1) * HD] = turn(keys[:, g * HD : (g + 1) * HD]).astype(bf16)
    fresh[:, kvw:] = project(wv_v).astype(bf16)

    def fresh_copy(i, block, to):
        area = fresh_all.at[block]
        return push(area, area, fr_send.at[i], fr_recv.at[i], to, me_t)

    news = [fresh_copy(i, me_d, to) for i, to in enumerate((dn, xn, yn, sib))]
    for copy in news:
        copy.start()
    load_q.wait()
    query = project(wq_v)
    for h in range(groups * per):
        g, j = h // per, h % per
        turned = turn(query[:, h * HD : (h + 1) * HD])
        for s in range(steps):
            qs[g, :, s * per + j, :] = turned[s * parts : (s + 1) * parts]
    relay((1, 0))

    lines = parts * pack
    row = lax.broadcasted_iota(jnp.int32, (lines, rows), 0)
    col = lax.broadcasted_iota(jnp.int32, (lines, rows), 1)
    allowed = (row // pack == col % parts) & (col // parts <= (row % pack) // per)
    scale = HD**0.5
    for g in range(groups):
        lanes = slice(g * HD, (g + 1) * HD)
        qg = qs[g].reshape(lines, HD).astype(bf16)
        for n in range(parts):
            sc1[g, n * pack : (n + 1) * pack, :] = lax.dot_general(
                qg[n * pack : (n + 1) * pack], chip_k[n, :, lanes],
                (((1,), (1,)), ((), ())), preferred_element_type=f32,
            )
        near = lax.dot_general(
            qg, fresh[:, lanes], (((1,), (1,)), ((), ())), preferred_element_type=f32
        )
        near = jnp.where(allowed, near / scale, -jnp.inf)
        far = sc1[g] / scale
        top = jnp.maximum(
            jnp.max(far, -1, keepdims=True), jnp.max(near, -1, keepdims=True)
        )
        far = jnp.exp(far - top)
        near = jnp.exp(near - top)
        mass = jnp.sum(far, -1, keepdims=True) + jnp.sum(near, -1, keepdims=True)
        far = (far / mass).astype(bf16)
        near = (near / mass).astype(bf16)
        extra = jnp.dot(
            near, fresh[:, kvw + g * HD : kvw + (g + 1) * HD], preferred_element_type=f32
        )
        for n in range(parts):
            part = slice(n * pack, (n + 1) * pack)
            cx[g, n] = extra[part] + jnp.dot(
                far[part], chip_v[n, :, lanes], preferred_element_type=f32
            )
        if g == 0:
            relay((1, 1), (2, 0))
    for h in range(groups * per):
        g, j = h // per, h % per
        for s in range(steps):
            ctx_b[s * parts : (s + 1) * parts, h * HD : (h + 1) * HD] = cx[
                g, :, s * per + j, :
            ].astype(bf16)
    relay((1, 2), (2, 1), (3, 0))
    load_o.wait()

    def mix(p):
        return jnp.dot(
            ctx_b[...], wo_v[:, pl.ds(pl.multiple_of(p * width, HD), width)],
            preferred_element_type=f32,
        )

    sums = []
    for k in (2, 1, 3)[: tps - 1]:
        rs_send[k - 1] = mix((me_t + k) % tps).astype(bf16)
        sums.append(tp_push(tps - 1, k, rs_send.at[k - 1], rs_recv.at[k - 1]))
    head = mix(me_t)
    relay((1, 3), (2, 2), (3, 1))
    for copy in news:
        copy.wait_recv()
    passed = [fresh_copy(4 + i, b + c, sib) for i, b in enumerate((dn - c, xn - c, yn - c))]
    for copy in passed:
        copy.start()
    for copy in sums:
        copy.wait()
    for k in range(1, tps):
        head = head + rs_recv[k - 1].astype(f32)
    attn_out[...] = head.astype(bf16)
    summed = act_all[me_t].astype(f32) + head
    along = jnp.sum(summed * twist[...], -1, keepdims=True)
    energy = jnp.sum(summed * summed, -1, keepdims=True)
    lane = lax.broadcasted_iota(jnp.int32, (rows, HD), 1)
    sc_all[me_t] = jnp.where(lane < HD // 2, along, energy)
    scores = [
        tp_push(2 * (tps - 1), k, sc_all.at[me_t], sc_all.at[me_t]) for k in range(1, tps)
    ]
    relay((2, 3), (3, 2))
    for copy in scores:
        copy.wait()
    both = sc_all[0]
    for t in range(1, tps):
        both = both + sc_all[t]
    score = both[:, :1] / jnp.sqrt(both[:, HD - 1 :] / (width * tps) + 1e-06)
    total = score[:parts]
    for s in range(1, steps):
        total = total + score[s * parts : (s + 1) * parts]
    mine = jnp.broadcast_to(aux[...] + total, (parts, HD))
    lw_all[me_d] = mine
    lws = []
    for k in range(1, doms):
        copy = push(
            lw_all.at[me_d], lw_all.at[me_d], lw_send.at[k - 1], lw_recv.at[k - 1],
            (me_d + k) % doms, me_t,
        )
        copy.start()
        lws.append(copy)

    for k in (1, 2, 3):
        for which in range(2):
            light(k, which).wait_recv()
            light_mirror(k, which).start()
    relay((3, 3))
    for copy in passed:
        copy.wait()
    index = lax.broadcasted_iota(jnp.int32, (doms * rows, HD), 0)
    pick = (index == tabv[3:4, :]).astype(f32).astype(bf16)
    chosen = lax.dot_general(
        pick, fresh_all[...].reshape(doms * rows, 2 * kvw),
        (((0,), (0,)), ((), ())), preferred_element_type=f32,
    ).astype(bf16)
    for i in range(parts):
        new_k[i, span:, :] = chosen[i * 8 : i * 8 + steps, :kvw]
        new_v[i, span:, :] = chosen[i * 8 : i * 8 + steps, kvw:]

    for copy in lws:
        copy.wait()
    largest = jnp.max(lw_all[...], (0, 1), keepdims=True)[0]
    mass = jnp.sum(jnp.exp(lw_all[...] - largest[None]), (0, 1), keepdims=True)[0]
    out_lw[...] = mine - (largest + jnp.log(mass))

    both_k.wait()
    both_v.wait()
    for k in (1, 2, 3):
        for which in range(2):
            light_mirror(k, which).wait_recv()

    @pl.when(pos > 0)
    def _():
        for q in range(4):
            for which in range(2):
                mirror(q, which).wait()

    for i in range(parts):
        at = tab[1, i]
        new_k[i, :span, :] = all_k[at]
        new_v[i, :span, :] = all_v[at]

    @pl.when(pos < 3)
    def _():
        for q in range(4):
            for which in range(2):
                forward(q, which).wait_send()

    for k in (1, 2, 3):
        for which in range(2):
            light(k, which).wait_send()
            light_mirror(k, which).wait_send()
    for copy in news:
        copy.wait_send()


def adaptive(
    activations, norm_gain, w_query, w_key, value_weight, w_output, cache_keys, cache_values,
    tokens, twisting_table, twist_vec, previous_log_weights, copy_counts,
):
    f32, bf16 = jnp.float32, jnp.bfloat16
    steps, parts, width = activations.shape
    rows = steps * parts
    span = cache_keys.shape[1]
    kvw = w_key.shape[1]
    qw = w_query.shape[1]
    groups = kvw // HD
    pack = steps * (qw // kvw)
    doms = lax.axis_size("dom")
    tps = lax.axis_size("tp")
    middle = HD // 2
    cap = CAP
    angles = (span + np.arange(rows) // parts)[:, None] * (
        500000.0 ** (-2.0 * np.arange(middle) / HD)
    )
    cosine = np.concatenate([np.cos(angles)] * 2, 1).astype(np.float32)
    sine = np.concatenate([-np.sin(angles), np.sin(angles)], 1).astype(np.float32)
    reward = jnp.sum(twisting_table[tokens].astype(f32), 0)
    aux = (previous_log_weights + reward).reshape(parts, 1)
    vmem = pl.BlockSpec(memory_space=pltpu.VMEM)
    smem = pl.BlockSpec(memory_space=pltpu.SMEM)
    hbm = pl.BlockSpec(memory_space=pl.ANY)
    tab = pl.pallas_call(
        functools.partial(plan_kernel, parts, doms, cap, steps, rows),
        out_shape=jax.ShapeDtypeStruct((8, HD), jnp.int32),
        in_specs=[vmem],
        out_specs=vmem,
        scratch_shapes=[
            pltpu.VMEM((doms, 8, HD), f32),
            pltpu.SemaphoreType.DMA((doms - 1,)),
            pltpu.SemaphoreType.DMA((doms - 1,)),
        ],
        compiler_params=pltpu.CompilerParams(collective_id=5, has_side_effects=True),
        name="plan",
    )(copy_counts.reshape(1, parts))

    def hot_branch(hot):
        result = jax.ShapeDtypeStruct((parts, span + steps, kvw), bf16)
        dma = pltpu.SemaphoreType.DMA
        call = pl.pallas_call(
            functools.partial(main_kernel, steps, parts, doms, tps, cap, hot),
            out_shape=(
                jax.ShapeDtypeStruct((rows, width), bf16), result, result,
                jax.ShapeDtypeStruct((parts, HD), f32),
            ),
            in_specs=[hbm, vmem] + [hbm] * 6 + [vmem] * 4 + [smem, vmem],
            out_specs=(vmem,) * 4,
            scratch_shapes=[
                pltpu.VMEM((tps, rows, width), bf16),
                pltpu.VMEM(w_query.shape, bf16),
                pltpu.VMEM(w_key.shape, bf16),
                pltpu.VMEM(value_weight.shape, bf16),
                pltpu.VMEM(w_output.shape, bf16),
                pltpu.VMEM((2 * parts, span, kvw), bf16),
                pltpu.VMEM((2 * parts, span, kvw), bf16),
                pltpu.VMEM((3 * parts + 3 * cap, span, kvw), bf16),
                pltpu.VMEM((3 * parts + 3 * cap, span, kvw), bf16),
                pltpu.VMEM((3, cap // 2, span, kvw), bf16),
                pltpu.VMEM((3, cap // 2, span, kvw), bf16),
                pltpu.VMEM((groups, parts, pack, HD), f32),
                pltpu.VMEM((groups, parts, pack, HD), f32),
                pltpu.VMEM((groups, parts * pack, span), f32),
                pltpu.VMEM((rows, qw), bf16),
                pltpu.VMEM((doms, rows, 2 * kvw), bf16),
                pltpu.VMEM((tps - 1, rows, width), bf16),
                pltpu.VMEM((tps - 1, rows, width), bf16),
                pltpu.VMEM((tps, rows, HD), f32),
                pltpu.VMEM((doms, parts, HD), f32),
                dma((9,)),
                dma((3 * (tps - 1),)), dma((3 * (tps - 1),)),
                dma((doms - 1,)), dma((doms - 1,)),
                dma((2,)), dma((2,)),
                dma((16,)), dma((16,)),
                dma((12,)), dma((12,)),
                dma((7,)), dma((7,)),
            ],
            compiler_params=pltpu.CompilerParams(
                collective_id=hot, has_side_effects=True, vmem_limit_bytes=60 << 20
            ),
            name=f"main{hot}",
        )

        def run(act, gain, wq, wk, wv, wo, ck, cv, twist, aux, counts, cosine, sine, tab):
            attn, new_k, new_v, out_lw = call(
                act, gain, wq, wk, wv, wo, ck, cv, twist, aux, cosine, sine, tab, tab
            )
            return attn, new_k, new_v, out_lw

        return run

    def every(act, gain, wq, wk, wv, wo, ck, cv, twist, aux, counts, cosine, sine, tab):
        return all_rows(
            steps, parts, act, gain, wq, wk, wv, wo, ck, cv, twist,
            jnp.concatenate([aux, counts.astype(f32)], 1), cosine, sine,
        )

    attn, new_k, new_v, out_lw = lax.switch(
        tab[4, 0],
        [hot_branch(hot) for hot in range(4)] + [every],
        activations.reshape(rows, width), norm_gain.reshape(1, -1), w_query, w_key,
        value_weight, w_output, cache_keys, cache_values, twist_vec.reshape(1, -1), aux,
        copy_counts.reshape(parts, 1), jnp.asarray(cosine), jnp.asarray(sine), tab,
    )
    return attn.reshape(steps, parts, width), new_k, new_v, out_lw[:, 0]


def solution(mesh):
    body = adaptive if mesh.shape["dom"] == 8 else local
    return jax.shard_map(
        body,
        mesh=mesh,
        in_specs=(
            P(None, "dom", "tp"),
            P(),
            P(None, "tp"),
            P(None, "tp"),
            P(None, "tp"),
            P("tp", None),
            P("dom", None, "tp"),
            P("dom", None, "tp"),
            P(None, "dom"),
            P(),
            P("tp"),
            P("dom"),
            P("dom"),
        ),
        out_specs=(P(None, "dom", "tp"), P("dom", None, "tp"), P("dom", None, "tp"), P("dom")),
        check_vma=False,
    )
```

```python
import functools

import jax
import jax.numpy as jnp
import numpy as np
from jax import lax
from jax.experimental import pallas as pl
from jax.experimental.pallas import tpu as pltpu
from jax.sharding import PartitionSpec as P

D = 4096
HD = 128
CAP = 6
HOT_CAP = 4


def rotate(tensor, positions):
    middle = tensor.shape[-1] // 2
    frequency = 500000.0 ** (-2.0 * jnp.arange(middle, dtype=jnp.float32) / tensor.shape[-1])
    angles = positions[:, None] * frequency[None, :]
    cosine = jnp.cos(angles)[:, None, None, :]
    sine_part = jnp.sin(angles)[:, None, None, :]
    lower_half = tensor[..., :middle]
    upper_half = tensor[..., middle:]
    return jnp.concatenate(
        [
            lower_half * cosine - upper_half * sine_part,
            upper_half * cosine + lower_half * sine_part,
        ],
        -1,
    )


def local(
    activations,
    norm_gain,
    w_query,
    w_key,
    value_weight,
    w_output,
    cache_keys,
    cache_values,
    tokens,
    twisting_table,
    twist_vec,
    previous_log_weights,
    copy_counts,
):
    step_count = activations.shape[0]
    particle_count = activations.shape[1]
    span_old = cache_keys.shape[1]
    dom_size = lax.axis_size("dom")
    kv_local = w_key.shape[1] // HD
    q_local = w_query.shape[1] // HD
    group_size = q_local // kv_local
    all_counts = lax.all_gather(copy_counts, "dom", axis=0, tiled=True)
    copy_ends = jnp.cumsum(all_counts)
    ranks = jnp.arange(particle_count, dtype=jnp.int32) * dom_size + lax.axis_index("dom")
    ancestor = jnp.sum((copy_ends[None, :] <= ranks[:, None]).astype(jnp.int32), 1)
    all_keys = lax.all_gather(cache_keys, "dom", axis=0, tiled=True)
    all_values = lax.all_gather(cache_values, "dom", axis=0, tiled=True)

    gathered = lax.all_gather(activations, "tp", axis=2, tiled=True)
    inputs = gathered.astype(jnp.float32)
    normed = (
        inputs * lax.rsqrt(jnp.mean(inputs * inputs, -1, keepdims=True) + 1e-05) * norm_gain
    ).astype(jnp.bfloat16)
    flat_rows = normed.reshape(step_count * particle_count, D)
    positions = (span_old + jnp.arange(step_count, dtype=jnp.int32)).astype(jnp.float32)
    queries = jnp.dot(flat_rows, w_query, preferred_element_type=jnp.float32).reshape(
        step_count, particle_count, q_local, HD
    )
    queries = rotate(queries, positions).astype(jnp.bfloat16)
    fresh_keys = jnp.dot(flat_rows, w_key, preferred_element_type=jnp.float32).reshape(
        step_count, particle_count, kv_local, HD
    )
    fresh_keys = (
        rotate(fresh_keys, positions)
        .astype(jnp.bfloat16)
        .reshape(step_count, particle_count, kv_local * HD)
    )
    fresh_values = jnp.dot(flat_rows, value_weight, preferred_element_type=jnp.float32).astype(
        jnp.bfloat16
    )
    fresh_values = fresh_values.reshape(step_count, particle_count, kv_local * HD)
    fresh_keys = jnp.transpose(fresh_keys, (1, 0, 2))
    fresh_values = jnp.transpose(fresh_values, (1, 0, 2))
    key_rows = jnp.concatenate([cache_keys, fresh_keys], 1)
    value_rows = jnp.concatenate([cache_values, fresh_values], 1)
    key_span = span_old + step_count
    query_heads = queries.reshape(step_count, particle_count, kv_local, group_size, HD)
    key_heads = key_rows.reshape(particle_count, key_span, kv_local, HD)
    value_heads = value_rows.reshape(particle_count, key_span, kv_local, HD)
    scores = (
        jnp.einsum("snkgd,nlkd->snkgl", query_heads, key_heads, preferred_element_type=jnp.float32)
        / HD**0.5
    )
    allowed = (
        jnp.arange(key_span, dtype=jnp.int32)[None, :]
        <= (span_old + jnp.arange(step_count, dtype=jnp.int32))[:, None]
    )
    allowed = allowed[:, None, None, None, :]
    masked = jnp.where(allowed, scores, -jnp.inf)
    highest = jnp.max(masked, -1, keepdims=True)
    exponent = jnp.exp(masked - highest)
    weights = (exponent / jnp.sum(exponent, -1, keepdims=True)).astype(jnp.bfloat16)
    context = jnp.einsum(
        "snkgl,nlkd->snkgd", weights, value_heads, preferred_element_type=jnp.float32
    ).astype(jnp.bfloat16)
    context = context.reshape(step_count * particle_count, q_local * HD)
    partial_value = jnp.dot(context, w_output, preferred_element_type=jnp.float32).reshape(
        step_count, particle_count, D
    )
    head_mix = lax.psum_scatter(partial_value, "tp", scatter_dimension=2, tiled=True)
    attn_out = head_mix.astype(jnp.bfloat16)
    summed = activations.astype(jnp.float32) + head_mix
    aligned, energy = lax.psum(
        (jnp.sum(summed * twist_vec, -1), jnp.sum(summed * summed, -1)), "tp"
    )
    twisting_score = aligned / jnp.sqrt(energy / D + 1e-06)
    token_reward = twisting_table[tokens].astype(jnp.float32)
    particle_log_weight = previous_log_weights + jnp.sum(token_reward + twisting_score, 0)
    largest = lax.pmax(jnp.max(particle_log_weight), "dom")
    mass_total = lax.psum(jnp.sum(jnp.exp(particle_log_weight - largest)), "dom")
    out_logw = particle_log_weight - (largest + jnp.log(mass_total))
    fresh = lax.all_gather(
        jnp.concatenate([fresh_keys, fresh_values], 2), "dom", axis=0, tiled=True
    )[ancestor]
    width = fresh_keys.shape[2]
    new_keys = jnp.concatenate([all_keys[ancestor], fresh[..., :width]], 1)
    new_values = jnp.concatenate([all_values[ancestor], fresh[..., width:]], 1)
    return (attn_out, new_keys, new_values, out_logw)


MESH = pl.DeviceIdType.MESH


def layer_kernel(
    steps, parts, doms, tps,
    act, gain, wq, wk, wv, wo, ck, cv, twist, aux, cosine, sine,
    attn_out, all_k, all_v, fresh_sel, out_lw, anc_out,
    act_all, wq_v, wk_v, wv_v, wo_v, ck_v, cv_v, qs, cx, sc1, ctx_b, fresh, fresh_all,
    rs_send, rs_recv, sc_all, lw_all, cnt_all,
    loc, tp_send, tp_recv, dom_send, dom_recv, blk_send, blk_recv,
):
    f32, bf16 = jnp.float32, jnp.bfloat16
    me_d = lax.axis_index("dom")
    me_t = lax.axis_index("tp")
    rows, width = act.shape
    half = parts // 2
    kvw = wk.shape[1]
    groups = kvw // HD
    per = wq.shape[1] // kvw
    pack = steps * per
    c = me_d % 2
    x = (me_d // 2) % 2
    y = me_d // 4
    sib = me_d + 1 - 2 * c
    xn = me_d + 2 - 4 * x
    yn = me_d + 4 - 8 * y
    dn = xn + 4 - 8 * y

    barrier = pltpu.get_barrier_semaphore()
    for k in range(1, tps):
        pl.semaphore_signal(
            barrier, inc=1, device_id=(me_d, (me_t + k) % tps), device_id_type=MESH
        )
    for k in range(1, doms):
        pl.semaphore_signal(
            barrier, inc=1, device_id=((me_d + k) % doms, me_t), device_id_type=MESH
        )

    def fetch(i, src, dst):
        copy = pltpu.make_async_copy(src, dst, loc.at[i])
        copy.start()
        return copy

    own_act = fetch(0, act, act_all.at[me_t])
    load_q = fetch(1, wq, wq_v)
    load_k = fetch(2, wk, wk_v)
    load_v = fetch(3, wv, wv_v)
    load_ck = fetch(4, ck, ck_v)
    load_cv = fetch(5, cv, cv_v)
    load_o = fetch(6, wo, wo_v)

    cnt_all[me_d] = jnp.broadcast_to(aux[:, 1:], cnt_all.shape[1:])
    pl.semaphore_wait(barrier, tps + doms - 2)

    def tp_push(base, k, src, dst):
        copy = pltpu.make_async_remote_copy(
            src_ref=src, dst_ref=dst, send_sem=tp_send.at[base + k - 1],
            recv_sem=tp_recv.at[base + k - 1],
            device_id=(me_d, (me_t + k) % tps), device_id_type=MESH,
        )
        copy.start()
        return copy

    def dom_push(base, k, src, dst):
        copy = pltpu.make_async_remote_copy(
            src_ref=src, dst_ref=dst, send_sem=dom_send.at[base + k - 1],
            recv_sem=dom_recv.at[base + k - 1],
            device_id=((me_d + k) % doms, me_t), device_id_type=MESH,
        )
        copy.start()
        return copy

    acts = [tp_push(0, k, act, act_all.at[me_t]) for k in range(1, tps)]

    def piece(kind, to, which, h, slot, own):
        dst = (all_k, all_v)[which].at[slot, pl.ds(h * half, half)]
        src = (ck, cv)[which].at[pl.ds(h * half, half)] if own else dst
        i = kind * 4 + h * 2 + which
        copy = pltpu.make_async_remote_copy(
            src_ref=src, dst_ref=dst, send_sem=blk_send.at[i], recv_sem=blk_recv.at[i],
            device_id=(to, me_t), device_id_type=MESH,
        )
        copy.start()
        return copy

    moves = {}
    for h, kind, to in ((0, 0, xn), (1, 1, yn), (1, 0, xn), (0, 1, yn)):
        for which in range(2):
            moves[kind, h, which] = piece(kind, to, which, h, me_d, True)
    cnts = [dom_push(0, k, cnt_all.at[me_d], cnt_all.at[me_d]) for k in range(1, doms)]
    for h in range(2):
        for which in range(2):
            moves[3, h, which] = piece(3, sib, which, h, me_d, True)

    own_act.wait()
    for copy in acts:
        copy.wait()
    square = jnp.zeros((rows, 1), f32)
    for t in range(tps):
        u = act_all[t].astype(f32)
        square = square + jnp.sum(u * u, -1, keepdims=True)
    inv = lax.rsqrt(square / (width * tps) + 1e-05)
    normed = []
    for t in range(tps):
        u = act_all[t].astype(f32)
        normed.append((u * inv * gain[:, t * width : (t + 1) * width]).astype(bf16))

    def project(w):
        total = None
        for t in range(tps):
            part = jnp.dot(
                normed[t], w[t * width : (t + 1) * width, :], preferred_element_type=f32
            )
            total = part if total is None else total + part
        return total

    cos_t, sin_t = cosine[...], sine[...]

    def turn(u):
        return u * cos_t + pltpu.roll(u, HD // 2, 1) * sin_t

    load_k.wait()
    load_v.wait()
    keys = project(wk_v)
    for g in range(groups):
        fresh[:, g * HD : (g + 1) * HD] = turn(keys[:, g * HD : (g + 1) * HD]).astype(bf16)
    fresh[:, kvw:] = project(wv_v).astype(bf16)
    fresh_all[me_d] = fresh[...]
    news = [dom_push(doms - 1, k, fresh, fresh_all.at[me_d]) for k in range(1, doms)]
    load_q.wait()
    query = project(wq_v)
    for h in range(groups * per):
        g, j = h // per, h % per
        turned = turn(query[:, h * HD : (h + 1) * HD])
        for s in range(steps):
            qs[g, :, s * per + j, :] = turned[s * parts : (s + 1) * parts]
    load_ck.wait()
    load_cv.wait()
    put_k = fetch(7, ck_v, all_k.at[me_d])
    put_v = fetch(8, cv_v, all_v.at[me_d])

    lines = parts * pack
    row = lax.broadcasted_iota(jnp.int32, (lines, rows), 0)
    col = lax.broadcasted_iota(jnp.int32, (lines, rows), 1)
    allowed = (row // pack == col % parts) & (col // parts <= (row % pack) // per)
    scale = HD**0.5
    for g in range(groups):
        lanes = slice(g * HD, (g + 1) * HD)
        qg = qs[g].reshape(lines, HD).astype(bf16)
        for n in range(parts):
            sc1[g, n * pack : (n + 1) * pack, :] = lax.dot_general(
                qg[n * pack : (n + 1) * pack], ck_v[n, :, lanes],
                (((1,), (1,)), ((), ())), preferred_element_type=f32,
            )
        near = lax.dot_general(
            qg, fresh[:, lanes], (((1,), (1,)), ((), ())), preferred_element_type=f32
        )
        near = jnp.where(allowed, near / scale, -jnp.inf)
        far = sc1[g] / scale
        top = jnp.maximum(
            jnp.max(far, -1, keepdims=True), jnp.max(near, -1, keepdims=True)
        )
        far = jnp.exp(far - top)
        near = jnp.exp(near - top)
        mass = jnp.sum(far, -1, keepdims=True) + jnp.sum(near, -1, keepdims=True)
        far = (far / mass).astype(bf16)
        near = (near / mass).astype(bf16)
        extra = jnp.dot(
            near, fresh[:, kvw + g * HD : kvw + (g + 1) * HD], preferred_element_type=f32
        )
        for n in range(parts):
            span = slice(n * pack, (n + 1) * pack)
            cx[g, n] = extra[span] + jnp.dot(
                far[span], cv_v[n, :, lanes], preferred_element_type=f32
            )
    for h in range(groups * per):
        g, j = h // per, h % per
        for s in range(steps):
            ctx_b[s * parts : (s + 1) * parts, h * HD : (h + 1) * HD] = cx[
                g, :, s * per + j, :
            ].astype(bf16)
    load_o.wait()

    def mix(p):
        return jnp.dot(
            ctx_b[...], wo_v[:, pl.ds(pl.multiple_of(p * width, HD), width)],
            preferred_element_type=f32,
        )

    sums = []
    for k in range(1, tps):
        rs_send[k - 1] = mix((me_t + k) % tps)
        sums.append(tp_push(tps - 1, k, rs_send.at[k - 1], rs_recv.at[k - 1]))
    head = mix(me_t)

    def done(kind, h):
        for which in range(2):
            moves[kind, h, which].wait_recv()

    def relay(kind, to, h, slot):
        for which in range(2):
            moves[kind, h, which] = piece(kind, to, which, h, slot, False)

    done(0, 0)
    relay(2, yn, 0, xn)
    relay(4, sib, 0, xn)
    done(1, 1)
    relay(6, xn, 1, yn)
    relay(5, sib, 1, yn)
    for k in range(1, tps):
        sums[k - 1].wait()
        head = head + rs_recv[k - 1]
    attn_out[...] = head.astype(bf16)
    summed = act_all[me_t].astype(f32) + head
    along = jnp.sum(summed * twist[...], -1, keepdims=True)
    energy = jnp.sum(summed * summed, -1, keepdims=True)
    lane = lax.broadcasted_iota(jnp.int32, (rows, HD), 1)
    sc_all[me_t] = jnp.where(lane < HD // 2, along, energy)
    scores = [
        tp_push(2 * (tps - 1), k, sc_all.at[me_t], sc_all.at[me_t]) for k in range(1, tps)
    ]
    for copy in scores:
        copy.wait()
    both = sc_all[0]
    for t in range(1, tps):
        both = both + sc_all[t]
    score = both[:, :1] / jnp.sqrt(both[:, HD - 1 :] / (width * tps) + 1e-06)
    total = score[:parts]
    for s in range(1, steps):
        total = total + score[s * parts : (s + 1) * parts]
    mine = jnp.broadcast_to(aux[:, :1] + total, (parts, HD))
    lw_all[me_d] = mine
    lws = [
        dom_push(2 * (doms - 1), k, lw_all.at[me_d], lw_all.at[me_d]) for k in range(1, doms)
    ]

    done(0, 1)
    relay(4, sib, 1, xn)
    done(1, 0)
    relay(5, sib, 0, yn)

    for copy in cnts:
        copy.wait()
    for copy in news:
        copy.wait()
    whole = parts * doms
    number = cnt_all[...].reshape(whole, HD).astype(bf16)
    lower = lax.broadcasted_iota(jnp.int32, (whole, whole), 0)
    upper = lax.broadcasted_iota(jnp.int32, (whole, whole), 1)
    ends = jnp.dot(
        (upper <= lower).astype(f32).astype(bf16), number, preferred_element_type=f32
    )
    slot = lax.broadcasted_iota(jnp.int32, (whole, HD), 1)

    def ancestor(place):
        rank = (place * doms + me_d).astype(f32)
        return jnp.sum((ends <= rank).astype(f32), 0, keepdims=True).astype(jnp.int32)

    anc_out[...] = jnp.broadcast_to(ancestor(slot), anc_out.shape)
    lanes = lax.broadcasted_iota(jnp.int32, (1, HD), 1)
    wide = ancestor(slot // 8)
    target = (wide // parts) * rows + (lanes % 8) * parts + wide % parts
    target = jnp.where(lanes % 8 < steps, target, -1)
    index = lax.broadcasted_iota(jnp.int32, (doms * rows, HD), 0)
    pick = (index == target).astype(f32).astype(bf16)
    fresh_sel[...] = lax.dot_general(
        pick, fresh_all[...].reshape(doms * rows, 2 * kvw),
        (((0,), (0,)), ((), ())), preferred_element_type=f32,
    ).astype(bf16)

    for copy in lws:
        copy.wait()
    largest = jnp.max(lw_all[...], (0, 1), keepdims=True)[0]
    mass = jnp.sum(jnp.exp(lw_all[...] - largest[None]), (0, 1), keepdims=True)[0]
    out_lw[...] = mine - (largest + jnp.log(mass))

    done(2, 0)
    relay_d0 = [piece(7, sib, which, 0, dn, False) for which in range(2)]
    done(6, 1)
    relay_d1 = [piece(7, sib, which, 1, dn, False) for which in range(2)]
    for kind in (3, 4, 5):
        for h in range(2):
            done(kind, h)
    for copy in moves.values():
        copy.wait_send()
    for copy in relay_d0 + relay_d1:
        copy.wait()
    put_k.wait()
    put_v.wait()


def select_kernel(parts, steps, anc, fresh_sel, all_k, all_v, new_k, new_v, sem):
    span = all_k.shape[2]
    width = all_k.shape[3]
    copies = []
    for i in range(parts):
        a = anc[0, i]
        d, n = a // parts, a % parts
        for which, (src, dst) in enumerate(((all_k, new_k), (all_v, new_v))):
            copy = pltpu.make_async_copy(
                src.at[d, n], dst.at[i, pl.ds(0, span)], sem.at[2 * i + which]
            )
            copy.start()
            copies.append(copy)
    for i in range(parts):
        new_k[i, span:, :] = fresh_sel[i * 8 : i * 8 + steps, :width]
        new_v[i, span:, :] = fresh_sel[i * 8 : i * 8 + steps, width:]
    for copy in copies:
        copy.wait()


def all_rows(
    steps, parts, act, gain, wq, wk, wv, wo, ck, cv, twist, aux, cosine, sine,
):
    f32, bf16 = jnp.float32, jnp.bfloat16
    rows, width = act.shape
    span = ck.shape[1]
    kvw = wk.shape[1]
    qw = wq.shape[1]
    groups = kvw // HD
    pack = steps * (qw // kvw)
    doms = lax.axis_size("dom")
    tps = lax.axis_size("tp")
    vmem = pl.BlockSpec(memory_space=pltpu.VMEM)
    hbm = pl.BlockSpec(memory_space=pl.ANY)
    block = jax.ShapeDtypeStruct((doms,) + ck.shape, bf16)
    attn, all_k, all_v, fresh_sel, out_lw, anc = pl.pallas_call(
        functools.partial(layer_kernel, steps, parts, doms, tps),
        out_shape=(
            jax.ShapeDtypeStruct((rows, width), bf16), block, block,
            jax.ShapeDtypeStruct((HD, 2 * kvw), bf16),
            jax.ShapeDtypeStruct((parts, HD), f32),
            jax.ShapeDtypeStruct((8, HD), jnp.int32),
        ),
        in_specs=[hbm, vmem] + [hbm] * 6 + [vmem] * 4,
        out_specs=(vmem, hbm, hbm, vmem, vmem, vmem),
        scratch_shapes=[
            pltpu.VMEM((tps, rows, width), bf16),
            pltpu.VMEM(wq.shape, bf16),
            pltpu.VMEM(wk.shape, bf16),
            pltpu.VMEM(wv.shape, bf16),
            pltpu.VMEM(wo.shape, bf16),
            pltpu.VMEM(ck.shape, bf16),
            pltpu.VMEM(cv.shape, bf16),
            pltpu.VMEM((groups, parts, pack, HD), f32),
            pltpu.VMEM((groups, parts, pack, HD), f32),
            pltpu.VMEM((groups, parts * pack, span), f32),
            pltpu.VMEM((rows, qw), bf16),
            pltpu.VMEM((rows, 2 * kvw), bf16),
            pltpu.VMEM((doms, rows, 2 * kvw), bf16),
            pltpu.VMEM((tps - 1, rows, width), f32),
            pltpu.VMEM((tps - 1, rows, width), f32),
            pltpu.VMEM((tps, rows, HD), f32),
            pltpu.VMEM((doms, parts, HD), f32),
            pltpu.VMEM((doms, parts, HD), f32),
            pltpu.SemaphoreType.DMA((9,)),
            pltpu.SemaphoreType.DMA((3 * (tps - 1),)),
            pltpu.SemaphoreType.DMA((3 * (tps - 1),)),
            pltpu.SemaphoreType.DMA((3 * (doms - 1),)),
            pltpu.SemaphoreType.DMA((3 * (doms - 1),)),
            pltpu.SemaphoreType.DMA((32,)),
            pltpu.SemaphoreType.DMA((32,)),
        ],
        compiler_params=pltpu.CompilerParams(
            collective_id=4, has_side_effects=True, vmem_limit_bytes=52 << 20
        ),
        name="layer",
    )(act, gain, wq, wk, wv, wo, ck, cv, twist, aux, cosine, sine)
    result = jax.ShapeDtypeStruct((parts, span + steps, kvw), bf16)
    new_k, new_v = pl.pallas_call(
        functools.partial(select_kernel, parts, steps),
        out_shape=(result, result),
        in_specs=[pl.BlockSpec(memory_space=pltpu.SMEM), vmem, hbm, hbm],
        out_specs=(vmem, vmem),
        scratch_shapes=[pltpu.SemaphoreType.DMA((2 * parts,))],
        compiler_params=pltpu.CompilerParams(vmem_limit_bytes=8 << 20),
        name="select",
    )(anc, fresh_sel, all_k, all_v)
    return attn, new_k, new_v, out_lw


def plan_kernel(
    parts, doms, cap, hot_cap, steps, rows,
    cnt, ck, cv, tab, chip_k, chip_v, cnt_all, send, recv, loc, sib_send, sib_recv,
):
    f32, bf16, i32 = jnp.float32, jnp.bfloat16, jnp.int32
    me_d = lax.axis_index("dom")
    me_t = lax.axis_index("tp")
    core = me_d % 2
    x = (me_d // 2) % 2
    y = me_d // 4
    chip = me_d // 2
    barrier = pltpu.get_barrier_semaphore()
    for k in range(1, doms):
        pl.semaphore_signal(
            barrier, inc=1, device_id=((me_d + k) % doms, me_t), device_id_type=MESH
        )
    owns = []
    for i, (src, dst) in enumerate(((ck, chip_k), (cv, chip_v))):
        copy = pltpu.make_async_copy(src, dst.at[pl.ds(0, parts)], loc.at[i])
        copy.start()
        owns.append(copy)
    cnt_all[me_d] = jnp.zeros(cnt_all.shape[1:], f32)
    cnt_all[me_d, :, :parts] = jnp.broadcast_to(cnt[...].astype(f32), (8, parts))
    pl.semaphore_wait(barrier, doms - 1)
    copies = []
    for k in range(1, doms):
        copy = pltpu.make_async_remote_copy(
            src_ref=cnt_all.at[me_d], dst_ref=cnt_all.at[me_d],
            send_sem=send.at[k - 1], recv_sem=recv.at[k - 1],
            device_id=((me_d + k) % doms, me_t), device_id_type=MESH,
        )
        copy.start()
        copies.append(copy)
    swaps = []
    for i, (src, dst) in enumerate(((ck, chip_k), (cv, chip_v))):
        copy = pltpu.make_async_remote_copy(
            src_ref=src, dst_ref=dst.at[pl.ds(parts, parts)],
            send_sem=sib_send.at[i], recv_sem=sib_recv.at[i],
            device_id=(me_d + 1 - 2 * core, me_t), device_id_type=MESH,
        )
        copy.start()
        swaps.append(copy)
    for copy in copies:
        copy.wait()
    whole = parts * doms
    j = lax.broadcasted_iota(i32, (whole, HD), 0)
    lane = lax.broadcasted_iota(i32, (whole, HD), 1)
    spread = jnp.concatenate([cnt_all[d] for d in range(doms) for _ in range(parts // 8)], 0)
    column = jnp.sum(jnp.where(lane == j % parts, spread, 0.0), -1, keepdims=True)
    number = jnp.broadcast_to(column, (whole, HD))
    first = lax.broadcasted_iota(i32, (whole, whole), 0)
    second = lax.broadcasted_iota(i32, (whole, whole), 1)

    def total(mask, values):
        return jnp.dot(
            mask.astype(f32).astype(bf16), values.astype(bf16), preferred_element_type=f32
        )

    ends = total(second <= first, number)
    loads = total(second // parts == first // parts, number)
    number = number.astype(i32)
    ends = ends.astype(i32)
    starts = ends - number
    top = jnp.max(loads, (0, 1), keepdims=True)
    owner = j // parts
    heavy = jnp.min(jnp.where(loads == top, owner, doms).astype(f32), (0, 1), keepdims=True)
    heavy = heavy.astype(i32)
    light = owner != heavy
    home = j // (2 * parts)

    def needs(to):
        hit = None
        for m in range(4):
            one = (m < number) & (((starts + m) % doms) // 2 == to)
            hit = one if hit is None else hit | one
        return hit & light & (home != to)

    kind = (lane // cap) % 4
    there_x = x + kind % 2 - 2 * x * (kind % 2)
    there_y = y + kind // 2 - 2 * y * (kind // 2)
    need_send = needs(2 * there_y + there_x)
    need_here = needs(jnp.broadcast_to(chip, (whole, HD)))
    need_any = needs(lane % 4)
    before = (second < first) & (second // (2 * parts) == first // (2 * parts))
    places = total(
        before,
        jnp.concatenate([u.astype(f32) for u in (need_send, need_here, need_any)], 1),
    ).astype(i32)
    place_send = places[:, :HD]
    place_here = places[:, HD : 2 * HD]
    place_any = places[:, 2 * HD :]
    local_row = j % parts + parts * (owner % 2 + core - 2 * core * (owner % 2))
    half = cap // 2
    entry = lane % cap
    picked = need_send & (place_send == 2 * (entry % half) + entry // half) & (home == chip)
    sources = jnp.sum(jnp.where(picked, local_row, 0).astype(f32), 0, keepdims=True)
    hx, hy = home % 2, home // 2
    away = (hx + x - 2 * x * hx) + 2 * (hy + y - 2 * y * hy)
    value = jnp.where(
        away == 0,
        local_row,
        jnp.where(
            light,
            3 * parts + (away - 1) * cap + place_here % 2 * half + place_here // 2,
            2 * parts + j % parts,
        ),
    )
    rank = lane * doms + me_d
    mine = (starts <= rank) & (rank < ends)
    index = jnp.sum(jnp.where(mine, value, 0).astype(f32), 0, keepdims=True)
    wide = (lane // 8) * doms + me_d
    old = jnp.sum((ends <= wide).astype(f32), 0, keepdims=True).astype(i32)
    row = lax.broadcasted_iota(i32, (1, HD), 1)
    target = (old // parts) * rows + (row % 8) * parts + old % parts
    target = jnp.where(row % 8 < steps, target, -1)
    room = jnp.where(home == heavy // 2, hot_cap, cap)
    over = jnp.max(
        (need_any & (place_any >= room)).astype(f32), (0, 1), keepdims=True
    ).astype(i32)
    base = parts * (heavy % 2 + core - 2 * core * (heavy % 2))
    branch = jnp.where(over == 0, heavy // 2, 4)
    tab[0:1, :] = sources.astype(i32)
    tab[1:2, :] = index.astype(i32)
    tab[2:3, :] = jnp.broadcast_to(base, (1, HD))
    tab[3:4, :] = target
    tab[4:5, :] = jnp.broadcast_to(branch, (1, HD))
    tab[5:8, :] = jnp.zeros((3, HD), i32)
    for copy in owns + swaps:
        copy.wait()


def main_kernel(
    steps, parts, doms, tps, cap, hot_cap, hot,
    act, gain, wq, wk, wv, wo, chip_k, chip_v, twist, tokens, table, prev, cosine, sine,
    tab, tabv,
    attn_out, new_k, new_v, out_lw,
    act_all, wq_v, wk_v, wv_v, wo_v, all_k, all_v, send_k, send_v,
    qs, cx, sc1, ctx_b, fresh_all, rs_send, rs_recv, sc_all, lw_all,
    loc, tp_send, tp_recv, lw_send, lw_recv,
    hv_send, hv_recv, li_send, li_recv, fr_send, fr_recv,
):
    f32, bf16 = jnp.float32, jnp.bfloat16
    me_d = lax.axis_index("dom")
    me_t = lax.axis_index("tp")
    rows, width = act.shape
    kvw = wk.shape[1]
    groups = kvw // HD
    per = wq.shape[1] // kvw
    pack = steps * per
    span = chip_k.shape[1]
    c = me_d % 2
    x = (me_d // 2) % 2
    y = me_d // 4
    sib = me_d + 1 - 2 * c
    xn = me_d + 2 - 4 * x
    yn = me_d + 4 - 8 * y
    dn = xn + 4 - 8 * y
    rx = x if hot % 2 == 0 else 1 - x
    ry = y if hot // 2 == 0 else 1 - y
    pos = (1 - c) * (3 * ry + rx * (1 - 2 * ry)) + c * (3 * rx + ry * (1 - 2 * rx))
    turn_y = (pos + c) % 2
    onward = xn + turn_y * (yn - xn)

    barrier = pltpu.get_barrier_semaphore()
    for k in range(1, tps):
        pl.semaphore_signal(
            barrier, inc=1, device_id=(me_d, (me_t + k) % tps), device_id_type=MESH
        )
    for k in range(1, doms):
        pl.semaphore_signal(
            barrier, inc=1, device_id=((me_d + k) % doms, me_t), device_id_type=MESH
        )

    def fetch(i, src, dst):
        copy = pltpu.make_async_copy(src, dst, loc.at[i])
        copy.start()
        return copy

    own_act = fetch(0, act, act_all.at[me_t])
    load_k = fetch(2, wk, wk_v)
    load_v = fetch(3, wv, wv_v)
    load_q = fetch(1, wq, wq_v)
    load_o = fetch(6, wo, wo_v)
    pl.semaphore_wait(barrier, tps + doms - 2)

    def push(src, dst, ssem, rsem, to_d, to_t):
        return pltpu.make_async_remote_copy(
            src_ref=src, dst_ref=dst, send_sem=ssem, recv_sem=rsem,
            device_id=(to_d, to_t), device_id_type=MESH,
        )

    def tp_push(base, k, src, dst):
        copy = push(
            src, dst, tp_send.at[base + k - 1], tp_recv.at[base + k - 1],
            me_d, (me_t + k) % tps,
        )
        copy.start()
        return copy

    acts = [tp_push(0, k, act, act_all.at[me_t]) for k in range(1, tps)]
    lane_rows = cap // 2
    hot_lane = hot_cap // 2
    rel = rx + 2 * ry
    hot_rows = parts // 2
    chunk = hot_rows // 4

    def hot_copy(q, which, to, base):
        ref = (all_k, all_v)[which]
        area = ref.at[pl.ds(2 * parts + hot_rows * c + q * chunk, chunk)]
        i = base + q * 2 + which
        return push(area, area, hv_send.at[i], hv_recv.at[i], to, me_t)

    def forward(q, which):
        return hot_copy(q, which, onward, 0)

    def mirror(q, which):
        return hot_copy(q, which, sib, 8)

    def light_part(ref, base, piece):
        if piece == 0:
            return ref.at[pl.ds(base, hot_lane)]
        return ref.at[pl.ds(base + hot_lane, lane_rows - hot_lane)]

    def light_area(which, k, piece):
        base = 3 * parts + (k - 1) * cap + lane_rows * c
        return light_part((all_k, all_v)[which], base, piece)

    def light(k, which, piece):
        i = ((k - 1) * 2 + which) * 2 + piece
        return push(
            light_part((send_k, send_v)[which].at[k - 1], 0, piece),
            light_area(which, k, piece),
            li_send.at[i], li_recv.at[i], (xn, yn, dn)[k - 1], me_t,
        )

    def light_mirror(k, which, piece):
        i = 12 + ((k - 1) * 2 + which) * 2 + piece
        area = light_area(which, k, piece)
        return push(area, area, li_send.at[i], li_recv.at[i], sib, me_t)

    def send_lights(count, pieces):
        for k in (3, 1, 2):
            for t in range(count):
                at = tab[0, k * cap + lane_rows * c + t]
                send_k[k - 1, t] = chip_k[at]
                send_v[k - 1, t] = chip_v[at]
            for piece in range(pieces):
                for which in range(2):
                    light(k, which, piece).start()

    def arrived(k):
        for which in range(2):
            light(k, which, 0).wait_recv()
            light_mirror(k, which, 0).start()

        @pl.when(rel != k)
        def _():
            for which in range(2):
                light(k, which, 1).wait_recv()
                light_mirror(k, which, 1).start()

    both_k = fetch(7, chip_k, all_k.at[pl.ds(0, 2 * parts)])
    both_v = fetch(8, chip_v, all_v.at[pl.ds(0, 2 * parts)])

    @pl.when(pos == 0)
    def _():
        for i in range(hot_rows):
            at = tab[2, 0] + hot_rows * c + i
            all_k[2 * parts + hot_rows * c + i] = chip_k[at]
            all_v[2 * parts + hot_rows * c + i] = chip_v[at]
            if i % chunk == chunk - 1:
                for which in range(2):
                    forward(i // chunk, which).start()

    @pl.when(pos > 0)
    def _():
        send_lights(lane_rows, 2)

    def relay(*list_of):
        for where, q in list_of:

            @pl.when(pos == where)
            def _():
                for which in range(2):
                    forward(q, which).wait_recv()
                    if where < 3:
                        forward(q, which).start()
                    mirror(q, which).start()

    relay((1, 0))
    relay((1, 1))
    relay((1, 2))
    own_act.wait()
    for copy in acts:
        copy.wait()
    square = jnp.zeros((rows, 1), f32)
    for t in range(tps):
        u = act_all[t].astype(f32)
        square = square + jnp.sum(u * u, -1, keepdims=True)
    inv = lax.rsqrt(square / (width * tps) + 1e-05)
    normed = []
    for t in range(tps):
        u = act_all[t].astype(f32)
        normed.append((u * inv * gain[:, t * width : (t + 1) * width]).astype(bf16))

    def project(w):
        total = None
        for t in range(tps):
            part = jnp.dot(
                normed[t], w[t * width : (t + 1) * width, :], preferred_element_type=f32
            )
            total = part if total is None else total + part
        return total

    cos_t, sin_t = cosine[...], sine[...]

    def turn(u):
        return u * cos_t + pltpu.roll(u, HD // 2, 1) * sin_t

    load_k.wait()
    load_v.wait()
    keys = project(wk_v)
    fresh = fresh_all.at[me_d]
    for g in range(groups):
        fresh[:, g * HD : (g + 1) * HD] = turn(keys[:, g * HD : (g + 1) * HD]).astype(bf16)
    fresh[:, kvw:] = project(wv_v).astype(bf16)

    def fresh_copy(i, block, to):
        area = fresh_all.at[block]
        return push(area, area, fr_send.at[i], fr_recv.at[i], to, me_t)

    news = [fresh_copy(i, me_d, to) for i, to in enumerate((dn, xn, yn, sib))]
    for copy in news:
        copy.start()
    load_q.wait()
    query = project(wq_v)
    for h in range(groups * per):
        g, j = h // per, h % per
        turned = turn(query[:, h * HD : (h + 1) * HD])
        for s in range(steps):
            qs[g, :, s * per + j, :] = turned[s * parts : (s + 1) * parts]
    relay((1, 3), (2, 0))

    @pl.when(pos == 0)
    def _():
        send_lights(hot_lane, 1)

    lines = parts * pack
    row = lax.broadcasted_iota(jnp.int32, (lines, rows), 0)
    col = lax.broadcasted_iota(jnp.int32, (lines, rows), 1)
    allowed = (row // pack == col % parts) & (col // parts <= (row % pack) // per)
    scale = HD**0.5
    for g in range(groups):
        lanes = slice(g * HD, (g + 1) * HD)
        qg = qs[g].reshape(lines, HD).astype(bf16)
        for n in range(parts):
            sc1[g, n * pack : (n + 1) * pack, :] = lax.dot_general(
                qg[n * pack : (n + 1) * pack], chip_k[n, :, lanes],
                (((1,), (1,)), ((), ())), preferred_element_type=f32,
            )
        near = lax.dot_general(
            qg, fresh[:, lanes], (((1,), (1,)), ((), ())), preferred_element_type=f32
        )
        near = jnp.where(allowed, near / scale, -jnp.inf)
        far = sc1[g] / scale
        top = jnp.maximum(
            jnp.max(far, -1, keepdims=True), jnp.max(near, -1, keepdims=True)
        )
        far = jnp.exp(far - top)
        near = jnp.exp(near - top)
        mass = jnp.sum(far, -1, keepdims=True) + jnp.sum(near, -1, keepdims=True)
        far = (far / mass).astype(bf16)
        near = (near / mass).astype(bf16)
        extra = jnp.dot(
            near, fresh[:, kvw + g * HD : kvw + (g + 1) * HD], preferred_element_type=f32
        )
        for n in range(parts):
            part = slice(n * pack, (n + 1) * pack)
            cx[g, n] = extra[part] + jnp.dot(
                far[part], chip_v[n, :, lanes], preferred_element_type=f32
            )
    for h in range(groups * per):
        g, j = h // per, h % per
        for s in range(steps):
            ctx_b[s * parts : (s + 1) * parts, h * HD : (h + 1) * HD] = cx[
                g, :, s * per + j, :
            ].astype(bf16)
    load_o.wait()

    def mix(p):
        return jnp.dot(
            ctx_b[...], wo_v[:, pl.ds(pl.multiple_of(p * width, HD), width)],
            preferred_element_type=f32,
        )

    sums = []
    for k in (2, 1, 3)[: tps - 1]:
        rs_send[k - 1] = mix((me_t + k) % tps).astype(bf16)
        sums.append(tp_push(tps - 1, k, rs_send.at[k - 1], rs_recv.at[k - 1]))
    head = mix(me_t)
    relay((2, 1))
    relay((2, 2))
    relay((2, 3), (3, 0))
    relay((3, 1))
    arrived(1)
    arrived(2)
    for copy in news:
        copy.wait_recv()
    passed = [fresh_copy(4 + i, b + c, sib) for i, b in enumerate((dn - c, xn - c, yn - c))]
    for copy in passed:
        copy.start()
    for copy in sums:
        copy.wait()
    for k in range(1, tps):
        head = head + rs_recv[k - 1].astype(f32)
    attn_out[...] = head.astype(bf16)
    summed = act_all[me_t].astype(f32) + head
    along = jnp.sum(summed * twist[...], -1, keepdims=True)
    energy = jnp.sum(summed * summed, -1, keepdims=True)
    lane = lax.broadcasted_iota(jnp.int32, (rows, HD), 1)
    sc_all[me_t] = jnp.where(lane < HD // 2, along, energy)
    scores = [
        tp_push(2 * (tps - 1), k, sc_all.at[me_t], sc_all.at[me_t]) for k in range(1, tps)
    ]
    relay((3, 2))
    arrived(3)
    for copy in scores:
        copy.wait()
    both = sc_all[0]
    for t in range(1, tps):
        both = both + sc_all[t]
    score = both[:, :1] / jnp.sqrt(both[:, HD - 1 :] / (width * tps) + 1e-06)
    total = score[:parts]
    for s in range(1, steps):
        total = total + score[s * parts : (s + 1) * parts]
    count = table.shape[0]
    deep = lax.broadcasted_iota(jnp.int32, (rows, parts), 0) % parts
    broad = lax.broadcasted_iota(jnp.int32, (rows, parts), 1)
    names = jnp.concatenate(
        [jnp.broadcast_to(tokens[s : s + 1, :], (parts, parts)) for s in range(steps)], 0
    )
    name = jnp.sum(jnp.where(deep == broad, names, 0).astype(f32), -1, keepdims=True)
    name = name.astype(jnp.int32)
    line = lax.broadcasted_iota(jnp.int32, (rows, count), 1)
    found = jnp.dot(
        (line == name // HD).astype(f32).astype(bf16), table[...], preferred_element_type=f32
    )
    gift = jnp.sum(jnp.where(lane == name % HD, found, 0.0), -1, keepdims=True)
    for s in range(steps):
        total = total + gift[s * parts : (s + 1) * parts]
    past = jnp.where(deep[:parts] == broad[:parts], prev[...], 0.0)
    total = total + jnp.sum(past, -1, keepdims=True)
    mine = jnp.broadcast_to(total, (parts, HD))
    lw_all[me_d] = mine
    lws = []
    for k in range(1, doms):
        copy = push(
            lw_all.at[me_d], lw_all.at[me_d], lw_send.at[k - 1], lw_recv.at[k - 1],
            (me_d + k) % doms, me_t,
        )
        copy.start()
        lws.append(copy)

    relay((3, 3))
    for copy in passed:
        copy.wait()
    index = lax.broadcasted_iota(jnp.int32, (doms * rows, HD), 0)
    pick = (index == tabv[3:4, :]).astype(f32).astype(bf16)
    chosen = lax.dot_general(
        pick, fresh_all[...].reshape(doms * rows, 2 * kvw),
        (((0,), (0,)), ((), ())), preferred_element_type=f32,
    ).astype(bf16)
    for i in range(parts):
        new_k[i, span:, :] = chosen[i * 8 : i * 8 + steps, :kvw]
        new_v[i, span:, :] = chosen[i * 8 : i * 8 + steps, kvw:]

    for copy in lws:
        copy.wait()
    largest = jnp.max(lw_all[...], (0, 1), keepdims=True)[0]
    mass = jnp.sum(jnp.exp(lw_all[...] - largest[None]), (0, 1), keepdims=True)[0]
    out_lw[...] = mine - (largest + jnp.log(mass))

    both_k.wait()
    both_v.wait()
    for k in (1, 2, 3):
        for which in range(2):
            light_mirror(k, which, 0).wait()

        @pl.when(rel != k)
        def _():
            for which in range(2):
                light_mirror(k, which, 1).wait()

    @pl.when(pos > 0)
    def _():
        for q in range(4):
            for which in range(2):
                mirror(q, which).wait()

    for i in range(parts):
        at = tab[1, i]
        new_k[i, :span, :] = all_k[at]
        new_v[i, :span, :] = all_v[at]

    @pl.when(pos < 3)
    def _():
        for q in range(4):
            for which in range(2):
                forward(q, which).wait_send()

    for k in (1, 2, 3):
        for which in range(2):
            light(k, which, 0).wait_send()

    @pl.when(pos > 0)
    def _():
        for k in (1, 2, 3):
            for which in range(2):
                light(k, which, 1).wait_send()

    for copy in news:
        copy.wait_send()


def adaptive(
    activations, norm_gain, w_query, w_key, value_weight, w_output, cache_keys, cache_values,
    tokens, twisting_table, twist_vec, previous_log_weights, copy_counts,
):
    f32, bf16 = jnp.float32, jnp.bfloat16
    steps, parts, width = activations.shape
    rows = steps * parts
    span = cache_keys.shape[1]
    kvw = w_key.shape[1]
    qw = w_query.shape[1]
    groups = kvw // HD
    pack = steps * (qw // kvw)
    doms = lax.axis_size("dom")
    tps = lax.axis_size("tp")
    middle = HD // 2
    cap = CAP
    angles = (span + np.arange(rows) // parts)[:, None] * (
        500000.0 ** (-2.0 * np.arange(middle) / HD)
    )
    cosine = np.concatenate([np.cos(angles)] * 2, 1).astype(np.float32)
    sine = np.concatenate([-np.sin(angles), np.sin(angles)], 1).astype(np.float32)
    vmem = pl.BlockSpec(memory_space=pltpu.VMEM)
    smem = pl.BlockSpec(memory_space=pltpu.SMEM)
    hbm = pl.BlockSpec(memory_space=pl.ANY)
    dma = pltpu.SemaphoreType.DMA
    both = jax.ShapeDtypeStruct((2 * parts, span, kvw), bf16)
    tab, chip_k, chip_v = pl.pallas_call(
        functools.partial(plan_kernel, parts, doms, cap, HOT_CAP, steps, rows),
        out_shape=(jax.ShapeDtypeStruct((8, HD), jnp.int32), both, both),
        in_specs=[vmem, hbm, hbm],
        out_specs=(vmem,) * 3,
        scratch_shapes=[
            pltpu.VMEM((doms, 8, HD), f32),
            dma((doms - 1,)), dma((doms - 1,)), dma((2,)), dma((2,)), dma((2,)),
        ],
        compiler_params=pltpu.CompilerParams(
            collective_id=5, has_side_effects=True, vmem_limit_bytes=16 << 20
        ),
        name="plan",
    )(copy_counts.reshape(1, parts), cache_keys, cache_values)

    def hot_branch(hot):
        result = jax.ShapeDtypeStruct((parts, span + steps, kvw), bf16)
        call = pl.pallas_call(
            functools.partial(main_kernel, steps, parts, doms, tps, cap, HOT_CAP, hot),
            out_shape=(
                jax.ShapeDtypeStruct((rows, width), bf16), result, result,
                jax.ShapeDtypeStruct((parts, HD), f32),
            ),
            in_specs=[hbm, vmem] + [hbm] * 4 + [vmem] * 8 + [smem, vmem],
            out_specs=(vmem,) * 4,
            scratch_shapes=[
                pltpu.VMEM((tps, rows, width), bf16),
                pltpu.VMEM(w_query.shape, bf16),
                pltpu.VMEM(w_key.shape, bf16),
                pltpu.VMEM(value_weight.shape, bf16),
                pltpu.VMEM(w_output.shape, bf16),
                pltpu.VMEM((3 * parts + 3 * cap, span, kvw), bf16),
                pltpu.VMEM((3 * parts + 3 * cap, span, kvw), bf16),
                pltpu.VMEM((3, cap // 2, span, kvw), bf16),
                pltpu.VMEM((3, cap // 2, span, kvw), bf16),
                pltpu.VMEM((groups, parts, pack, HD), f32),
                pltpu.VMEM((groups, parts, pack, HD), f32),
                pltpu.VMEM((groups, parts * pack, span), f32),
                pltpu.VMEM((rows, qw), bf16),
                pltpu.VMEM((doms, rows, 2 * kvw), bf16),
                pltpu.VMEM((tps - 1, rows, width), bf16),
                pltpu.VMEM((tps - 1, rows, width), bf16),
                pltpu.VMEM((tps, rows, HD), f32),
                pltpu.VMEM((doms, parts, HD), f32),
                dma((9,)),
                dma((3 * (tps - 1),)), dma((3 * (tps - 1),)),
                dma((doms - 1,)), dma((doms - 1,)),
                dma((16,)), dma((16,)),
                dma((24,)), dma((24,)),
                dma((7,)), dma((7,)),
            ],
            compiler_params=pltpu.CompilerParams(
                collective_id=hot, has_side_effects=True, vmem_limit_bytes=42 << 20
            ),
            name=f"main{hot}",
        )

        def run(
            act, gain, wq, wk, wv, wo, chip_k, chip_v, twist, tokens, table, prev, cosine,
            sine, tab, ck, cv, counts,
        ):
            return call(
                act, gain, wq, wk, wv, wo, chip_k, chip_v, twist, tokens, table, prev,
                cosine, sine, tab, tab,
            )

        return run

    def every(
        act, gain, wq, wk, wv, wo, chip_k, chip_v, twist, tokens, table, prev, cosine,
        sine, tab, ck, cv, counts,
    ):
        reward = jnp.sum(table.reshape(-1)[tokens].astype(f32), 0)
        aux = jnp.stack([prev[0] + reward, counts.astype(f32)], 1)
        return all_rows(
            steps, parts, act, gain, wq, wk, wv, wo, ck, cv, twist, aux, cosine, sine
        )

    attn, new_k, new_v, out_lw = lax.switch(
        tab[4, 0],
        [hot_branch(hot) for hot in range(4)] + [every],
        activations.reshape(rows, width), norm_gain.reshape(1, -1), w_query, w_key,
        value_weight, w_output, chip_k, chip_v, twist_vec.reshape(1, -1), tokens,
        twisting_table.reshape(-1, HD), previous_log_weights.reshape(1, parts),
        jnp.asarray(cosine), jnp.asarray(sine), tab, cache_keys, cache_values, copy_counts,
    )
    return attn.reshape(steps, parts, width), new_k, new_v, out_lw[:, 0]


def solution(mesh):
    body = adaptive if mesh.shape["dom"] == 8 else local
    return jax.shard_map(
        body,
        mesh=mesh,
        in_specs=(
            P(None, "dom", "tp"),
            P(),
            P(None, "tp"),
            P(None, "tp"),
            P(None, "tp"),
            P("tp", None),
            P("dom", None, "tp"),
            P("dom", None, "tp"),
            P(None, "dom"),
            P(),
            P("tp"),
            P("dom"),
            P("dom"),
        ),
        out_specs=(P(None, "dom", "tp"), P("dom", None, "tp"), P("dom", None, "tp"), P("dom")),
        check_vma=False,
    )
```

```python
import functools

import jax
import jax.numpy as jnp
import numpy as np
from jax import lax
from jax.experimental import pallas as pl
from jax.experimental.pallas import tpu as pltpu
from jax.sharding import PartitionSpec as P

D = 4096
HD = 128
CAP = 6
HOT_CAP = 4
EARLY = 1


def rotate(tensor, positions):
    middle = tensor.shape[-1] // 2
    frequency = 500000.0 ** (-2.0 * jnp.arange(middle, dtype=jnp.float32) / tensor.shape[-1])
    angles = positions[:, None] * frequency[None, :]
    cosine = jnp.cos(angles)[:, None, None, :]
    sine_part = jnp.sin(angles)[:, None, None, :]
    lower_half = tensor[..., :middle]
    upper_half = tensor[..., middle:]
    return jnp.concatenate(
        [
            lower_half * cosine - upper_half * sine_part,
            upper_half * cosine + lower_half * sine_part,
        ],
        -1,
    )


def local(
    activations,
    norm_gain,
    w_query,
    w_key,
    value_weight,
    w_output,
    cache_keys,
    cache_values,
    tokens,
    twisting_table,
    twist_vec,
    previous_log_weights,
    copy_counts,
):
    step_count = activations.shape[0]
    particle_count = activations.shape[1]
    span_old = cache_keys.shape[1]
    dom_size = lax.axis_size("dom")
    kv_local = w_key.shape[1] // HD
    q_local = w_query.shape[1] // HD
    group_size = q_local // kv_local
    all_counts = lax.all_gather(copy_counts, "dom", axis=0, tiled=True)
    copy_ends = jnp.cumsum(all_counts)
    ranks = jnp.arange(particle_count, dtype=jnp.int32) * dom_size + lax.axis_index("dom")
    ancestor = jnp.sum((copy_ends[None, :] <= ranks[:, None]).astype(jnp.int32), 1)
    all_keys = lax.all_gather(cache_keys, "dom", axis=0, tiled=True)
    all_values = lax.all_gather(cache_values, "dom", axis=0, tiled=True)

    gathered = lax.all_gather(activations, "tp", axis=2, tiled=True)
    inputs = gathered.astype(jnp.float32)
    normed = (
        inputs * lax.rsqrt(jnp.mean(inputs * inputs, -1, keepdims=True) + 1e-05) * norm_gain
    ).astype(jnp.bfloat16)
    flat_rows = normed.reshape(step_count * particle_count, D)
    positions = (span_old + jnp.arange(step_count, dtype=jnp.int32)).astype(jnp.float32)
    queries = jnp.dot(flat_rows, w_query, preferred_element_type=jnp.float32).reshape(
        step_count, particle_count, q_local, HD
    )
    queries = rotate(queries, positions).astype(jnp.bfloat16)
    fresh_keys = jnp.dot(flat_rows, w_key, preferred_element_type=jnp.float32).reshape(
        step_count, particle_count, kv_local, HD
    )
    fresh_keys = (
        rotate(fresh_keys, positions)
        .astype(jnp.bfloat16)
        .reshape(step_count, particle_count, kv_local * HD)
    )
    fresh_values = jnp.dot(flat_rows, value_weight, preferred_element_type=jnp.float32).astype(
        jnp.bfloat16
    )
    fresh_values = fresh_values.reshape(step_count, particle_count, kv_local * HD)
    fresh_keys = jnp.transpose(fresh_keys, (1, 0, 2))
    fresh_values = jnp.transpose(fresh_values, (1, 0, 2))
    key_rows = jnp.concatenate([cache_keys, fresh_keys], 1)
    value_rows = jnp.concatenate([cache_values, fresh_values], 1)
    key_span = span_old + step_count
    query_heads = queries.reshape(step_count, particle_count, kv_local, group_size, HD)
    key_heads = key_rows.reshape(particle_count, key_span, kv_local, HD)
    value_heads = value_rows.reshape(particle_count, key_span, kv_local, HD)
    scores = (
        jnp.einsum("snkgd,nlkd->snkgl", query_heads, key_heads, preferred_element_type=jnp.float32)
        / HD**0.5
    )
    allowed = (
        jnp.arange(key_span, dtype=jnp.int32)[None, :]
        <= (span_old + jnp.arange(step_count, dtype=jnp.int32))[:, None]
    )
    allowed = allowed[:, None, None, None, :]
    masked = jnp.where(allowed, scores, -jnp.inf)
    highest = jnp.max(masked, -1, keepdims=True)
    exponent = jnp.exp(masked - highest)
    weights = (exponent / jnp.sum(exponent, -1, keepdims=True)).astype(jnp.bfloat16)
    context = jnp.einsum(
        "snkgl,nlkd->snkgd", weights, value_heads, preferred_element_type=jnp.float32
    ).astype(jnp.bfloat16)
    context = context.reshape(step_count * particle_count, q_local * HD)
    partial_value = jnp.dot(context, w_output, preferred_element_type=jnp.float32).reshape(
        step_count, particle_count, D
    )
    head_mix = lax.psum_scatter(partial_value, "tp", scatter_dimension=2, tiled=True)
    attn_out = head_mix.astype(jnp.bfloat16)
    summed = activations.astype(jnp.float32) + head_mix
    aligned, energy = lax.psum(
        (jnp.sum(summed * twist_vec, -1), jnp.sum(summed * summed, -1)), "tp"
    )
    twisting_score = aligned / jnp.sqrt(energy / D + 1e-06)
    token_reward = twisting_table[tokens].astype(jnp.float32)
    particle_log_weight = previous_log_weights + jnp.sum(token_reward + twisting_score, 0)
    largest = lax.pmax(jnp.max(particle_log_weight), "dom")
    mass_total = lax.psum(jnp.sum(jnp.exp(particle_log_weight - largest)), "dom")
    out_logw = particle_log_weight - (largest + jnp.log(mass_total))
    fresh = lax.all_gather(
        jnp.concatenate([fresh_keys, fresh_values], 2), "dom", axis=0, tiled=True
    )[ancestor]
    width = fresh_keys.shape[2]
    new_keys = jnp.concatenate([all_keys[ancestor], fresh[..., :width]], 1)
    new_values = jnp.concatenate([all_values[ancestor], fresh[..., width:]], 1)
    return (attn_out, new_keys, new_values, out_logw)


MESH = pl.DeviceIdType.MESH


def layer_kernel(
    steps, parts, doms, tps,
    act, gain, wq, wk, wv, wo, ck, cv, twist, aux, cosine, sine,
    attn_out, all_k, all_v, fresh_sel, out_lw, anc_out,
    act_all, wq_v, wk_v, wv_v, wo_v, ck_v, cv_v, qs, cx, sc1, ctx_b, fresh, fresh_all,
    rs_send, rs_recv, sc_all, lw_all, cnt_all,
    loc, tp_send, tp_recv, dom_send, dom_recv, blk_send, blk_recv,
):
    f32, bf16 = jnp.float32, jnp.bfloat16
    me_d = lax.axis_index("dom")
    me_t = lax.axis_index("tp")
    rows, width = act.shape
    half = parts // 2
    kvw = wk.shape[1]
    groups = kvw // HD
    per = wq.shape[1] // kvw
    pack = steps * per
    c = me_d % 2
    x = (me_d // 2) % 2
    y = me_d // 4
    sib = me_d + 1 - 2 * c
    xn = me_d + 2 - 4 * x
    yn = me_d + 4 - 8 * y
    dn = xn + 4 - 8 * y

    barrier = pltpu.get_barrier_semaphore()
    for k in range(1, tps):
        pl.semaphore_signal(
            barrier, inc=1, device_id=(me_d, (me_t + k) % tps), device_id_type=MESH
        )
    for k in range(1, doms):
        pl.semaphore_signal(
            barrier, inc=1, device_id=((me_d + k) % doms, me_t), device_id_type=MESH
        )

    def fetch(i, src, dst):
        copy = pltpu.make_async_copy(src, dst, loc.at[i])
        copy.start()
        return copy

    own_act = fetch(0, act, act_all.at[me_t])
    load_q = fetch(1, wq, wq_v)
    load_k = fetch(2, wk, wk_v)
    load_v = fetch(3, wv, wv_v)
    load_ck = fetch(4, ck, ck_v)
    load_cv = fetch(5, cv, cv_v)
    load_o = fetch(6, wo, wo_v)

    cnt_all[me_d] = jnp.broadcast_to(aux[:, 1:], cnt_all.shape[1:])
    pl.semaphore_wait(barrier, tps + doms - 2)

    def tp_push(base, k, src, dst):
        copy = pltpu.make_async_remote_copy(
            src_ref=src, dst_ref=dst, send_sem=tp_send.at[base + k - 1],
            recv_sem=tp_recv.at[base + k - 1],
            device_id=(me_d, (me_t + k) % tps), device_id_type=MESH,
        )
        copy.start()
        return copy

    def dom_push(base, k, src, dst):
        copy = pltpu.make_async_remote_copy(
            src_ref=src, dst_ref=dst, send_sem=dom_send.at[base + k - 1],
            recv_sem=dom_recv.at[base + k - 1],
            device_id=((me_d + k) % doms, me_t), device_id_type=MESH,
        )
        copy.start()
        return copy

    acts = [tp_push(0, k, act, act_all.at[me_t]) for k in range(1, tps)]

    def piece(kind, to, which, h, slot, own):
        dst = (all_k, all_v)[which].at[slot, pl.ds(h * half, half)]
        src = (ck, cv)[which].at[pl.ds(h * half, half)] if own else dst
        i = kind * 4 + h * 2 + which
        copy = pltpu.make_async_remote_copy(
            src_ref=src, dst_ref=dst, send_sem=blk_send.at[i], recv_sem=blk_recv.at[i],
            device_id=(to, me_t), device_id_type=MESH,
        )
        copy.start()
        return copy

    moves = {}
    for h, kind, to in ((0, 0, xn), (1, 1, yn), (1, 0, xn), (0, 1, yn)):
        for which in range(2):
            moves[kind, h, which] = piece(kind, to, which, h, me_d, True)
    cnts = [dom_push(0, k, cnt_all.at[me_d], cnt_all.at[me_d]) for k in range(1, doms)]
    for h in range(2):
        for which in range(2):
            moves[3, h, which] = piece(3, sib, which, h, me_d, True)

    own_act.wait()
    for copy in acts:
        copy.wait()
    square = jnp.zeros((rows, 1), f32)
    for t in range(tps):
        u = act_all[t].astype(f32)
        square = square + jnp.sum(u * u, -1, keepdims=True)
    inv = lax.rsqrt(square / (width * tps) + 1e-05)
    normed = []
    for t in range(tps):
        u = act_all[t].astype(f32)
        normed.append((u * inv * gain[:, t * width : (t + 1) * width]).astype(bf16))

    def project(w):
        total = None
        for t in range(tps):
            part = jnp.dot(
                normed[t], w[t * width : (t + 1) * width, :], preferred_element_type=f32
            )
            total = part if total is None else total + part
        return total

    cos_t, sin_t = cosine[...], sine[...]

    def turn(u):
        return u * cos_t + pltpu.roll(u, HD // 2, 1) * sin_t

    load_k.wait()
    load_v.wait()
    keys = project(wk_v)
    for g in range(groups):
        fresh[:, g * HD : (g + 1) * HD] = turn(keys[:, g * HD : (g + 1) * HD]).astype(bf16)
    fresh[:, kvw:] = project(wv_v).astype(bf16)
    fresh_all[me_d] = fresh[...]
    news = [dom_push(doms - 1, k, fresh, fresh_all.at[me_d]) for k in range(1, doms)]
    load_q.wait()
    query = project(wq_v)
    for h in range(groups * per):
        g, j = h // per, h % per
        turned = turn(query[:, h * HD : (h + 1) * HD])
        for s in range(steps):
            qs[g, :, s * per + j, :] = turned[s * parts : (s + 1) * parts]
    load_ck.wait()
    load_cv.wait()
    put_k = fetch(7, ck_v, all_k.at[me_d])
    put_v = fetch(8, cv_v, all_v.at[me_d])

    lines = parts * pack
    row = lax.broadcasted_iota(jnp.int32, (lines, rows), 0)
    col = lax.broadcasted_iota(jnp.int32, (lines, rows), 1)
    allowed = (row // pack == col % parts) & (col // parts <= (row % pack) // per)
    scale = HD**0.5
    for g in range(groups):
        lanes = slice(g * HD, (g + 1) * HD)
        qg = qs[g].reshape(lines, HD).astype(bf16)
        for n in range(parts):
            sc1[g, n * pack : (n + 1) * pack, :] = lax.dot_general(
                qg[n * pack : (n + 1) * pack], ck_v[n, :, lanes],
                (((1,), (1,)), ((), ())), preferred_element_type=f32,
            )
        near = lax.dot_general(
            qg, fresh[:, lanes], (((1,), (1,)), ((), ())), preferred_element_type=f32
        )
        near = jnp.where(allowed, near / scale, -jnp.inf)
        far = sc1[g] / scale
        top = jnp.maximum(
            jnp.max(far, -1, keepdims=True), jnp.max(near, -1, keepdims=True)
        )
        far = jnp.exp(far - top)
        near = jnp.exp(near - top)
        mass = jnp.sum(far, -1, keepdims=True) + jnp.sum(near, -1, keepdims=True)
        far = (far / mass).astype(bf16)
        near = (near / mass).astype(bf16)
        extra = jnp.dot(
            near, fresh[:, kvw + g * HD : kvw + (g + 1) * HD], preferred_element_type=f32
        )
        for n in range(parts):
            span = slice(n * pack, (n + 1) * pack)
            cx[g, n] = extra[span] + jnp.dot(
                far[span], cv_v[n, :, lanes], preferred_element_type=f32
            )
    for h in range(groups * per):
        g, j = h // per, h % per
        for s in range(steps):
            ctx_b[s * parts : (s + 1) * parts, h * HD : (h + 1) * HD] = cx[
                g, :, s * per + j, :
            ].astype(bf16)
    load_o.wait()

    def mix(p):
        return jnp.dot(
            ctx_b[...], wo_v[:, pl.ds(pl.multiple_of(p * width, HD), width)],
            preferred_element_type=f32,
        )

    sums = []
    for k in range(1, tps):
        rs_send[k - 1] = mix((me_t + k) % tps)
        sums.append(tp_push(tps - 1, k, rs_send.at[k - 1], rs_recv.at[k - 1]))
    head = mix(me_t)

    def done(kind, h):
        for which in range(2):
            moves[kind, h, which].wait_recv()

    def relay(kind, to, h, slot):
        for which in range(2):
            moves[kind, h, which] = piece(kind, to, which, h, slot, False)

    done(0, 0)
    relay(2, yn, 0, xn)
    relay(4, sib, 0, xn)
    done(1, 1)
    relay(6, xn, 1, yn)
    relay(5, sib, 1, yn)
    for k in range(1, tps):
        sums[k - 1].wait()
        head = head + rs_recv[k - 1]
    attn_out[...] = head.astype(bf16)
    summed = act_all[me_t].astype(f32) + head
    along = jnp.sum(summed * twist[...], -1, keepdims=True)
    energy = jnp.sum(summed * summed, -1, keepdims=True)
    lane = lax.broadcasted_iota(jnp.int32, (rows, HD), 1)
    sc_all[me_t] = jnp.where(lane < HD // 2, along, energy)
    scores = [
        tp_push(2 * (tps - 1), k, sc_all.at[me_t], sc_all.at[me_t]) for k in range(1, tps)
    ]
    for copy in scores:
        copy.wait()
    both = sc_all[0]
    for t in range(1, tps):
        both = both + sc_all[t]
    score = both[:, :1] / jnp.sqrt(both[:, HD - 1 :] / (width * tps) + 1e-06)
    total = score[:parts]
    for s in range(1, steps):
        total = total + score[s * parts : (s + 1) * parts]
    mine = jnp.broadcast_to(aux[:, :1] + total, (parts, HD))
    lw_all[me_d] = mine
    lws = [
        dom_push(2 * (doms - 1), k, lw_all.at[me_d], lw_all.at[me_d]) for k in range(1, doms)
    ]

    done(0, 1)
    relay(4, sib, 1, xn)
    done(1, 0)
    relay(5, sib, 0, yn)

    for copy in cnts:
        copy.wait()
    for copy in news:
        copy.wait()
    whole = parts * doms
    number = cnt_all[...].reshape(whole, HD).astype(bf16)
    lower = lax.broadcasted_iota(jnp.int32, (whole, whole), 0)
    upper = lax.broadcasted_iota(jnp.int32, (whole, whole), 1)
    ends = jnp.dot(
        (upper <= lower).astype(f32).astype(bf16), number, preferred_element_type=f32
    )
    slot = lax.broadcasted_iota(jnp.int32, (whole, HD), 1)

    def ancestor(place):
        rank = (place * doms + me_d).astype(f32)
        return jnp.sum((ends <= rank).astype(f32), 0, keepdims=True).astype(jnp.int32)

    anc_out[...] = jnp.broadcast_to(ancestor(slot), anc_out.shape)
    lanes = lax.broadcasted_iota(jnp.int32, (1, HD), 1)
    wide = ancestor(slot // 8)
    target = (wide // parts) * rows + (lanes % 8) * parts + wide % parts
    target = jnp.where(lanes % 8 < steps, target, -1)
    index = lax.broadcasted_iota(jnp.int32, (doms * rows, HD), 0)
    pick = (index == target).astype(f32).astype(bf16)
    fresh_sel[...] = lax.dot_general(
        pick, fresh_all[...].reshape(doms * rows, 2 * kvw),
        (((0,), (0,)), ((), ())), preferred_element_type=f32,
    ).astype(bf16)

    for copy in lws:
        copy.wait()
    largest = jnp.max(lw_all[...], (0, 1), keepdims=True)[0]
    mass = jnp.sum(jnp.exp(lw_all[...] - largest[None]), (0, 1), keepdims=True)[0]
    out_lw[...] = mine - (largest + jnp.log(mass))

    done(2, 0)
    relay_d0 = [piece(7, sib, which, 0, dn, False) for which in range(2)]
    done(6, 1)
    relay_d1 = [piece(7, sib, which, 1, dn, False) for which in range(2)]
    for kind in (3, 4, 5):
        for h in range(2):
            done(kind, h)
    for copy in moves.values():
        copy.wait_send()
    for copy in relay_d0 + relay_d1:
        copy.wait()
    put_k.wait()
    put_v.wait()


def select_kernel(parts, steps, anc, fresh_sel, all_k, all_v, new_k, new_v, sem):
    span = all_k.shape[2]
    width = all_k.shape[3]
    copies = []
    for i in range(parts):
        a = anc[0, i]
        d, n = a // parts, a % parts
        for which, (src, dst) in enumerate(((all_k, new_k), (all_v, new_v))):
            copy = pltpu.make_async_copy(
                src.at[d, n], dst.at[i, pl.ds(0, span)], sem.at[2 * i + which]
            )
            copy.start()
            copies.append(copy)
    for i in range(parts):
        new_k[i, span:, :] = fresh_sel[i * 8 : i * 8 + steps, :width]
        new_v[i, span:, :] = fresh_sel[i * 8 : i * 8 + steps, width:]
    for copy in copies:
        copy.wait()


def all_rows(
    steps, parts, act, gain, wq, wk, wv, wo, ck, cv, twist, aux, cosine, sine,
):
    f32, bf16 = jnp.float32, jnp.bfloat16
    rows, width = act.shape
    span = ck.shape[1]
    kvw = wk.shape[1]
    qw = wq.shape[1]
    groups = kvw // HD
    pack = steps * (qw // kvw)
    doms = lax.axis_size("dom")
    tps = lax.axis_size("tp")
    vmem = pl.BlockSpec(memory_space=pltpu.VMEM)
    hbm = pl.BlockSpec(memory_space=pl.ANY)
    block = jax.ShapeDtypeStruct((doms,) + ck.shape, bf16)
    attn, all_k, all_v, fresh_sel, out_lw, anc = pl.pallas_call(
        functools.partial(layer_kernel, steps, parts, doms, tps),
        out_shape=(
            jax.ShapeDtypeStruct((rows, width), bf16), block, block,
            jax.ShapeDtypeStruct((HD, 2 * kvw), bf16),
            jax.ShapeDtypeStruct((parts, HD), f32),
            jax.ShapeDtypeStruct((8, HD), jnp.int32),
        ),
        in_specs=[hbm, vmem] + [hbm] * 6 + [vmem] * 4,
        out_specs=(vmem, hbm, hbm, vmem, vmem, vmem),
        scratch_shapes=[
            pltpu.VMEM((tps, rows, width), bf16),
            pltpu.VMEM(wq.shape, bf16),
            pltpu.VMEM(wk.shape, bf16),
            pltpu.VMEM(wv.shape, bf16),
            pltpu.VMEM(wo.shape, bf16),
            pltpu.VMEM(ck.shape, bf16),
            pltpu.VMEM(cv.shape, bf16),
            pltpu.VMEM((groups, parts, pack, HD), f32),
            pltpu.VMEM((groups, parts, pack, HD), f32),
            pltpu.VMEM((groups, parts * pack, span), f32),
            pltpu.VMEM((rows, qw), bf16),
            pltpu.VMEM((rows, 2 * kvw), bf16),
            pltpu.VMEM((doms, rows, 2 * kvw), bf16),
            pltpu.VMEM((tps - 1, rows, width), f32),
            pltpu.VMEM((tps - 1, rows, width), f32),
            pltpu.VMEM((tps, rows, HD), f32),
            pltpu.VMEM((doms, parts, HD), f32),
            pltpu.VMEM((doms, parts, HD), f32),
            pltpu.SemaphoreType.DMA((9,)),
            pltpu.SemaphoreType.DMA((3 * (tps - 1),)),
            pltpu.SemaphoreType.DMA((3 * (tps - 1),)),
            pltpu.SemaphoreType.DMA((3 * (doms - 1),)),
            pltpu.SemaphoreType.DMA((3 * (doms - 1),)),
            pltpu.SemaphoreType.DMA((32,)),
            pltpu.SemaphoreType.DMA((32,)),
        ],
        compiler_params=pltpu.CompilerParams(
            collective_id=4, has_side_effects=True, vmem_limit_bytes=52 << 20
        ),
        name="layer",
    )(act, gain, wq, wk, wv, wo, ck, cv, twist, aux, cosine, sine)
    result = jax.ShapeDtypeStruct((parts, span + steps, kvw), bf16)
    new_k, new_v = pl.pallas_call(
        functools.partial(select_kernel, parts, steps),
        out_shape=(result, result),
        in_specs=[pl.BlockSpec(memory_space=pltpu.SMEM), vmem, hbm, hbm],
        out_specs=(vmem, vmem),
        scratch_shapes=[pltpu.SemaphoreType.DMA((2 * parts,))],
        compiler_params=pltpu.CompilerParams(vmem_limit_bytes=8 << 20),
        name="select",
    )(anc, fresh_sel, all_k, all_v)
    return attn, new_k, new_v, out_lw


def plan_kernel(
    parts, doms, tps, cap, hot_cap, steps, rows,
    cnt, act, ck, cv, tab, chip_k, chip_v, act_part,
    cnt_all, send, recv, loc, sib_send, sib_recv, tp_send, tp_recv,
):
    f32, bf16, i32 = jnp.float32, jnp.bfloat16, jnp.int32
    me_d = lax.axis_index("dom")
    me_t = lax.axis_index("tp")
    core = me_d % 2
    x = (me_d // 2) % 2
    y = me_d // 4
    chip = me_d // 2
    barrier = pltpu.get_barrier_semaphore()
    for k in range(1, tps):
        pl.semaphore_signal(
            barrier, inc=1, device_id=(me_d, (me_t + k) % tps), device_id_type=MESH
        )
    for k in range(1, doms):
        pl.semaphore_signal(
            barrier, inc=1, device_id=((me_d + k) % doms, me_t), device_id_type=MESH
        )
    owns = []
    for i, (src, dst) in enumerate(((ck, chip_k), (cv, chip_v))):
        copy = pltpu.make_async_copy(src, dst.at[pl.ds(0, parts)], loc.at[i])
        copy.start()
        owns.append(copy)
    early = act.at[pl.ds(0, act_part.shape[1])]
    copy = pltpu.make_async_copy(early, act_part.at[me_t], loc.at[2])
    copy.start()
    owns.append(copy)
    cnt_all[me_d] = jnp.zeros(cnt_all.shape[1:], f32)
    cnt_all[me_d, :, :parts] = jnp.broadcast_to(cnt[...].astype(f32), (8, parts))
    pl.semaphore_wait(barrier, tps + doms - 2)
    copies = []
    for k in range(1, doms):
        copy = pltpu.make_async_remote_copy(
            src_ref=cnt_all.at[me_d], dst_ref=cnt_all.at[me_d],
            send_sem=send.at[k - 1], recv_sem=recv.at[k - 1],
            device_id=((me_d + k) % doms, me_t), device_id_type=MESH,
        )
        copy.start()
        copies.append(copy)
    swaps = []
    for k in range(1, tps):
        copy = pltpu.make_async_remote_copy(
            src_ref=early, dst_ref=act_part.at[me_t],
            send_sem=tp_send.at[k - 1], recv_sem=tp_recv.at[k - 1],
            device_id=(me_d, (me_t + k) % tps), device_id_type=MESH,
        )
        copy.start()
        swaps.append(copy)
    for i, (src, dst) in enumerate(((ck, chip_k), (cv, chip_v))):
        copy = pltpu.make_async_remote_copy(
            src_ref=src, dst_ref=dst.at[pl.ds(parts, parts)],
            send_sem=sib_send.at[i], recv_sem=sib_recv.at[i],
            device_id=(me_d + 1 - 2 * core, me_t), device_id_type=MESH,
        )
        copy.start()
        swaps.append(copy)
    for copy in copies:
        copy.wait()
    whole = parts * doms
    j = lax.broadcasted_iota(i32, (whole, HD), 0)
    lane = lax.broadcasted_iota(i32, (whole, HD), 1)
    spread = jnp.concatenate([cnt_all[d] for d in range(doms) for _ in range(parts // 8)], 0)
    column = jnp.sum(jnp.where(lane == j % parts, spread, 0.0), -1, keepdims=True)
    number = jnp.broadcast_to(column, (whole, HD))
    first = lax.broadcasted_iota(i32, (whole, whole), 0)
    second = lax.broadcasted_iota(i32, (whole, whole), 1)

    def total(mask, values):
        return jnp.dot(
            mask.astype(f32).astype(bf16), values.astype(bf16), preferred_element_type=f32
        )

    ends = total(second <= first, number)
    loads = total(second // parts == first // parts, number)
    number = number.astype(i32)
    ends = ends.astype(i32)
    starts = ends - number
    top = jnp.max(loads, (0, 1), keepdims=True)
    owner = j // parts
    heavy = jnp.min(jnp.where(loads == top, owner, doms).astype(f32), (0, 1), keepdims=True)
    heavy = heavy.astype(i32)
    light = owner != heavy
    home = j // (2 * parts)

    def needs(to):
        hit = None
        for m in range(4):
            one = (m < number) & (((starts + m) % doms) // 2 == to)
            hit = one if hit is None else hit | one
        return hit & light & (home != to)

    kind = (lane // cap) % 4
    there_x = x + kind % 2 - 2 * x * (kind % 2)
    there_y = y + kind // 2 - 2 * y * (kind // 2)
    need_send = needs(2 * there_y + there_x)
    need_here = needs(jnp.broadcast_to(chip, (whole, HD)))
    need_any = needs(lane % 4)
    before = (second < first) & (second // (2 * parts) == first // (2 * parts))
    places = total(
        before,
        jnp.concatenate([u.astype(f32) for u in (need_send, need_here, need_any)], 1),
    ).astype(i32)
    place_send = places[:, :HD]
    place_here = places[:, HD : 2 * HD]
    place_any = places[:, 2 * HD :]
    local_row = j % parts + parts * (owner % 2 + core - 2 * core * (owner % 2))
    half = cap // 2
    entry = lane % cap
    picked = need_send & (place_send == 2 * (entry % half) + entry // half) & (home == chip)
    sources = jnp.sum(jnp.where(picked, local_row, 0).astype(f32), 0, keepdims=True)
    hx, hy = home % 2, home // 2
    away = (hx + x - 2 * x * hx) + 2 * (hy + y - 2 * y * hy)
    value = jnp.where(
        away == 0,
        local_row,
        jnp.where(
            light,
            3 * parts + (away - 1) * cap + place_here % 2 * half + place_here // 2,
            2 * parts + j % parts,
        ),
    )
    rank = lane * doms + me_d
    mine = (starts <= rank) & (rank < ends)
    index = jnp.sum(jnp.where(mine, value, 0).astype(f32), 0, keepdims=True)
    wide = (lane // 8) * doms + me_d
    old = jnp.sum((ends <= wide).astype(f32), 0, keepdims=True).astype(i32)
    row = lax.broadcasted_iota(i32, (1, HD), 1)
    target = (old // parts) * rows + (row % 8) * parts + old % parts
    target = jnp.where(row % 8 < steps, target, -1)
    room = jnp.where(home == heavy // 2, hot_cap, cap)
    over = jnp.max(
        (need_any & (place_any >= room)).astype(f32), (0, 1), keepdims=True
    ).astype(i32)
    base = parts * (heavy % 2 + core - 2 * core * (heavy % 2))
    branch = jnp.where(over == 0, heavy // 2, 4)
    tab[0:1, :] = sources.astype(i32)
    tab[1:2, :] = index.astype(i32)
    tab[2:3, :] = jnp.broadcast_to(base, (1, HD))
    tab[3:4, :] = target
    tab[4:5, :] = jnp.broadcast_to(branch, (1, HD))
    tab[5:8, :] = jnp.zeros((3, HD), i32)
    for copy in owns + swaps:
        copy.wait()


def main_kernel(
    steps, parts, doms, tps, cap, hot_cap, hot,
    act, act_part, gain, wq, wk, wv, wo, chip_k, chip_v, twist, tokens, table, prev,
    cosine, sine, tab, tabv,
    attn_out, new_k, new_v, out_lw,
    act_all, wq_v, wk_v, wv_v, wo_v, all_k, all_v, send_k, send_v,
    qs, cx, sc1, ctx_b, fresh_all, rs_send, rs_recv, sc_all, lw_all,
    loc, tp_send, tp_recv, lw_send, lw_recv,
    hv_send, hv_recv, li_send, li_recv, fr_send, fr_recv,
):
    f32, bf16 = jnp.float32, jnp.bfloat16
    me_d = lax.axis_index("dom")
    me_t = lax.axis_index("tp")
    rows, width = act.shape
    kvw = wk.shape[1]
    groups = kvw // HD
    per = wq.shape[1] // kvw
    pack = steps * per
    span = chip_k.shape[1]
    c = me_d % 2
    x = (me_d // 2) % 2
    y = me_d // 4
    sib = me_d + 1 - 2 * c
    xn = me_d + 2 - 4 * x
    yn = me_d + 4 - 8 * y
    dn = xn + 4 - 8 * y
    rx = x if hot % 2 == 0 else 1 - x
    ry = y if hot // 2 == 0 else 1 - y
    pos = (1 - c) * (3 * ry + rx * (1 - 2 * ry)) + c * (3 * rx + ry * (1 - 2 * rx))
    turn_y = (pos + c) % 2
    onward = xn + turn_y * (yn - xn)

    barrier = pltpu.get_barrier_semaphore()
    for k in range(1, tps):
        pl.semaphore_signal(
            barrier, inc=1, device_id=(me_d, (me_t + k) % tps), device_id_type=MESH
        )
    for k in range(1, doms):
        pl.semaphore_signal(
            barrier, inc=1, device_id=((me_d + k) % doms, me_t), device_id_type=MESH
        )

    def fetch(i, src, dst):
        copy = pltpu.make_async_copy(src, dst, loc.at[i])
        copy.start()
        return copy

    first = act_part.shape[1]
    later = act.at[pl.ds(first, rows - first)]
    own_act = fetch(0, later, act_all.at[me_t])
    load_k = fetch(2, wk, wk_v)
    load_v = fetch(3, wv, wv_v)
    load_q = fetch(1, wq, wq_v)
    load_o = fetch(6, wo, wo_v)
    pl.semaphore_wait(barrier, tps + doms - 2)

    def push(src, dst, ssem, rsem, to_d, to_t):
        return pltpu.make_async_remote_copy(
            src_ref=src, dst_ref=dst, send_sem=ssem, recv_sem=rsem,
            device_id=(to_d, to_t), device_id_type=MESH,
        )

    def tp_push(base, k, src, dst):
        copy = push(
            src, dst, tp_send.at[base + k - 1], tp_recv.at[base + k - 1],
            me_d, (me_t + k) % tps,
        )
        copy.start()
        return copy

    acts = [tp_push(0, k, later, act_all.at[me_t]) for k in range(1, tps)]
    lane_rows = cap // 2
    hot_lane = hot_cap // 2
    rel = rx + 2 * ry
    hot_rows = parts // 2
    chunk = hot_rows // 4

    def hot_copy(q, which, to, base):
        ref = (all_k, all_v)[which]
        area = ref.at[pl.ds(2 * parts + hot_rows * c + q * chunk, chunk)]
        i = base + q * 2 + which
        return push(area, area, hv_send.at[i], hv_recv.at[i], to, me_t)

    def forward(q, which):
        return hot_copy(q, which, onward, 0)

    def mirror(q, which):
        return hot_copy(q, which, sib, 8)

    def light_part(ref, base, piece):
        if piece == 0:
            return ref.at[pl.ds(base, hot_lane)]
        return ref.at[pl.ds(base + hot_lane, lane_rows - hot_lane)]

    def light_area(which, k, piece):
        base = 3 * parts + (k - 1) * cap + lane_rows * c
        return light_part((all_k, all_v)[which], base, piece)

    def light(k, which, piece):
        i = ((k - 1) * 2 + which) * 2 + piece
        return push(
            light_part((send_k, send_v)[which].at[k - 1], 0, piece),
            light_area(which, k, piece),
            li_send.at[i], li_recv.at[i], (xn, yn, dn)[k - 1], me_t,
        )

    def light_mirror(k, which, piece):
        i = 12 + ((k - 1) * 2 + which) * 2 + piece
        area = light_area(which, k, piece)
        return push(area, area, li_send.at[i], li_recv.at[i], sib, me_t)

    def send_lights(when, kinds, pieces):
        @pl.when(when)
        def _():
            for k in kinds:
                for piece in range(pieces):
                    for which in range(2):
                        light(k, which, piece).start()

    def arrived(k):
        for which in range(2):
            light(k, which, 0).wait_recv()
            light_mirror(k, which, 0).start()

        @pl.when(rel != k)
        def _():
            for which in range(2):
                light(k, which, 1).wait_recv()
                light_mirror(k, which, 1).start()

    @pl.when(pos == 0)
    def _():
        for i in range(hot_rows):
            at = tab[2, 0] + hot_rows * c + i
            all_k[2 * parts + hot_rows * c + i] = chip_k[at]
            all_v[2 * parts + hot_rows * c + i] = chip_v[at]
            if i % chunk == chunk - 1:
                for which in range(2):
                    forward(i // chunk, which).start()

    for k in (2, 1, 3):
        for t in range(lane_rows):
            at = tab[0, k * cap + lane_rows * c + t]
            send_k[k - 1, t] = chip_k[at]
            send_v[k - 1, t] = chip_v[at]
    send_lights((pos == 1) & (rel == 1), (1,), 2)
    send_lights((pos == 1) & (rel == 2), (2,), 2)
    send_lights((pos == 3) & (rel == 1), (2, 1), 2)
    send_lights((pos == 3) & (rel == 2), (1, 2), 2)
    send_lights(pos == 2, (3, 2, 1), 2)
    send_lights((pos == 0) & (c == 0), (3, 1), 1)
    send_lights((pos == 0) & (c == 1), (2,), 1)
    both_k = fetch(7, chip_k, all_k.at[pl.ds(0, 2 * parts)])
    both_v = fetch(8, chip_v, all_v.at[pl.ds(0, 2 * parts)])

    def relay(*list_of):
        for where, q in list_of:

            @pl.when(pos == where)
            def _():
                for which in range(2):
                    forward(q, which).wait_recv()
                    if where < 3:
                        forward(q, which).start()
                    mirror(q, which).start()

    relay((1, 0))
    relay((1, 1))
    own_act.wait()
    for copy in acts:
        copy.wait()

    def features(t):
        return jnp.concatenate([act_part[t], act_all[t]], 0).astype(f32)

    square = jnp.zeros((rows, 1), f32)
    for t in range(tps):
        u = features(t)
        square = square + jnp.sum(u * u, -1, keepdims=True)
    inv = lax.rsqrt(square / (width * tps) + 1e-05)
    normed = []
    for t in range(tps):
        u = features(t)
        normed.append((u * inv * gain[:, t * width : (t + 1) * width]).astype(bf16))

    def project(w):
        total = None
        for t in range(tps):
            part = jnp.dot(
                normed[t], w[t * width : (t + 1) * width, :], preferred_element_type=f32
            )
            total = part if total is None else total + part
        return total

    cos_t, sin_t = cosine[...], sine[...]

    def turn(u):
        return u * cos_t + pltpu.roll(u, HD // 2, 1) * sin_t

    load_k.wait()
    load_v.wait()
    keys = project(wk_v)
    fresh = fresh_all.at[me_d]
    for g in range(groups):
        fresh[:, g * HD : (g + 1) * HD] = turn(keys[:, g * HD : (g + 1) * HD]).astype(bf16)
    fresh[:, kvw:] = project(wv_v).astype(bf16)

    def fresh_copy(i, block, to):
        area = fresh_all.at[block]
        return push(area, area, fr_send.at[i], fr_recv.at[i], to, me_t)

    news = [fresh_copy(i, me_d, to) for i, to in enumerate((dn, xn, yn, sib))]
    for copy in news:
        copy.start()
    load_q.wait()
    query = project(wq_v)
    for h in range(groups * per):
        g, j = h // per, h % per
        turned = turn(query[:, h * HD : (h + 1) * HD])
        for s in range(steps):
            qs[g, :, s * per + j, :] = turned[s * parts : (s + 1) * parts]
    relay((1, 2), (2, 0))

    lines = parts * pack
    row = lax.broadcasted_iota(jnp.int32, (lines, rows), 0)
    col = lax.broadcasted_iota(jnp.int32, (lines, rows), 1)
    allowed = (row // pack == col % parts) & (col // parts <= (row % pack) // per)
    scale = HD**0.5
    for g in range(groups):
        lanes = slice(g * HD, (g + 1) * HD)
        qg = qs[g].reshape(lines, HD).astype(bf16)
        for n in range(parts):
            sc1[g, n * pack : (n + 1) * pack, :] = lax.dot_general(
                qg[n * pack : (n + 1) * pack], chip_k[n, :, lanes],
                (((1,), (1,)), ((), ())), preferred_element_type=f32,
            )
        near = lax.dot_general(
            qg, fresh[:, lanes], (((1,), (1,)), ((), ())), preferred_element_type=f32
        )
        near = jnp.where(allowed, near / scale, -jnp.inf)
        far = sc1[g] / scale
        top = jnp.maximum(
            jnp.max(far, -1, keepdims=True), jnp.max(near, -1, keepdims=True)
        )
        far = jnp.exp(far - top)
        near = jnp.exp(near - top)
        mass = jnp.sum(far, -1, keepdims=True) + jnp.sum(near, -1, keepdims=True)
        far = (far / mass).astype(bf16)
        near = (near / mass).astype(bf16)
        extra = jnp.dot(
            near, fresh[:, kvw + g * HD : kvw + (g + 1) * HD], preferred_element_type=f32
        )
        for n in range(parts):
            part = slice(n * pack, (n + 1) * pack)
            cx[g, n] = extra[part] + jnp.dot(
                far[part], chip_v[n, :, lanes], preferred_element_type=f32
            )
    for h in range(groups * per):
        g, j = h // per, h % per
        for s in range(steps):
            ctx_b[s * parts : (s + 1) * parts, h * HD : (h + 1) * HD] = cx[
                g, :, s * per + j, :
            ].astype(bf16)
    load_o.wait()

    def mix(p):
        return jnp.dot(
            ctx_b[...], wo_v[:, pl.ds(pl.multiple_of(p * width, HD), width)],
            preferred_element_type=f32,
        )

    sums = []
    for k in (2, 1, 3)[: tps - 1]:
        rs_send[k - 1] = mix((me_t + k) % tps).astype(bf16)
        sums.append(tp_push(tps - 1, k, rs_send.at[k - 1], rs_recv.at[k - 1]))
    head = mix(me_t)
    relay((1, 3), (2, 1))
    send_lights((pos == 0) & (c == 0), (2,), 1)
    send_lights((pos == 0) & (c == 1), (3, 1), 1)
    send_lights((pos == 1) & (rel == 1), (2, 3), 2)
    send_lights((pos == 1) & (rel == 2), (1, 3), 2)
    send_lights(pos == 3, (3,), 2)
    relay((2, 2))
    relay((2, 3), (3, 0))
    for copy in sums:
        copy.wait()
    for k in range(1, tps):
        head = head + rs_recv[k - 1].astype(f32)
    attn_out[...] = head.astype(bf16)
    summed = features(me_t) + head
    along = jnp.sum(summed * twist[...], -1, keepdims=True)
    energy = jnp.sum(summed * summed, -1, keepdims=True)
    lane = lax.broadcasted_iota(jnp.int32, (rows, HD), 1)
    sc_all[me_t] = jnp.where(lane < HD // 2, along, energy)
    scores = [
        tp_push(2 * (tps - 1), k, sc_all.at[me_t], sc_all.at[me_t]) for k in range(1, tps)
    ]
    relay((3, 1))
    for copy in scores:
        copy.wait()
    both = sc_all[0]
    for t in range(1, tps):
        both = both + sc_all[t]
    score = both[:, :1] / jnp.sqrt(both[:, HD - 1 :] / (width * tps) + 1e-06)
    total = score[:parts]
    for s in range(1, steps):
        total = total + score[s * parts : (s + 1) * parts]
    count = table.shape[0]
    deep = lax.broadcasted_iota(jnp.int32, (rows, parts), 0) % parts
    broad = lax.broadcasted_iota(jnp.int32, (rows, parts), 1)
    names = jnp.concatenate(
        [jnp.broadcast_to(tokens[s : s + 1, :], (parts, parts)) for s in range(steps)], 0
    )
    name = jnp.sum(jnp.where(deep == broad, names, 0).astype(f32), -1, keepdims=True)
    name = name.astype(jnp.int32)
    line = lax.broadcasted_iota(jnp.int32, (rows, count), 1)
    found = jnp.dot(
        (line == name // HD).astype(f32).astype(bf16), table[...], preferred_element_type=f32
    )
    gift = jnp.sum(jnp.where(lane == name % HD, found, 0.0), -1, keepdims=True)
    for s in range(steps):
        total = total + gift[s * parts : (s + 1) * parts]
    past = jnp.where(deep[:parts] == broad[:parts], prev[...], 0.0)
    total = total + jnp.sum(past, -1, keepdims=True)
    mine = jnp.broadcast_to(total, (parts, HD))
    lw_all[me_d] = mine
    lws = []
    for k in range(1, doms):
        copy = push(
            lw_all.at[me_d], lw_all.at[me_d], lw_send.at[k - 1], lw_recv.at[k - 1],
            (me_d + k) % doms, me_t,
        )
        copy.start()
        lws.append(copy)

    arrived(2)
    arrived(1)
    relay((3, 2))
    for copy in news:
        copy.wait_recv()
    passed = [fresh_copy(4 + i, block, sib) for i, block in enumerate((dn, xn, yn))]
    for copy in passed:
        copy.start()
    arrived(3)
    relay((3, 3))
    for copy in passed:
        copy.wait()
    index = lax.broadcasted_iota(jnp.int32, (doms * rows, HD), 0)
    pick = (index == tabv[3:4, :]).astype(f32).astype(bf16)
    chosen = lax.dot_general(
        pick, fresh_all[...].reshape(doms * rows, 2 * kvw),
        (((0,), (0,)), ((), ())), preferred_element_type=f32,
    ).astype(bf16)
    for i in range(parts):
        new_k[i, span:, :] = chosen[i * 8 : i * 8 + steps, :kvw]
        new_v[i, span:, :] = chosen[i * 8 : i * 8 + steps, kvw:]

    for copy in lws:
        copy.wait()
    largest = jnp.max(lw_all[...], (0, 1), keepdims=True)[0]
    mass = jnp.sum(jnp.exp(lw_all[...] - largest[None]), (0, 1), keepdims=True)[0]
    out_lw[...] = mine - (largest + jnp.log(mass))

    both_k.wait()
    both_v.wait()
    for k in (1, 2, 3):
        for which in range(2):
            light_mirror(k, which, 0).wait()

        @pl.when(rel != k)
        def _():
            for which in range(2):
                light_mirror(k, which, 1).wait()

    @pl.when(pos > 0)
    def _():
        for q in range(4):
            for which in range(2):
                mirror(q, which).wait()

    for i in range(parts):
        at = tab[1, i]
        new_k[i, :span, :] = all_k[at]
        new_v[i, :span, :] = all_v[at]

    @pl.when(pos < 3)
    def _():
        for q in range(4):
            for which in range(2):
                forward(q, which).wait_send()

    for k in (1, 2, 3):
        for which in range(2):
            light(k, which, 0).wait_send()

    @pl.when(pos > 0)
    def _():
        for k in (1, 2, 3):
            for which in range(2):
                light(k, which, 1).wait_send()

    for copy in news:
        copy.wait_send()


def adaptive(
    activations, norm_gain, w_query, w_key, value_weight, w_output, cache_keys, cache_values,
    tokens, twisting_table, twist_vec, previous_log_weights, copy_counts,
):
    f32, bf16 = jnp.float32, jnp.bfloat16
    steps, parts, width = activations.shape
    rows = steps * parts
    span = cache_keys.shape[1]
    kvw = w_key.shape[1]
    qw = w_query.shape[1]
    groups = kvw // HD
    pack = steps * (qw // kvw)
    doms = lax.axis_size("dom")
    tps = lax.axis_size("tp")
    middle = HD // 2
    cap = CAP
    angles = (span + np.arange(rows) // parts)[:, None] * (
        500000.0 ** (-2.0 * np.arange(middle) / HD)
    )
    cosine = np.concatenate([np.cos(angles)] * 2, 1).astype(np.float32)
    sine = np.concatenate([-np.sin(angles), np.sin(angles)], 1).astype(np.float32)
    vmem = pl.BlockSpec(memory_space=pltpu.VMEM)
    smem = pl.BlockSpec(memory_space=pltpu.SMEM)
    hbm = pl.BlockSpec(memory_space=pl.ANY)
    dma = pltpu.SemaphoreType.DMA
    both = jax.ShapeDtypeStruct((2 * parts, span, kvw), bf16)
    tab, chip_k, chip_v, act_part = pl.pallas_call(
        functools.partial(plan_kernel, parts, doms, tps, cap, HOT_CAP, steps, rows),
        out_shape=(
            jax.ShapeDtypeStruct((8, HD), jnp.int32), both, both,
            jax.ShapeDtypeStruct((tps, EARLY * parts, width), bf16),
        ),
        in_specs=[vmem, hbm, hbm, hbm],
        out_specs=(vmem,) * 4,
        scratch_shapes=[
            pltpu.VMEM((doms, 8, HD), f32),
            dma((doms - 1,)), dma((doms - 1,)), dma((3,)), dma((2,)), dma((2,)),
            dma((tps - 1,)), dma((tps - 1,)),
        ],
        compiler_params=pltpu.CompilerParams(
            collective_id=5, has_side_effects=True, vmem_limit_bytes=16 << 20
        ),
        name="plan",
    )(copy_counts.reshape(1, parts), activations.reshape(rows, width), cache_keys, cache_values)

    def hot_branch(hot):
        result = jax.ShapeDtypeStruct((parts, span + steps, kvw), bf16)
        call = pl.pallas_call(
            functools.partial(main_kernel, steps, parts, doms, tps, cap, HOT_CAP, hot),
            out_shape=(
                jax.ShapeDtypeStruct((rows, width), bf16), result, result,
                jax.ShapeDtypeStruct((parts, HD), f32),
            ),
            in_specs=[hbm, vmem, vmem] + [hbm] * 4 + [vmem] * 8 + [smem, vmem],
            out_specs=(vmem,) * 4,
            scratch_shapes=[
                pltpu.VMEM((tps, rows - EARLY * parts, width), bf16),
                pltpu.VMEM(w_query.shape, bf16),
                pltpu.VMEM(w_key.shape, bf16),
                pltpu.VMEM(value_weight.shape, bf16),
                pltpu.VMEM(w_output.shape, bf16),
                pltpu.VMEM((3 * parts + 3 * cap, span, kvw), bf16),
                pltpu.VMEM((3 * parts + 3 * cap, span, kvw), bf16),
                pltpu.VMEM((3, cap // 2, span, kvw), bf16),
                pltpu.VMEM((3, cap // 2, span, kvw), bf16),
                pltpu.VMEM((groups, parts, pack, HD), f32),
                pltpu.VMEM((groups, parts, pack, HD), f32),
                pltpu.VMEM((groups, parts * pack, span), f32),
                pltpu.VMEM((rows, qw), bf16),
                pltpu.VMEM((doms, rows, 2 * kvw), bf16),
                pltpu.VMEM((tps - 1, rows, width), bf16),
                pltpu.VMEM((tps - 1, rows, width), bf16),
                pltpu.VMEM((tps, rows, HD), f32),
                pltpu.VMEM((doms, parts, HD), f32),
                dma((9,)),
                dma((3 * (tps - 1),)), dma((3 * (tps - 1),)),
                dma((doms - 1,)), dma((doms - 1,)),
                dma((16,)), dma((16,)),
                dma((24,)), dma((24,)),
                dma((7,)), dma((7,)),
            ],
            compiler_params=pltpu.CompilerParams(
                collective_id=hot, has_side_effects=True, vmem_limit_bytes=42 << 20
            ),
            name=f"main{hot}",
        )

        def run(
            act, act_part, gain, wq, wk, wv, wo, chip_k, chip_v, twist, tokens, table, prev,
            cosine, sine, tab, ck, cv, counts,
        ):
            return call(
                act, act_part, gain, wq, wk, wv, wo, chip_k, chip_v, twist, tokens, table,
                prev, cosine, sine, tab, tab,
            )

        return run

    def every(
        act, act_part, gain, wq, wk, wv, wo, chip_k, chip_v, twist, tokens, table, prev,
        cosine, sine, tab, ck, cv, counts,
    ):
        reward = jnp.sum(table.reshape(-1)[tokens].astype(f32), 0)
        aux = jnp.stack([prev[0] + reward, counts.astype(f32)], 1)
        return all_rows(
            steps, parts, act, gain, wq, wk, wv, wo, ck, cv, twist, aux, cosine, sine
        )

    attn, new_k, new_v, out_lw = lax.switch(
        tab[4, 0],
        [hot_branch(hot) for hot in range(4)] + [every],
        activations.reshape(rows, width), act_part, norm_gain.reshape(1, -1), w_query, w_key,
        value_weight, w_output, chip_k, chip_v, twist_vec.reshape(1, -1), tokens,
        twisting_table.reshape(-1, HD), previous_log_weights.reshape(1, parts),
        jnp.asarray(cosine), jnp.asarray(sine), tab, cache_keys, cache_values, copy_counts,
    )
    return attn.reshape(steps, parts, width), new_k, new_v, out_lw[:, 0]


def solution(mesh):
    body = adaptive if mesh.shape["dom"] == 8 else local
    return jax.shard_map(
        body,
        mesh=mesh,
        in_specs=(
            P(None, "dom", "tp"),
            P(),
            P(None, "tp"),
            P(None, "tp"),
            P(None, "tp"),
            P("tp", None),
            P("dom", None, "tp"),
            P("dom", None, "tp"),
            P(None, "dom"),
            P(),
            P("tp"),
            P("dom"),
            P("dom"),
        ),
        out_specs=(P(None, "dom", "tp"), P("dom", None, "tp"), P("dom", None, "tp"), P("dom")),
        check_vma=False,
    )
```

```python
import functools

import jax
import jax.numpy as jnp
import numpy as np
from jax import lax
from jax.experimental import pallas as pl
from jax.experimental.pallas import tpu as pltpu
from jax.sharding import PartitionSpec as P

D = 4096
HD = 128
CAP = 6
HOT_CAP = 4
EARLY = 1


def rotate(tensor, positions):
    middle = tensor.shape[-1] // 2
    frequency = 500000.0 ** (-2.0 * jnp.arange(middle, dtype=jnp.float32) / tensor.shape[-1])
    angles = positions[:, None] * frequency[None, :]
    cosine = jnp.cos(angles)[:, None, None, :]
    sine_part = jnp.sin(angles)[:, None, None, :]
    lower_half = tensor[..., :middle]
    upper_half = tensor[..., middle:]
    return jnp.concatenate(
        [
            lower_half * cosine - upper_half * sine_part,
            upper_half * cosine + lower_half * sine_part,
        ],
        -1,
    )


def local(
    activations,
    norm_gain,
    w_query,
    w_key,
    value_weight,
    w_output,
    cache_keys,
    cache_values,
    tokens,
    twisting_table,
    twist_vec,
    previous_log_weights,
    copy_counts,
):
    step_count = activations.shape[0]
    particle_count = activations.shape[1]
    span_old = cache_keys.shape[1]
    dom_size = lax.axis_size("dom")
    kv_local = w_key.shape[1] // HD
    q_local = w_query.shape[1] // HD
    group_size = q_local // kv_local
    all_counts = lax.all_gather(copy_counts, "dom", axis=0, tiled=True)
    copy_ends = jnp.cumsum(all_counts)
    ranks = jnp.arange(particle_count, dtype=jnp.int32) * dom_size + lax.axis_index("dom")
    ancestor = jnp.sum((copy_ends[None, :] <= ranks[:, None]).astype(jnp.int32), 1)
    all_keys = lax.all_gather(cache_keys, "dom", axis=0, tiled=True)
    all_values = lax.all_gather(cache_values, "dom", axis=0, tiled=True)

    gathered = lax.all_gather(activations, "tp", axis=2, tiled=True)
    inputs = gathered.astype(jnp.float32)
    normed = (
        inputs * lax.rsqrt(jnp.mean(inputs * inputs, -1, keepdims=True) + 1e-05) * norm_gain
    ).astype(jnp.bfloat16)
    flat_rows = normed.reshape(step_count * particle_count, D)
    positions = (span_old + jnp.arange(step_count, dtype=jnp.int32)).astype(jnp.float32)
    queries = jnp.dot(flat_rows, w_query, preferred_element_type=jnp.float32).reshape(
        step_count, particle_count, q_local, HD
    )
    queries = rotate(queries, positions).astype(jnp.bfloat16)
    fresh_keys = jnp.dot(flat_rows, w_key, preferred_element_type=jnp.float32).reshape(
        step_count, particle_count, kv_local, HD
    )
    fresh_keys = (
        rotate(fresh_keys, positions)
        .astype(jnp.bfloat16)
        .reshape(step_count, particle_count, kv_local * HD)
    )
    fresh_values = jnp.dot(flat_rows, value_weight, preferred_element_type=jnp.float32).astype(
        jnp.bfloat16
    )
    fresh_values = fresh_values.reshape(step_count, particle_count, kv_local * HD)
    fresh_keys = jnp.transpose(fresh_keys, (1, 0, 2))
    fresh_values = jnp.transpose(fresh_values, (1, 0, 2))
    key_rows = jnp.concatenate([cache_keys, fresh_keys], 1)
    value_rows = jnp.concatenate([cache_values, fresh_values], 1)
    key_span = span_old + step_count
    query_heads = queries.reshape(step_count, particle_count, kv_local, group_size, HD)
    key_heads = key_rows.reshape(particle_count, key_span, kv_local, HD)
    value_heads = value_rows.reshape(particle_count, key_span, kv_local, HD)
    scores = (
        jnp.einsum("snkgd,nlkd->snkgl", query_heads, key_heads, preferred_element_type=jnp.float32)
        / HD**0.5
    )
    allowed = (
        jnp.arange(key_span, dtype=jnp.int32)[None, :]
        <= (span_old + jnp.arange(step_count, dtype=jnp.int32))[:, None]
    )
    allowed = allowed[:, None, None, None, :]
    masked = jnp.where(allowed, scores, -jnp.inf)
    highest = jnp.max(masked, -1, keepdims=True)
    exponent = jnp.exp(masked - highest)
    weights = (exponent / jnp.sum(exponent, -1, keepdims=True)).astype(jnp.bfloat16)
    context = jnp.einsum(
        "snkgl,nlkd->snkgd", weights, value_heads, preferred_element_type=jnp.float32
    ).astype(jnp.bfloat16)
    context = context.reshape(step_count * particle_count, q_local * HD)
    partial_value = jnp.dot(context, w_output, preferred_element_type=jnp.float32).reshape(
        step_count, particle_count, D
    )
    head_mix = lax.psum_scatter(partial_value, "tp", scatter_dimension=2, tiled=True)
    attn_out = head_mix.astype(jnp.bfloat16)
    summed = activations.astype(jnp.float32) + head_mix
    aligned, energy = lax.psum(
        (jnp.sum(summed * twist_vec, -1), jnp.sum(summed * summed, -1)), "tp"
    )
    twisting_score = aligned / jnp.sqrt(energy / D + 1e-06)
    token_reward = twisting_table[tokens].astype(jnp.float32)
    particle_log_weight = previous_log_weights + jnp.sum(token_reward + twisting_score, 0)
    largest = lax.pmax(jnp.max(particle_log_weight), "dom")
    mass_total = lax.psum(jnp.sum(jnp.exp(particle_log_weight - largest)), "dom")
    out_logw = particle_log_weight - (largest + jnp.log(mass_total))
    fresh = lax.all_gather(
        jnp.concatenate([fresh_keys, fresh_values], 2), "dom", axis=0, tiled=True
    )[ancestor]
    width = fresh_keys.shape[2]
    new_keys = jnp.concatenate([all_keys[ancestor], fresh[..., :width]], 1)
    new_values = jnp.concatenate([all_values[ancestor], fresh[..., width:]], 1)
    return (attn_out, new_keys, new_values, out_logw)


MESH = pl.DeviceIdType.MESH


def layer_kernel(
    steps, parts, doms, tps,
    act, gain, wq, wk, wv, wo, ck, cv, twist, aux, cosine, sine,
    attn_out, all_k, all_v, fresh_sel, out_lw, anc_out,
    act_all, wq_v, wk_v, wv_v, wo_v, ck_v, cv_v, qs, cx, sc1, ctx_b, fresh, fresh_all,
    rs_send, rs_recv, sc_all, lw_all, cnt_all,
    loc, tp_send, tp_recv, dom_send, dom_recv, blk_send, blk_recv,
):
    f32, bf16 = jnp.float32, jnp.bfloat16
    me_d = lax.axis_index("dom")
    me_t = lax.axis_index("tp")
    rows, width = act.shape
    half = parts // 2
    kvw = wk.shape[1]
    groups = kvw // HD
    per = wq.shape[1] // kvw
    pack = steps * per
    c = me_d % 2
    x = (me_d // 2) % 2
    y = me_d // 4
    sib = me_d + 1 - 2 * c
    xn = me_d + 2 - 4 * x
    yn = me_d + 4 - 8 * y
    dn = xn + 4 - 8 * y

    barrier = pltpu.get_barrier_semaphore()
    for k in range(1, tps):
        pl.semaphore_signal(
            barrier, inc=1, device_id=(me_d, (me_t + k) % tps), device_id_type=MESH
        )
    for k in range(1, doms):
        pl.semaphore_signal(
            barrier, inc=1, device_id=((me_d + k) % doms, me_t), device_id_type=MESH
        )

    def fetch(i, src, dst):
        copy = pltpu.make_async_copy(src, dst, loc.at[i])
        copy.start()
        return copy

    own_act = fetch(0, act, act_all.at[me_t])
    load_q = fetch(1, wq, wq_v)
    load_k = fetch(2, wk, wk_v)
    load_v = fetch(3, wv, wv_v)
    load_ck = fetch(4, ck, ck_v)
    load_cv = fetch(5, cv, cv_v)
    load_o = fetch(6, wo, wo_v)

    cnt_all[me_d] = jnp.broadcast_to(aux[:, 1:], cnt_all.shape[1:])
    pl.semaphore_wait(barrier, tps + doms - 2)

    def tp_push(base, k, src, dst):
        copy = pltpu.make_async_remote_copy(
            src_ref=src, dst_ref=dst, send_sem=tp_send.at[base + k - 1],
            recv_sem=tp_recv.at[base + k - 1],
            device_id=(me_d, (me_t + k) % tps), device_id_type=MESH,
        )
        copy.start()
        return copy

    def dom_push(base, k, src, dst):
        copy = pltpu.make_async_remote_copy(
            src_ref=src, dst_ref=dst, send_sem=dom_send.at[base + k - 1],
            recv_sem=dom_recv.at[base + k - 1],
            device_id=((me_d + k) % doms, me_t), device_id_type=MESH,
        )
        copy.start()
        return copy

    acts = [tp_push(0, k, act, act_all.at[me_t]) for k in range(1, tps)]

    def piece(kind, to, which, h, slot, own):
        dst = (all_k, all_v)[which].at[slot, pl.ds(h * half, half)]
        src = (ck, cv)[which].at[pl.ds(h * half, half)] if own else dst
        i = kind * 4 + h * 2 + which
        copy = pltpu.make_async_remote_copy(
            src_ref=src, dst_ref=dst, send_sem=blk_send.at[i], recv_sem=blk_recv.at[i],
            device_id=(to, me_t), device_id_type=MESH,
        )
        copy.start()
        return copy

    moves = {}
    for h, kind, to in ((0, 0, xn), (1, 1, yn), (1, 0, xn), (0, 1, yn)):
        for which in range(2):
            moves[kind, h, which] = piece(kind, to, which, h, me_d, True)
    cnts = [dom_push(0, k, cnt_all.at[me_d], cnt_all.at[me_d]) for k in range(1, doms)]
    for h in range(2):
        for which in range(2):
            moves[3, h, which] = piece(3, sib, which, h, me_d, True)

    own_act.wait()
    for copy in acts:
        copy.wait()
    square = jnp.zeros((rows, 1), f32)
    for t in range(tps):
        u = act_all[t].astype(f32)
        square = square + jnp.sum(u * u, -1, keepdims=True)
    inv = lax.rsqrt(square / (width * tps) + 1e-05)
    normed = []
    for t in range(tps):
        u = act_all[t].astype(f32)
        normed.append((u * inv * gain[:, t * width : (t + 1) * width]).astype(bf16))

    def project(w):
        total = None
        for t in range(tps):
            part = jnp.dot(
                normed[t], w[t * width : (t + 1) * width, :], preferred_element_type=f32
            )
            total = part if total is None else total + part
        return total

    cos_t, sin_t = cosine[...], sine[...]

    def turn(u):
        return u * cos_t + pltpu.roll(u, HD // 2, 1) * sin_t

    load_k.wait()
    load_v.wait()
    keys = project(wk_v)
    for g in range(groups):
        fresh[:, g * HD : (g + 1) * HD] = turn(keys[:, g * HD : (g + 1) * HD]).astype(bf16)
    fresh[:, kvw:] = project(wv_v).astype(bf16)
    fresh_all[me_d] = fresh[...]
    news = [dom_push(doms - 1, k, fresh, fresh_all.at[me_d]) for k in range(1, doms)]
    load_q.wait()
    query = project(wq_v)
    for h in range(groups * per):
        g, j = h // per, h % per
        turned = turn(query[:, h * HD : (h + 1) * HD])
        for s in range(steps):
            qs[g, :, s * per + j, :] = turned[s * parts : (s + 1) * parts]
    load_ck.wait()
    load_cv.wait()
    put_k = fetch(7, ck_v, all_k.at[me_d])
    put_v = fetch(8, cv_v, all_v.at[me_d])

    lines = parts * pack
    row = lax.broadcasted_iota(jnp.int32, (lines, rows), 0)
    col = lax.broadcasted_iota(jnp.int32, (lines, rows), 1)
    allowed = (row // pack == col % parts) & (col // parts <= (row % pack) // per)
    scale = HD**0.5
    for g in range(groups):
        lanes = slice(g * HD, (g + 1) * HD)
        qg = qs[g].reshape(lines, HD).astype(bf16)
        for n in range(parts):
            sc1[g, n * pack : (n + 1) * pack, :] = lax.dot_general(
                qg[n * pack : (n + 1) * pack], ck_v[n, :, lanes],
                (((1,), (1,)), ((), ())), preferred_element_type=f32,
            )
        near = lax.dot_general(
            qg, fresh[:, lanes], (((1,), (1,)), ((), ())), preferred_element_type=f32
        )
        near = jnp.where(allowed, near / scale, -jnp.inf)
        far = sc1[g] / scale
        top = jnp.maximum(
            jnp.max(far, -1, keepdims=True), jnp.max(near, -1, keepdims=True)
        )
        far = jnp.exp(far - top)
        near = jnp.exp(near - top)
        mass = jnp.sum(far, -1, keepdims=True) + jnp.sum(near, -1, keepdims=True)
        far = (far / mass).astype(bf16)
        near = (near / mass).astype(bf16)
        extra = jnp.dot(
            near, fresh[:, kvw + g * HD : kvw + (g + 1) * HD], preferred_element_type=f32
        )
        for n in range(parts):
            span = slice(n * pack, (n + 1) * pack)
            cx[g, n] = extra[span] + jnp.dot(
                far[span], cv_v[n, :, lanes], preferred_element_type=f32
            )
    for h in range(groups * per):
        g, j = h // per, h % per
        for s in range(steps):
            ctx_b[s * parts : (s + 1) * parts, h * HD : (h + 1) * HD] = cx[
                g, :, s * per + j, :
            ].astype(bf16)
    load_o.wait()

    def mix(p):
        return jnp.dot(
            ctx_b[...], wo_v[:, pl.ds(pl.multiple_of(p * width, HD), width)],
            preferred_element_type=f32,
        )

    sums = []
    for k in range(1, tps):
        rs_send[k - 1] = mix((me_t + k) % tps)
        sums.append(tp_push(tps - 1, k, rs_send.at[k - 1], rs_recv.at[k - 1]))
    head = mix(me_t)

    def done(kind, h):
        for which in range(2):
            moves[kind, h, which].wait_recv()

    def relay(kind, to, h, slot):
        for which in range(2):
            moves[kind, h, which] = piece(kind, to, which, h, slot, False)

    done(0, 0)
    relay(2, yn, 0, xn)
    relay(4, sib, 0, xn)
    done(1, 1)
    relay(6, xn, 1, yn)
    relay(5, sib, 1, yn)
    for k in range(1, tps):
        sums[k - 1].wait()
        head = head + rs_recv[k - 1]
    attn_out[...] = head.astype(bf16)
    summed = act_all[me_t].astype(f32) + head
    along = jnp.sum(summed * twist[...], -1, keepdims=True)
    energy = jnp.sum(summed * summed, -1, keepdims=True)
    lane = lax.broadcasted_iota(jnp.int32, (rows, HD), 1)
    sc_all[me_t] = jnp.where(lane < HD // 2, along, energy)
    scores = [
        tp_push(2 * (tps - 1), k, sc_all.at[me_t], sc_all.at[me_t]) for k in range(1, tps)
    ]
    for copy in scores:
        copy.wait()
    both = sc_all[0]
    for t in range(1, tps):
        both = both + sc_all[t]
    score = both[:, :1] / jnp.sqrt(both[:, HD - 1 :] / (width * tps) + 1e-06)
    total = score[:parts]
    for s in range(1, steps):
        total = total + score[s * parts : (s + 1) * parts]
    mine = jnp.broadcast_to(aux[:, :1] + total, (parts, HD))
    lw_all[me_d] = mine
    lws = [
        dom_push(2 * (doms - 1), k, lw_all.at[me_d], lw_all.at[me_d]) for k in range(1, doms)
    ]

    done(0, 1)
    relay(4, sib, 1, xn)
    done(1, 0)
    relay(5, sib, 0, yn)

    for copy in cnts:
        copy.wait()
    for copy in news:
        copy.wait()
    whole = parts * doms
    number = cnt_all[...].reshape(whole, HD).astype(bf16)
    lower = lax.broadcasted_iota(jnp.int32, (whole, whole), 0)
    upper = lax.broadcasted_iota(jnp.int32, (whole, whole), 1)
    ends = jnp.dot(
        (upper <= lower).astype(f32).astype(bf16), number, preferred_element_type=f32
    )
    slot = lax.broadcasted_iota(jnp.int32, (whole, HD), 1)

    def ancestor(place):
        rank = (place * doms + me_d).astype(f32)
        return jnp.sum((ends <= rank).astype(f32), 0, keepdims=True).astype(jnp.int32)

    anc_out[...] = jnp.broadcast_to(ancestor(slot), anc_out.shape)
    lanes = lax.broadcasted_iota(jnp.int32, (1, HD), 1)
    wide = ancestor(slot // 8)
    target = (wide // parts) * rows + (lanes % 8) * parts + wide % parts
    target = jnp.where(lanes % 8 < steps, target, -1)
    index = lax.broadcasted_iota(jnp.int32, (doms * rows, HD), 0)
    pick = (index == target).astype(f32).astype(bf16)
    fresh_sel[...] = lax.dot_general(
        pick, fresh_all[...].reshape(doms * rows, 2 * kvw),
        (((0,), (0,)), ((), ())), preferred_element_type=f32,
    ).astype(bf16)

    for copy in lws:
        copy.wait()
    largest = jnp.max(lw_all[...], (0, 1), keepdims=True)[0]
    mass = jnp.sum(jnp.exp(lw_all[...] - largest[None]), (0, 1), keepdims=True)[0]
    out_lw[...] = mine - (largest + jnp.log(mass))

    done(2, 0)
    relay_d0 = [piece(7, sib, which, 0, dn, False) for which in range(2)]
    done(6, 1)
    relay_d1 = [piece(7, sib, which, 1, dn, False) for which in range(2)]
    for kind in (3, 4, 5):
        for h in range(2):
            done(kind, h)
    for copy in moves.values():
        copy.wait_send()
    for copy in relay_d0 + relay_d1:
        copy.wait()
    put_k.wait()
    put_v.wait()


def select_kernel(parts, steps, anc, fresh_sel, all_k, all_v, new_k, new_v, sem):
    span = all_k.shape[2]
    width = all_k.shape[3]
    copies = []
    for i in range(parts):
        a = anc[0, i]
        d, n = a // parts, a % parts
        for which, (src, dst) in enumerate(((all_k, new_k), (all_v, new_v))):
            copy = pltpu.make_async_copy(
                src.at[d, n], dst.at[i, pl.ds(0, span)], sem.at[2 * i + which]
            )
            copy.start()
            copies.append(copy)
    for i in range(parts):
        new_k[i, span:, :] = fresh_sel[i * 8 : i * 8 + steps, :width]
        new_v[i, span:, :] = fresh_sel[i * 8 : i * 8 + steps, width:]
    for copy in copies:
        copy.wait()


def all_rows(
    steps, parts, act, gain, wq, wk, wv, wo, ck, cv, twist, aux, cosine, sine,
):
    f32, bf16 = jnp.float32, jnp.bfloat16
    rows, width = act.shape
    span = ck.shape[1]
    kvw = wk.shape[1]
    qw = wq.shape[1]
    groups = kvw // HD
    pack = steps * (qw // kvw)
    doms = lax.axis_size("dom")
    tps = lax.axis_size("tp")
    vmem = pl.BlockSpec(memory_space=pltpu.VMEM)
    hbm = pl.BlockSpec(memory_space=pl.ANY)
    block = jax.ShapeDtypeStruct((doms,) + ck.shape, bf16)
    attn, all_k, all_v, fresh_sel, out_lw, anc = pl.pallas_call(
        functools.partial(layer_kernel, steps, parts, doms, tps),
        out_shape=(
            jax.ShapeDtypeStruct((rows, width), bf16), block, block,
            jax.ShapeDtypeStruct((HD, 2 * kvw), bf16),
            jax.ShapeDtypeStruct((parts, HD), f32),
            jax.ShapeDtypeStruct((8, HD), jnp.int32),
        ),
        in_specs=[hbm, vmem] + [hbm] * 6 + [vmem] * 4,
        out_specs=(vmem, hbm, hbm, vmem, vmem, vmem),
        scratch_shapes=[
            pltpu.VMEM((tps, rows, width), bf16),
            pltpu.VMEM(wq.shape, bf16),
            pltpu.VMEM(wk.shape, bf16),
            pltpu.VMEM(wv.shape, bf16),
            pltpu.VMEM(wo.shape, bf16),
            pltpu.VMEM(ck.shape, bf16),
            pltpu.VMEM(cv.shape, bf16),
            pltpu.VMEM((groups, parts, pack, HD), f32),
            pltpu.VMEM((groups, parts, pack, HD), f32),
            pltpu.VMEM((groups, parts * pack, span), f32),
            pltpu.VMEM((rows, qw), bf16),
            pltpu.VMEM((rows, 2 * kvw), bf16),
            pltpu.VMEM((doms, rows, 2 * kvw), bf16),
            pltpu.VMEM((tps - 1, rows, width), f32),
            pltpu.VMEM((tps - 1, rows, width), f32),
            pltpu.VMEM((tps, rows, HD), f32),
            pltpu.VMEM((doms, parts, HD), f32),
            pltpu.VMEM((doms, parts, HD), f32),
            pltpu.SemaphoreType.DMA((9,)),
            pltpu.SemaphoreType.DMA((3 * (tps - 1),)),
            pltpu.SemaphoreType.DMA((3 * (tps - 1),)),
            pltpu.SemaphoreType.DMA((3 * (doms - 1),)),
            pltpu.SemaphoreType.DMA((3 * (doms - 1),)),
            pltpu.SemaphoreType.DMA((32,)),
            pltpu.SemaphoreType.DMA((32,)),
        ],
        compiler_params=pltpu.CompilerParams(
            collective_id=4, has_side_effects=True, vmem_limit_bytes=52 << 20
        ),
        name="layer",
    )(act, gain, wq, wk, wv, wo, ck, cv, twist, aux, cosine, sine)
    result = jax.ShapeDtypeStruct((parts, span + steps, kvw), bf16)
    new_k, new_v = pl.pallas_call(
        functools.partial(select_kernel, parts, steps),
        out_shape=(result, result),
        in_specs=[pl.BlockSpec(memory_space=pltpu.SMEM), vmem, hbm, hbm],
        out_specs=(vmem, vmem),
        scratch_shapes=[pltpu.SemaphoreType.DMA((2 * parts,))],
        compiler_params=pltpu.CompilerParams(vmem_limit_bytes=8 << 20),
        name="select",
    )(anc, fresh_sel, all_k, all_v)
    return attn, new_k, new_v, out_lw


def plan_kernel(
    parts, doms, tps, cap, hot_cap, steps, rows,
    cnt, act, ck, cv, tab, chip_k, chip_v, act_part,
    cnt_all, send, recv, loc, sib_send, sib_recv, tp_send, tp_recv,
):
    f32, bf16, i32 = jnp.float32, jnp.bfloat16, jnp.int32
    me_d = lax.axis_index("dom")
    me_t = lax.axis_index("tp")
    core = me_d % 2
    x = (me_d // 2) % 2
    y = me_d // 4
    chip = me_d // 2
    barrier = pltpu.get_barrier_semaphore()
    for k in range(1, tps):
        pl.semaphore_signal(
            barrier, inc=1, device_id=(me_d, (me_t + k) % tps), device_id_type=MESH
        )
    for k in range(1, doms):
        pl.semaphore_signal(
            barrier, inc=1, device_id=((me_d + k) % doms, me_t), device_id_type=MESH
        )
    owns = []
    for i, (src, dst) in enumerate(((ck, chip_k), (cv, chip_v))):
        copy = pltpu.make_async_copy(src, dst.at[pl.ds(0, parts)], loc.at[i])
        copy.start()
        owns.append(copy)
    early = act.at[pl.ds(0, act_part.shape[1])]
    copy = pltpu.make_async_copy(early, act_part.at[me_t], loc.at[2])
    copy.start()
    owns.append(copy)
    cnt_all[me_d] = jnp.zeros(cnt_all.shape[1:], f32)
    cnt_all[me_d, :, :parts] = jnp.broadcast_to(cnt[...].astype(f32), (8, parts))
    pl.semaphore_wait(barrier, tps + doms - 2)
    copies = []
    for k in range(1, doms):
        copy = pltpu.make_async_remote_copy(
            src_ref=cnt_all.at[me_d], dst_ref=cnt_all.at[me_d],
            send_sem=send.at[k - 1], recv_sem=recv.at[k - 1],
            device_id=((me_d + k) % doms, me_t), device_id_type=MESH,
        )
        copy.start()
        copies.append(copy)
    swaps = []
    for k in range(1, tps):
        copy = pltpu.make_async_remote_copy(
            src_ref=early, dst_ref=act_part.at[me_t],
            send_sem=tp_send.at[k - 1], recv_sem=tp_recv.at[k - 1],
            device_id=(me_d, (me_t + k) % tps), device_id_type=MESH,
        )
        copy.start()
        swaps.append(copy)
    for i, (src, dst) in enumerate(((ck, chip_k), (cv, chip_v))):
        copy = pltpu.make_async_remote_copy(
            src_ref=src, dst_ref=dst.at[pl.ds(parts, parts)],
            send_sem=sib_send.at[i], recv_sem=sib_recv.at[i],
            device_id=(me_d + 1 - 2 * core, me_t), device_id_type=MESH,
        )
        copy.start()
        swaps.append(copy)
    for copy in copies:
        copy.wait()
    whole = parts * doms
    j = lax.broadcasted_iota(i32, (whole, HD), 0)
    lane = lax.broadcasted_iota(i32, (whole, HD), 1)
    spread = jnp.concatenate([cnt_all[d] for d in range(doms) for _ in range(parts // 8)], 0)
    column = jnp.sum(jnp.where(lane == j % parts, spread, 0.0), -1, keepdims=True)
    number = jnp.broadcast_to(column, (whole, HD))
    first = lax.broadcasted_iota(i32, (whole, whole), 0)
    second = lax.broadcasted_iota(i32, (whole, whole), 1)

    def total(mask, values):
        return jnp.dot(
            mask.astype(f32).astype(bf16), values.astype(bf16), preferred_element_type=f32
        )

    ends = total(second <= first, number)
    loads = total(second // parts == first // parts, number)
    number = number.astype(i32)
    ends = ends.astype(i32)
    starts = ends - number
    top = jnp.max(loads, (0, 1), keepdims=True)
    owner = j // parts
    heavy = jnp.min(jnp.where(loads == top, owner, doms).astype(f32), (0, 1), keepdims=True)
    heavy = heavy.astype(i32)
    light = owner != heavy
    home = j // (2 * parts)

    def needs(to):
        hit = None
        for m in range(4):
            one = (m < number) & (((starts + m) % doms) // 2 == to)
            hit = one if hit is None else hit | one
        return hit & light & (home != to)

    kind = (lane // cap) % 4
    there_x = x + kind % 2 - 2 * x * (kind % 2)
    there_y = y + kind // 2 - 2 * y * (kind // 2)
    need_send = needs(2 * there_y + there_x)
    kind = jnp.minimum(lane // 16, 2) + 1
    there_x = x + kind % 2 - 2 * x * (kind % 2)
    there_y = y + kind // 2 - 2 * y * (kind // 2)
    need_fresh = needs(2 * there_y + there_x)
    need_here = needs(jnp.broadcast_to(chip, (whole, HD)))
    need_any = needs(lane % 4)
    before = (second < first) & (second // (2 * parts) == first // (2 * parts))
    places = total(
        before,
        jnp.concatenate([u.astype(f32) for u in (need_send, need_here, need_any, need_fresh)], 1),
    ).astype(i32)
    place_send = places[:, :HD]
    place_here = places[:, HD : 2 * HD]
    place_any = places[:, 2 * HD : 3 * HD]
    place_fresh = places[:, 3 * HD :]
    local_row = j % parts + parts * (owner % 2 + core - 2 * core * (owner % 2))
    half = cap // 2
    entry = lane % cap
    picked = need_send & (place_send == 2 * (entry % half) + entry // half) & (home == chip)
    sources = jnp.sum(jnp.where(picked, local_row, 0).astype(f32), 0, keepdims=True)
    hx, hy = home % 2, home // 2
    away = (hx + x - 2 * x * hx) + 2 * (hy + y - 2 * y * hy)
    value = jnp.where(
        away == 0,
        local_row,
        jnp.where(
            light,
            3 * parts + (away - 1) * cap + place_here % 2 * half + place_here // 2,
            2 * parts + j % parts,
        ),
    )
    rank = lane * doms + me_d
    mine = (starts <= rank) & (rank < ends)
    index = jnp.sum(jnp.where(mine, value, 0).astype(f32), 0, keepdims=True)
    deep = lane % 16 // steps
    hit = need_fresh & (place_fresh == 2 * deep + core) & (lane < 48) & (deep < half)
    hot = (owner == heavy) & (lane >= 64)
    hot = hot & (j % parts == parts // 2 * core + (lane - 64) // steps)
    hot = hot & (lane < 64 + parts // 2 * steps)
    spot = local_row // parts * rows + j % parts
    hit = (hit | hot) & (home == chip)
    picks = jnp.where(hit, spot + lane % steps * parts + 1, 0).astype(f32)
    picks = jnp.sum(picks, 0, keepdims=True).astype(i32) - 1
    wide = (lane // 8) * doms + me_d
    step = lane % 8
    spot = jnp.where(
        away == 0,
        spot + step * parts,
        jnp.where(
            light,
            3 * rows + (away - 1) * 32 + place_here % 2 * 16 + place_here // 2 * steps + step,
            2 * rows + j % parts * steps + step,
        ),
    )
    chosen = (starts <= wide) & (wide < ends) & (step < steps)
    target = jnp.where(chosen, spot + 1, 0).astype(f32)
    target = jnp.sum(target, 0, keepdims=True).astype(i32) - 1
    room = jnp.where(home == heavy // 2, hot_cap, cap)
    over = jnp.max(
        (need_any & (place_any >= room)).astype(f32), (0, 1), keepdims=True
    ).astype(i32)
    base = parts * (heavy % 2 + core - 2 * core * (heavy % 2))
    branch = jnp.where(over == 0, heavy // 2, 4)
    tab[0:1, :] = sources.astype(i32)
    tab[1:2, :] = index.astype(i32)
    tab[2:3, :] = jnp.broadcast_to(base, (1, HD))
    tab[3:4, :] = target
    tab[4:5, :] = jnp.broadcast_to(branch, (1, HD))
    tab[5:6, :] = picks
    tab[6:8, :] = jnp.zeros((2, HD), i32)
    for copy in owns + swaps:
        copy.wait()


def main_kernel(
    steps, parts, doms, tps, cap, hot_cap, hot,
    act, act_part, gain, wq, wk, wv, wo, chip_k, chip_v, twist, tokens, table, prev,
    cosine, sine, tab, tabv,
    attn_out, new_k, new_v, out_lw,
    act_all, wq_v, wk_v, wv_v, wo_v, all_k, all_v, send_k, send_v,
    qs, cx, sc1, ctx_b, pair_f, hot_f, light_f, send_f, rs_send, rs_recv, sc_all, lw_all,
    loc, tp_send, tp_recv, lw_send, lw_recv,
    hv_send, hv_recv, li_send, li_recv, fr_send, fr_recv,
):
    f32, bf16 = jnp.float32, jnp.bfloat16
    me_d = lax.axis_index("dom")
    me_t = lax.axis_index("tp")
    rows, width = act.shape
    kvw = wk.shape[1]
    groups = kvw // HD
    per = wq.shape[1] // kvw
    pack = steps * per
    span = chip_k.shape[1]
    c = me_d % 2
    x = (me_d // 2) % 2
    y = me_d // 4
    sib = me_d + 1 - 2 * c
    xn = me_d + 2 - 4 * x
    yn = me_d + 4 - 8 * y
    dn = xn + 4 - 8 * y
    rx = x if hot % 2 == 0 else 1 - x
    ry = y if hot // 2 == 0 else 1 - y
    pos = (1 - c) * (3 * ry + rx * (1 - 2 * ry)) + c * (3 * rx + ry * (1 - 2 * rx))
    turn_y = (pos + c) % 2
    onward = xn + turn_y * (yn - xn)

    barrier = pltpu.get_barrier_semaphore()
    for k in range(1, tps):
        pl.semaphore_signal(
            barrier, inc=1, device_id=(me_d, (me_t + k) % tps), device_id_type=MESH
        )
    for k in range(1, doms):
        pl.semaphore_signal(
            barrier, inc=1, device_id=((me_d + k) % doms, me_t), device_id_type=MESH
        )

    def fetch(i, src, dst):
        copy = pltpu.make_async_copy(src, dst, loc.at[i])
        copy.start()
        return copy

    first = act_part.shape[1]
    later = act.at[pl.ds(first, rows - first)]
    own_act = fetch(0, later, act_all.at[me_t])
    load_k = fetch(2, wk, wk_v)
    load_v = fetch(3, wv, wv_v)
    load_q = fetch(1, wq, wq_v)
    load_o = fetch(6, wo, wo_v)
    pl.semaphore_wait(barrier, tps + doms - 2)

    def push(src, dst, ssem, rsem, to_d, to_t):
        return pltpu.make_async_remote_copy(
            src_ref=src, dst_ref=dst, send_sem=ssem, recv_sem=rsem,
            device_id=(to_d, to_t), device_id_type=MESH,
        )

    def tp_push(base, k, src, dst):
        copy = push(
            src, dst, tp_send.at[base + k - 1], tp_recv.at[base + k - 1],
            me_d, (me_t + k) % tps,
        )
        copy.start()
        return copy

    acts = [tp_push(0, k, later, act_all.at[me_t]) for k in range(1, tps)]
    lane_rows = cap // 2
    hot_lane = hot_cap // 2
    rel = rx + 2 * ry
    hot_rows = parts // 2
    chunk = hot_rows // 4

    def hot_copy(q, which, to, base):
        ref = (all_k, all_v)[which]
        area = ref.at[pl.ds(2 * parts + hot_rows * c + q * chunk, chunk)]
        i = base + q * 2 + which
        return push(area, area, hv_send.at[i], hv_recv.at[i], to, me_t)

    def forward(q, which):
        return hot_copy(q, which, onward, 0)

    def mirror(q, which):
        return hot_copy(q, which, sib, 8)

    def light_part(ref, base, piece):
        if piece == 0:
            return ref.at[pl.ds(base, hot_lane)]
        return ref.at[pl.ds(base + hot_lane, lane_rows - hot_lane)]

    def light_area(which, k, piece):
        base = 3 * parts + (k - 1) * cap + lane_rows * c
        return light_part((all_k, all_v)[which], base, piece)

    def light(k, which, piece):
        i = ((k - 1) * 2 + which) * 2 + piece
        return push(
            light_part((send_k, send_v)[which].at[k - 1], 0, piece),
            light_area(which, k, piece),
            li_send.at[i], li_recv.at[i], (xn, yn, dn)[k - 1], me_t,
        )

    def light_mirror(k, which, piece):
        i = 12 + ((k - 1) * 2 + which) * 2 + piece
        area = light_area(which, k, piece)
        return push(area, area, li_send.at[i], li_recv.at[i], sib, me_t)

    def send_lights(when, kinds, pieces):
        @pl.when(when)
        def _():
            for k in kinds:
                for piece in range(pieces):
                    for which in range(2):
                        light(k, which, piece).start()

    def arrived(k):
        for which in range(2):
            light(k, which, 0).wait_recv()
            light_mirror(k, which, 0).start()

        @pl.when(rel != k)
        def _():
            for which in range(2):
                light(k, which, 1).wait_recv()
                light_mirror(k, which, 1).start()

    @pl.when(pos == 0)
    def _():
        for i in range(hot_rows):
            at = tab[2, 0] + hot_rows * c + i
            all_k[2 * parts + hot_rows * c + i] = chip_k[at]
            all_v[2 * parts + hot_rows * c + i] = chip_v[at]
            if i % chunk == chunk - 1:
                for which in range(2):
                    forward(i // chunk, which).start()

    def gather(i, carry):
        at = tab[0, (i // lane_rows + 1) * cap + lane_rows * c + i % lane_rows]
        send_k[i // lane_rows, i % lane_rows] = chip_k[at]
        send_v[i // lane_rows, i % lane_rows] = chip_v[at]
        return carry

    lax.fori_loop(0, 3 * lane_rows, gather, 0)
    send_lights((pos == 1) & (rel == 1), (1,), 2)
    send_lights((pos == 1) & (rel == 2), (2,), 2)
    send_lights((pos == 3) & (rel == 1), (2, 1), 2)
    send_lights((pos == 3) & (rel == 2), (1, 2), 2)
    send_lights(pos == 2, (3, 2, 1), 2)
    send_lights((pos == 0) & (c == 0), (3, 1), 1)
    send_lights((pos == 0) & (c == 1), (2,), 1)
    both_k = fetch(7, chip_k, all_k.at[pl.ds(0, 2 * parts)])
    both_v = fetch(8, chip_v, all_v.at[pl.ds(0, 2 * parts)])

    def relay(*list_of):
        for where, q in list_of:

            @pl.when(pos == where)
            def _():
                for which in range(2):
                    forward(q, which).wait_recv()
                    if where < 3:
                        forward(q, which).start()
                    mirror(q, which).start()

    relay((1, 0))
    relay((1, 1))
    own_act.wait()
    for copy in acts:
        copy.wait()

    def features(t):
        return jnp.concatenate([act_part[t], act_all[t]], 0).astype(f32)

    square = jnp.zeros((rows, 1), f32)
    for t in range(tps):
        u = features(t)
        square = square + jnp.sum(u * u, -1, keepdims=True)
    inv = lax.rsqrt(square / (width * tps) + 1e-05)
    normed = []
    for t in range(tps):
        u = features(t)
        normed.append((u * inv * gain[:, t * width : (t + 1) * width]).astype(bf16))

    def project(w):
        total = None
        for t in range(tps):
            part = jnp.dot(
                normed[t], w[t * width : (t + 1) * width, :], preferred_element_type=f32
            )
            total = part if total is None else total + part
        return total

    cos_t, sin_t = cosine[...], sine[...]

    def turn(u):
        return u * cos_t + pltpu.roll(u, HD // 2, 1) * sin_t

    load_k.wait()
    load_v.wait()
    keys = project(wk_v)
    fresh = pair_f.at[0]
    for g in range(groups):
        fresh[:, g * HD : (g + 1) * HD] = turn(keys[:, g * HD : (g + 1) * HD]).astype(bf16)
    fresh[:, kvw:] = project(wv_v).astype(bf16)

    swap_f = push(fresh, pair_f.at[1], fr_send.at[0], fr_recv.at[0], sib, me_t)
    swap_f.start()

    def light_fresh(k):
        return push(
            send_f.at[k - 1], light_f.at[k - 1, c], fr_send.at[k], fr_recv.at[k],
            (xn, yn, dn)[k - 1], me_t,
        )

    def hot_fresh(k):
        return push(
            send_f.at[pl.ds(4, 2)], hot_f.at[c], fr_send.at[3 + k], fr_recv.at[3 + k],
            (xn, yn, dn)[k - 1], me_t,
        )

    def light_fresh_mirror(k):
        area = light_f.at[k - 1, c]
        return push(area, area, fr_send.at[6 + k], fr_recv.at[6 + k], sib, me_t)

    def hot_fresh_mirror():
        return push(hot_f.at[c], hot_f.at[c], fr_send.at[10], fr_recv.at[10], sib, me_t)

    load_q.wait()
    query = project(wq_v)
    for h in range(groups * per):
        g, j = h // per, h % per
        turned = turn(query[:, h * HD : (h + 1) * HD])
        for s in range(steps):
            qs[g, :, s * per + j, :] = turned[s * parts : (s + 1) * parts]
    relay((1, 2), (2, 0))

    lines = parts * pack
    row = lax.broadcasted_iota(jnp.int32, (lines, rows), 0)
    col = lax.broadcasted_iota(jnp.int32, (lines, rows), 1)
    allowed = (row // pack == col % parts) & (col // parts <= (row % pack) // per)
    scale = HD**0.5
    for g in range(groups):
        lanes = slice(g * HD, (g + 1) * HD)
        qg = qs[g].reshape(lines, HD).astype(bf16)
        for n in range(parts):
            sc1[g, n * pack : (n + 1) * pack, :] = lax.dot_general(
                qg[n * pack : (n + 1) * pack], chip_k[n, :, lanes],
                (((1,), (1,)), ((), ())), preferred_element_type=f32,
            )
        near = lax.dot_general(
            qg, fresh[:, lanes], (((1,), (1,)), ((), ())), preferred_element_type=f32
        )
        near = jnp.where(allowed, near / scale, -jnp.inf)
        far = sc1[g] / scale
        top = jnp.maximum(
            jnp.max(far, -1, keepdims=True), jnp.max(near, -1, keepdims=True)
        )
        far = jnp.exp(far - top)
        near = jnp.exp(near - top)
        mass = jnp.sum(far, -1, keepdims=True) + jnp.sum(near, -1, keepdims=True)
        far = (far / mass).astype(bf16)
        near = (near / mass).astype(bf16)
        extra = jnp.dot(
            near, fresh[:, kvw + g * HD : kvw + (g + 1) * HD], preferred_element_type=f32
        )
        for n in range(parts):
            part = slice(n * pack, (n + 1) * pack)
            cx[g, n] = extra[part] + jnp.dot(
                far[part], chip_v[n, :, lanes], preferred_element_type=f32
            )
    for h in range(groups * per):
        g, j = h // per, h % per
        for s in range(steps):
            ctx_b[s * parts : (s + 1) * parts, h * HD : (h + 1) * HD] = cx[
                g, :, s * per + j, :
            ].astype(bf16)
    load_o.wait()

    def mix(p):
        return jnp.dot(
            ctx_b[...], wo_v[:, pl.ds(pl.multiple_of(p * width, HD), width)],
            preferred_element_type=f32,
        )

    lane = lax.broadcasted_iota(jnp.int32, (rows, HD), 1)
    line = lax.broadcasted_iota(jnp.int32, (rows, HD), 0)

    def flat(column, start=0):
        return jnp.sum(jnp.where(lane == line + start, column, 0.0), 0, keepdims=True)

    count = table.shape[0]
    deep = lax.broadcasted_iota(jnp.int32, (rows, parts), 0) % parts
    broad = lax.broadcasted_iota(jnp.int32, (rows, parts), 1)
    names = jnp.concatenate(
        [jnp.broadcast_to(tokens[s : s + 1, :], (parts, parts)) for s in range(steps)], 0
    )
    name = jnp.sum(jnp.where(deep == broad, names, 0).astype(f32), -1, keepdims=True)
    name = name.astype(jnp.int32)
    entry = lax.broadcasted_iota(jnp.int32, (rows, count), 1)
    found = jnp.dot(
        (entry == name // HD).astype(f32).astype(bf16), table[...], preferred_element_type=f32
    )
    gift = flat(jnp.sum(jnp.where(lane == name % HD, found, 0.0), -1, keepdims=True))
    lw_all[me_d] = jnp.full((8, HD), -jnp.inf, f32)

    sums = []
    for k in (2, 1, 3)[: tps - 1]:
        rs_send[k - 1] = mix((me_t + k) % tps).astype(bf16)
        sums.append(tp_push(tps - 1, k, rs_send.at[k - 1], rs_recv.at[k - 1]))
    head = mix(me_t)
    swap_f.wait_recv()
    pair = pair_f[...].reshape(2 * rows, 2 * kvw)
    index = lax.broadcasted_iota(jnp.int32, (2 * rows, HD), 0)
    pick = (index == tabv[5:6, :]).astype(f32).astype(bf16)
    send_f[...] = lax.dot_general(
        pick, pair, (((0,), (0,)), ((), ())), preferred_element_type=f32
    ).astype(bf16).reshape(send_f.shape)
    for k in (3, 1, 2):
        light_fresh(k).start()

    @pl.when(pos == 0)
    def _():
        hot_f[...] = jnp.zeros(hot_f.shape, bf16)
        for k in (3, 1, 2):
            hot_fresh(k).start()

    relay((1, 3), (2, 1))
    send_lights((pos == 0) & (c == 0), (2,), 1)
    send_lights((pos == 0) & (c == 1), (3, 1), 1)
    send_lights((pos == 1) & (rel == 1), (3, 2), 2)
    send_lights((pos == 1) & (rel == 2), (3, 1), 2)
    send_lights(pos == 3, (3,), 2)
    relay((2, 2))
    relay((2, 3), (3, 0))
    for copy in sums:
        copy.wait()
    for k in range(1, tps):
        head = head + rs_recv[k - 1].astype(f32)
    attn_out[...] = head.astype(bf16)
    summed = features(me_t) + head
    along = jnp.sum(summed * twist[...], -1, keepdims=True)
    energy = jnp.sum(summed * summed, -1, keepdims=True)
    sc_all[me_t] = jnp.broadcast_to(flat(along) + flat(energy, HD // 2), (8, HD))
    scores = [
        tp_push(2 * (tps - 1), k, sc_all.at[me_t], sc_all.at[me_t]) for k in range(1, tps)
    ]
    relay((3, 1))
    for copy in scores:
        copy.wait()
    both = sc_all[0]
    for t in range(1, tps):
        both = both + sc_all[t]
    power = pltpu.roll(both, HD // 2, 1)
    score = both / jnp.sqrt(power / (width * tps) + 1e-06)
    score = jnp.where(lane[:8] < rows, score + gift, 0.0)
    total = score
    for s in range(1, steps):
        total = total + pltpu.roll(score, HD - s * parts, 1)
    mine = total[:, :parts] + jnp.broadcast_to(prev[...], (8, parts))
    lw_all[me_d, :, :parts] = mine
    lws = []
    for k in range(1, doms):
        copy = push(
            lw_all.at[me_d], lw_all.at[me_d], lw_send.at[k - 1], lw_recv.at[k - 1],
            (me_d + k) % doms, me_t,
        )
        copy.start()
        lws.append(copy)

    arrived(2)
    arrived(1)
    relay((3, 2))
    for k in (1, 2, 3):
        light_fresh(k).wait_recv()
        light_fresh_mirror(k).start()

        @pl.when(rel == k)
        def _():
            hot_fresh(k).wait_recv()
            hot_fresh_mirror().start()

    arrived(3)
    relay((3, 3))
    for k in (1, 2, 3):
        light_fresh_mirror(k).wait()

    @pl.when(pos > 0)
    def _():
        hot_fresh_mirror().wait()

    pool = jnp.concatenate(
        [
            pair_f[...].reshape(2 * rows, 2 * kvw),
            hot_f[...].reshape(rows, 2 * kvw),
            light_f[...].reshape(96, 2 * kvw),
        ],
        0,
    )
    index = lax.broadcasted_iota(jnp.int32, (3 * rows + 96, HD), 0)
    pick = (index == tabv[3:4, :]).astype(f32).astype(bf16)
    chosen = lax.dot_general(
        pick, pool, (((0,), (0,)), ((), ())), preferred_element_type=f32
    ).astype(bf16)
    for i in range(parts):
        new_k[i, span:, :] = chosen[i * 8 : i * 8 + steps, :kvw]
        new_v[i, span:, :] = chosen[i * 8 : i * 8 + steps, kvw:]

    both_k.wait()
    both_v.wait()
    for k in (1, 2, 3):
        for which in range(2):
            light_mirror(k, which, 0).wait()

        @pl.when(rel != k)
        def _():
            for which in range(2):
                light_mirror(k, which, 1).wait()

    @pl.when(pos > 0)
    def _():
        for q in range(4):
            for which in range(2):
                mirror(q, which).wait()

    def place(i, carry):
        at = tab[1, i]
        new_k[i, :span, :] = all_k[at]
        new_v[i, :span, :] = all_v[at]
        return carry

    lax.fori_loop(0, parts, place, 0)

    for copy in lws:
        copy.wait()
    every_lw = lw_all[:, 0, :]
    largest = jnp.max(every_lw, (0, 1), keepdims=True)
    mass = jnp.sum(jnp.exp(every_lw - largest), (0, 1), keepdims=True)
    out_lw[...] = mine[:1] - (largest + jnp.log(mass))

    @pl.when(pos < 3)
    def _():
        for q in range(4):
            for which in range(2):
                forward(q, which).wait_send()

    for k in (1, 2, 3):
        for which in range(2):
            light(k, which, 0).wait_send()

    @pl.when(pos > 0)
    def _():
        for k in (1, 2, 3):
            for which in range(2):
                light(k, which, 1).wait_send()

    for k in (1, 2, 3):
        light_fresh(k).wait_send()
    swap_f.wait_send()

    @pl.when(pos == 0)
    def _():
        for k in (1, 2, 3):
            hot_fresh(k).wait_send()


def adaptive(
    activations, norm_gain, w_query, w_key, value_weight, w_output, cache_keys, cache_values,
    tokens, twisting_table, twist_vec, previous_log_weights, copy_counts,
):
    f32, bf16 = jnp.float32, jnp.bfloat16
    steps, parts, width = activations.shape
    rows = steps * parts
    span = cache_keys.shape[1]
    kvw = w_key.shape[1]
    qw = w_query.shape[1]
    groups = kvw // HD
    pack = steps * (qw // kvw)
    doms = lax.axis_size("dom")
    tps = lax.axis_size("tp")
    middle = HD // 2
    cap = CAP
    angles = (span + np.arange(rows) // parts)[:, None] * (
        500000.0 ** (-2.0 * np.arange(middle) / HD)
    )
    cosine = np.concatenate([np.cos(angles)] * 2, 1).astype(np.float32)
    sine = np.concatenate([-np.sin(angles), np.sin(angles)], 1).astype(np.float32)
    vmem = pl.BlockSpec(memory_space=pltpu.VMEM)
    smem = pl.BlockSpec(memory_space=pltpu.SMEM)
    hbm = pl.BlockSpec(memory_space=pl.ANY)
    dma = pltpu.SemaphoreType.DMA
    both = jax.ShapeDtypeStruct((2 * parts, span, kvw), bf16)
    tab, chip_k, chip_v, act_part = pl.pallas_call(
        functools.partial(plan_kernel, parts, doms, tps, cap, HOT_CAP, steps, rows),
        out_shape=(
            jax.ShapeDtypeStruct((8, HD), jnp.int32), both, both,
            jax.ShapeDtypeStruct((tps, EARLY * parts, width), bf16),
        ),
        in_specs=[vmem, hbm, hbm, hbm],
        out_specs=(vmem,) * 4,
        scratch_shapes=[
            pltpu.VMEM((doms, 8, HD), f32),
            dma((doms - 1,)), dma((doms - 1,)), dma((3,)), dma((2,)), dma((2,)),
            dma((tps - 1,)), dma((tps - 1,)),
        ],
        compiler_params=pltpu.CompilerParams(
            collective_id=5, has_side_effects=True, vmem_limit_bytes=16 << 20
        ),
        name="plan",
    )(copy_counts.reshape(1, parts), activations.reshape(rows, width), cache_keys, cache_values)

    def hot_branch(hot):
        result = jax.ShapeDtypeStruct((parts, span + steps, kvw), bf16)
        call = pl.pallas_call(
            functools.partial(main_kernel, steps, parts, doms, tps, cap, HOT_CAP, hot),
            out_shape=(
                jax.ShapeDtypeStruct((rows, width), bf16), result, result,
                jax.ShapeDtypeStruct((1, parts), f32),
            ),
            in_specs=[hbm, vmem, vmem] + [hbm] * 4 + [vmem] * 8 + [smem, vmem],
            out_specs=(vmem,) * 4,
            scratch_shapes=[
                pltpu.VMEM((tps, rows - EARLY * parts, width), bf16),
                pltpu.VMEM(w_query.shape, bf16),
                pltpu.VMEM(w_key.shape, bf16),
                pltpu.VMEM(value_weight.shape, bf16),
                pltpu.VMEM(w_output.shape, bf16),
                pltpu.VMEM((3 * parts + 3 * cap, span, kvw), bf16),
                pltpu.VMEM((3 * parts + 3 * cap, span, kvw), bf16),
                pltpu.VMEM((3, cap // 2, span, kvw), bf16),
                pltpu.VMEM((3, cap // 2, span, kvw), bf16),
                pltpu.VMEM((groups, parts, pack, HD), f32),
                pltpu.VMEM((groups, parts, pack, HD), f32),
                pltpu.VMEM((groups, parts * pack, span), f32),
                pltpu.VMEM((rows, qw), bf16),
                pltpu.VMEM((2, rows, 2 * kvw), bf16),
                pltpu.VMEM((2, 2, 16, 2 * kvw), bf16),
                pltpu.VMEM((3, 2, 16, 2 * kvw), bf16),
                pltpu.VMEM((8, 16, 2 * kvw), bf16),
                pltpu.VMEM((tps - 1, rows, width), bf16),
                pltpu.VMEM((tps - 1, rows, width), bf16),
                pltpu.VMEM((tps, 8, HD), f32),
                pltpu.VMEM((doms, 8, HD), f32),
                dma((9,)),
                dma((3 * (tps - 1),)), dma((3 * (tps - 1),)),
                dma((doms - 1,)), dma((doms - 1,)),
                dma((16,)), dma((16,)),
                dma((24,)), dma((24,)),
                dma((11,)), dma((11,)),
            ],
            compiler_params=pltpu.CompilerParams(
                collective_id=hot, has_side_effects=True, vmem_limit_bytes=42 << 20
            ),
            name=f"main{hot}",
        )

        def run(
            act, act_part, gain, wq, wk, wv, wo, chip_k, chip_v, twist, tokens, table, prev,
            cosine, sine, tab, ck, cv, counts,
        ):
            return call(
                act, act_part, gain, wq, wk, wv, wo, chip_k, chip_v, twist, tokens, table,
                prev, cosine, sine, tab, tab,
            )

        return run

    def every(
        act, act_part, gain, wq, wk, wv, wo, chip_k, chip_v, twist, tokens, table, prev,
        cosine, sine, tab, ck, cv, counts,
    ):
        reward = jnp.sum(table.reshape(-1)[tokens].astype(f32), 0)
        aux = jnp.stack([prev[0] + reward, counts.astype(f32)], 1)
        attn, new_k, new_v, out_lw = all_rows(
            steps, parts, act, gain, wq, wk, wv, wo, ck, cv, twist, aux, cosine, sine
        )
        return attn, new_k, new_v, out_lw[:, 0].reshape(1, parts)

    attn, new_k, new_v, out_lw = lax.switch(
        tab[4, 0],
        [hot_branch(hot) for hot in range(4)] + [every],
        activations.reshape(rows, width), act_part, norm_gain.reshape(1, -1), w_query, w_key,
        value_weight, w_output, chip_k, chip_v, twist_vec.reshape(1, -1), tokens,
        twisting_table.reshape(-1, HD), previous_log_weights.reshape(1, parts),
        jnp.asarray(cosine), jnp.asarray(sine), tab, cache_keys, cache_values, copy_counts,
    )
    return attn.reshape(steps, parts, width), new_k, new_v, out_lw.reshape(parts)


def solution(mesh):
    body = adaptive if (mesh.shape["dom"], mesh.shape["tp"]) == (8, 4) else local
    return jax.shard_map(
        body,
        mesh=mesh,
        in_specs=(
            P(None, "dom", "tp"),
            P(),
            P(None, "tp"),
            P(None, "tp"),
            P(None, "tp"),
            P("tp", None),
            P("dom", None, "tp"),
            P("dom", None, "tp"),
            P(None, "dom"),
            P(),
            P("tp"),
            P("dom"),
            P("dom"),
        ),
        out_specs=(P(None, "dom", "tp"), P("dom", None, "tp"), P("dom", None, "tp"), P("dom")),
        check_vma=False,
    )
```

```python
import functools

import jax
import jax.numpy as jnp
import numpy as np
from jax import lax
from jax.experimental import pallas as pl
from jax.experimental.pallas import tpu as pltpu
from jax.sharding import PartitionSpec as P

D = 4096
HD = 128
CAP = 6
HOT_CAP = 4
EARLY = 1


def rotate(tensor, positions):
    middle = tensor.shape[-1] // 2
    frequency = 500000.0 ** (-2.0 * jnp.arange(middle, dtype=jnp.float32) / tensor.shape[-1])
    angles = positions[:, None] * frequency[None, :]
    cosine = jnp.cos(angles)[:, None, None, :]
    sine_part = jnp.sin(angles)[:, None, None, :]
    lower_half = tensor[..., :middle]
    upper_half = tensor[..., middle:]
    return jnp.concatenate(
        [
            lower_half * cosine - upper_half * sine_part,
            upper_half * cosine + lower_half * sine_part,
        ],
        -1,
    )


def local(
    activations,
    norm_gain,
    w_query,
    w_key,
    value_weight,
    w_output,
    cache_keys,
    cache_values,
    tokens,
    twisting_table,
    twist_vec,
    previous_log_weights,
    copy_counts,
):
    step_count = activations.shape[0]
    particle_count = activations.shape[1]
    span_old = cache_keys.shape[1]
    dom_size = lax.axis_size("dom")
    kv_local = w_key.shape[1] // HD
    q_local = w_query.shape[1] // HD
    group_size = q_local // kv_local
    all_counts = lax.all_gather(copy_counts, "dom", axis=0, tiled=True)
    copy_ends = jnp.cumsum(all_counts)
    ranks = jnp.arange(particle_count, dtype=jnp.int32) * dom_size + lax.axis_index("dom")
    ancestor = jnp.sum((copy_ends[None, :] <= ranks[:, None]).astype(jnp.int32), 1)
    all_keys = lax.all_gather(cache_keys, "dom", axis=0, tiled=True)
    all_values = lax.all_gather(cache_values, "dom", axis=0, tiled=True)

    gathered = lax.all_gather(activations, "tp", axis=2, tiled=True)
    inputs = gathered.astype(jnp.float32)
    normed = (
        inputs * lax.rsqrt(jnp.mean(inputs * inputs, -1, keepdims=True) + 1e-05) * norm_gain
    ).astype(jnp.bfloat16)
    flat_rows = normed.reshape(step_count * particle_count, D)
    positions = (span_old + jnp.arange(step_count, dtype=jnp.int32)).astype(jnp.float32)
    queries = jnp.dot(flat_rows, w_query, preferred_element_type=jnp.float32).reshape(
        step_count, particle_count, q_local, HD
    )
    queries = rotate(queries, positions).astype(jnp.bfloat16)
    fresh_keys = jnp.dot(flat_rows, w_key, preferred_element_type=jnp.float32).reshape(
        step_count, particle_count, kv_local, HD
    )
    fresh_keys = (
        rotate(fresh_keys, positions)
        .astype(jnp.bfloat16)
        .reshape(step_count, particle_count, kv_local * HD)
    )
    fresh_values = jnp.dot(flat_rows, value_weight, preferred_element_type=jnp.float32).astype(
        jnp.bfloat16
    )
    fresh_values = fresh_values.reshape(step_count, particle_count, kv_local * HD)
    fresh_keys = jnp.transpose(fresh_keys, (1, 0, 2))
    fresh_values = jnp.transpose(fresh_values, (1, 0, 2))
    key_rows = jnp.concatenate([cache_keys, fresh_keys], 1)
    value_rows = jnp.concatenate([cache_values, fresh_values], 1)
    key_span = span_old + step_count
    query_heads = queries.reshape(step_count, particle_count, kv_local, group_size, HD)
    key_heads = key_rows.reshape(particle_count, key_span, kv_local, HD)
    value_heads = value_rows.reshape(particle_count, key_span, kv_local, HD)
    scores = (
        jnp.einsum("snkgd,nlkd->snkgl", query_heads, key_heads, preferred_element_type=jnp.float32)
        / HD**0.5
    )
    allowed = (
        jnp.arange(key_span, dtype=jnp.int32)[None, :]
        <= (span_old + jnp.arange(step_count, dtype=jnp.int32))[:, None]
    )
    allowed = allowed[:, None, None, None, :]
    masked = jnp.where(allowed, scores, -jnp.inf)
    highest = jnp.max(masked, -1, keepdims=True)
    exponent = jnp.exp(masked - highest)
    weights = (exponent / jnp.sum(exponent, -1, keepdims=True)).astype(jnp.bfloat16)
    context = jnp.einsum(
        "snkgl,nlkd->snkgd", weights, value_heads, preferred_element_type=jnp.float32
    ).astype(jnp.bfloat16)
    context = context.reshape(step_count * particle_count, q_local * HD)
    partial_value = jnp.dot(context, w_output, preferred_element_type=jnp.float32).reshape(
        step_count, particle_count, D
    )
    head_mix = lax.psum_scatter(partial_value, "tp", scatter_dimension=2, tiled=True)
    attn_out = head_mix.astype(jnp.bfloat16)
    summed = activations.astype(jnp.float32) + head_mix
    aligned, energy = lax.psum(
        (jnp.sum(summed * twist_vec, -1), jnp.sum(summed * summed, -1)), "tp"
    )
    twisting_score = aligned / jnp.sqrt(energy / D + 1e-06)
    token_reward = twisting_table[tokens].astype(jnp.float32)
    particle_log_weight = previous_log_weights + jnp.sum(token_reward + twisting_score, 0)
    largest = lax.pmax(jnp.max(particle_log_weight), "dom")
    mass_total = lax.psum(jnp.sum(jnp.exp(particle_log_weight - largest)), "dom")
    out_logw = particle_log_weight - (largest + jnp.log(mass_total))
    fresh = lax.all_gather(
        jnp.concatenate([fresh_keys, fresh_values], 2), "dom", axis=0, tiled=True
    )[ancestor]
    width = fresh_keys.shape[2]
    new_keys = jnp.concatenate([all_keys[ancestor], fresh[..., :width]], 1)
    new_values = jnp.concatenate([all_values[ancestor], fresh[..., width:]], 1)
    return (attn_out, new_keys, new_values, out_logw)


MESH = pl.DeviceIdType.MESH


def layer_kernel(
    steps, parts, doms, tps,
    act, gain, wq, wk, wv, wo, ck, cv, twist, aux, cosine, sine,
    attn_out, all_k, all_v, fresh_sel, out_lw, anc_out,
    act_all, wq_v, wk_v, wv_v, wo_v, ck_v, cv_v, qs, cx, sc1, ctx_b, fresh, fresh_all,
    rs_send, rs_recv, sc_all, lw_all, cnt_all,
    loc, tp_send, tp_recv, dom_send, dom_recv, blk_send, blk_recv,
):
    f32, bf16 = jnp.float32, jnp.bfloat16
    me_d = lax.axis_index("dom")
    me_t = lax.axis_index("tp")
    rows, width = act.shape
    half = parts // 2
    kvw = wk.shape[1]
    groups = kvw // HD
    per = wq.shape[1] // kvw
    pack = steps * per
    c = me_d % 2
    x = (me_d // 2) % 2
    y = me_d // 4
    sib = me_d + 1 - 2 * c
    xn = me_d + 2 - 4 * x
    yn = me_d + 4 - 8 * y
    dn = xn + 4 - 8 * y

    barrier = pltpu.get_barrier_semaphore()
    for k in range(1, tps):
        pl.semaphore_signal(
            barrier, inc=1, device_id=(me_d, (me_t + k) % tps), device_id_type=MESH
        )
    for k in range(1, doms):
        pl.semaphore_signal(
            barrier, inc=1, device_id=((me_d + k) % doms, me_t), device_id_type=MESH
        )

    def fetch(i, src, dst):
        copy = pltpu.make_async_copy(src, dst, loc.at[i])
        copy.start()
        return copy

    own_act = fetch(0, act, act_all.at[me_t])
    load_q = fetch(1, wq, wq_v)
    load_k = fetch(2, wk, wk_v)
    load_v = fetch(3, wv, wv_v)
    load_ck = fetch(4, ck, ck_v)
    load_cv = fetch(5, cv, cv_v)
    load_o = fetch(6, wo, wo_v)

    cnt_all[me_d] = jnp.broadcast_to(aux[:, 1:], cnt_all.shape[1:])
    pl.semaphore_wait(barrier, tps + doms - 2)

    def tp_push(base, k, src, dst):
        copy = pltpu.make_async_remote_copy(
            src_ref=src, dst_ref=dst, send_sem=tp_send.at[base + k - 1],
            recv_sem=tp_recv.at[base + k - 1],
            device_id=(me_d, (me_t + k) % tps), device_id_type=MESH,
        )
        copy.start()
        return copy

    def dom_push(base, k, src, dst):
        copy = pltpu.make_async_remote_copy(
            src_ref=src, dst_ref=dst, send_sem=dom_send.at[base + k - 1],
            recv_sem=dom_recv.at[base + k - 1],
            device_id=((me_d + k) % doms, me_t), device_id_type=MESH,
        )
        copy.start()
        return copy

    acts = [tp_push(0, k, act, act_all.at[me_t]) for k in range(1, tps)]

    def piece(kind, to, which, h, slot, own):
        dst = (all_k, all_v)[which].at[slot, pl.ds(h * half, half)]
        src = (ck, cv)[which].at[pl.ds(h * half, half)] if own else dst
        i = kind * 4 + h * 2 + which
        copy = pltpu.make_async_remote_copy(
            src_ref=src, dst_ref=dst, send_sem=blk_send.at[i], recv_sem=blk_recv.at[i],
            device_id=(to, me_t), device_id_type=MESH,
        )
        copy.start()
        return copy

    moves = {}
    for h, kind, to in ((0, 0, xn), (1, 1, yn), (1, 0, xn), (0, 1, yn)):
        for which in range(2):
            moves[kind, h, which] = piece(kind, to, which, h, me_d, True)
    cnts = [dom_push(0, k, cnt_all.at[me_d], cnt_all.at[me_d]) for k in range(1, doms)]
    for h in range(2):
        for which in range(2):
            moves[3, h, which] = piece(3, sib, which, h, me_d, True)

    own_act.wait()
    for copy in acts:
        copy.wait()
    square = jnp.zeros((rows, 1), f32)
    for t in range(tps):
        u = act_all[t].astype(f32)
        square = square + jnp.sum(u * u, -1, keepdims=True)
    inv = lax.rsqrt(square / (width * tps) + 1e-05)
    normed = []
    for t in range(tps):
        u = act_all[t].astype(f32)
        normed.append((u * inv * gain[:, t * width : (t + 1) * width]).astype(bf16))

    def project(w):
        total = None
        for t in range(tps):
            part = jnp.dot(
                normed[t], w[t * width : (t + 1) * width, :], preferred_element_type=f32
            )
            total = part if total is None else total + part
        return total

    cos_t, sin_t = cosine[...], sine[...]

    def turn(u):
        return u * cos_t + pltpu.roll(u, HD // 2, 1) * sin_t

    load_k.wait()
    load_v.wait()
    keys = project(wk_v)
    for g in range(groups):
        fresh[:, g * HD : (g + 1) * HD] = turn(keys[:, g * HD : (g + 1) * HD]).astype(bf16)
    fresh[:, kvw:] = project(wv_v).astype(bf16)
    fresh_all[me_d] = fresh[...]
    news = [dom_push(doms - 1, k, fresh, fresh_all.at[me_d]) for k in range(1, doms)]
    load_q.wait()
    query = project(wq_v)
    for h in range(groups * per):
        g, j = h // per, h % per
        turned = turn(query[:, h * HD : (h + 1) * HD])
        for s in range(steps):
            qs[g, :, s * per + j, :] = turned[s * parts : (s + 1) * parts]
    load_ck.wait()
    load_cv.wait()
    put_k = fetch(7, ck_v, all_k.at[me_d])
    put_v = fetch(8, cv_v, all_v.at[me_d])

    lines = parts * pack
    row = lax.broadcasted_iota(jnp.int32, (lines, rows), 0)
    col = lax.broadcasted_iota(jnp.int32, (lines, rows), 1)
    allowed = (row // pack == col % parts) & (col // parts <= (row % pack) // per)
    scale = HD**0.5
    for g in range(groups):
        lanes = slice(g * HD, (g + 1) * HD)
        qg = qs[g].reshape(lines, HD).astype(bf16)
        for n in range(parts):
            sc1[g, n * pack : (n + 1) * pack, :] = lax.dot_general(
                qg[n * pack : (n + 1) * pack], ck_v[n, :, lanes],
                (((1,), (1,)), ((), ())), preferred_element_type=f32,
            )
        near = lax.dot_general(
            qg, fresh[:, lanes], (((1,), (1,)), ((), ())), preferred_element_type=f32
        )
        near = jnp.where(allowed, near / scale, -jnp.inf)
        far = sc1[g] / scale
        top = jnp.maximum(
            jnp.max(far, -1, keepdims=True), jnp.max(near, -1, keepdims=True)
        )
        far = jnp.exp(far - top)
        near = jnp.exp(near - top)
        mass = jnp.sum(far, -1, keepdims=True) + jnp.sum(near, -1, keepdims=True)
        far = (far / mass).astype(bf16)
        near = (near / mass).astype(bf16)
        extra = jnp.dot(
            near, fresh[:, kvw + g * HD : kvw + (g + 1) * HD], preferred_element_type=f32
        )
        for n in range(parts):
            span = slice(n * pack, (n + 1) * pack)
            cx[g, n] = extra[span] + jnp.dot(
                far[span], cv_v[n, :, lanes], preferred_element_type=f32
            )
    for h in range(groups * per):
        g, j = h // per, h % per
        for s in range(steps):
            ctx_b[s * parts : (s + 1) * parts, h * HD : (h + 1) * HD] = cx[
                g, :, s * per + j, :
            ].astype(bf16)
    load_o.wait()

    def mix(p):
        return jnp.dot(
            ctx_b[...], wo_v[:, pl.ds(pl.multiple_of(p * width, HD), width)],
            preferred_element_type=f32,
        )

    sums = []
    for k in range(1, tps):
        rs_send[k - 1] = mix((me_t + k) % tps)
        sums.append(tp_push(tps - 1, k, rs_send.at[k - 1], rs_recv.at[k - 1]))
    head = mix(me_t)

    def done(kind, h):
        for which in range(2):
            moves[kind, h, which].wait_recv()

    def relay(kind, to, h, slot):
        for which in range(2):
            moves[kind, h, which] = piece(kind, to, which, h, slot, False)

    done(0, 0)
    relay(2, yn, 0, xn)
    relay(4, sib, 0, xn)
    done(1, 1)
    relay(6, xn, 1, yn)
    relay(5, sib, 1, yn)
    for k in range(1, tps):
        sums[k - 1].wait()
        head = head + rs_recv[k - 1]
    attn_out[...] = head.astype(bf16)
    summed = act_all[me_t].astype(f32) + head
    along = jnp.sum(summed * twist[...], -1, keepdims=True)
    energy = jnp.sum(summed * summed, -1, keepdims=True)
    lane = lax.broadcasted_iota(jnp.int32, (rows, HD), 1)
    sc_all[me_t] = jnp.where(lane < HD // 2, along, energy)
    scores = [
        tp_push(2 * (tps - 1), k, sc_all.at[me_t], sc_all.at[me_t]) for k in range(1, tps)
    ]
    for copy in scores:
        copy.wait()
    both = sc_all[0]
    for t in range(1, tps):
        both = both + sc_all[t]
    score = both[:, :1] / jnp.sqrt(both[:, HD - 1 :] / (width * tps) + 1e-06)
    total = score[:parts]
    for s in range(1, steps):
        total = total + score[s * parts : (s + 1) * parts]
    mine = jnp.broadcast_to(aux[:, :1] + total, (parts, HD))
    lw_all[me_d] = mine
    lws = [
        dom_push(2 * (doms - 1), k, lw_all.at[me_d], lw_all.at[me_d]) for k in range(1, doms)
    ]

    done(0, 1)
    relay(4, sib, 1, xn)
    done(1, 0)
    relay(5, sib, 0, yn)

    for copy in cnts:
        copy.wait()
    for copy in news:
        copy.wait()
    whole = parts * doms
    number = cnt_all[...].reshape(whole, HD).astype(bf16)
    lower = lax.broadcasted_iota(jnp.int32, (whole, whole), 0)
    upper = lax.broadcasted_iota(jnp.int32, (whole, whole), 1)
    ends = jnp.dot(
        (upper <= lower).astype(f32).astype(bf16), number, preferred_element_type=f32
    )
    slot = lax.broadcasted_iota(jnp.int32, (whole, HD), 1)

    def ancestor(place):
        rank = (place * doms + me_d).astype(f32)
        return jnp.sum((ends <= rank).astype(f32), 0, keepdims=True).astype(jnp.int32)

    anc_out[...] = jnp.broadcast_to(ancestor(slot), anc_out.shape)
    lanes = lax.broadcasted_iota(jnp.int32, (1, HD), 1)
    wide = ancestor(slot // 8)
    target = (wide // parts) * rows + (lanes % 8) * parts + wide % parts
    target = jnp.where(lanes % 8 < steps, target, -1)
    index = lax.broadcasted_iota(jnp.int32, (doms * rows, HD), 0)
    pick = (index == target).astype(f32).astype(bf16)
    fresh_sel[...] = lax.dot_general(
        pick, fresh_all[...].reshape(doms * rows, 2 * kvw),
        (((0,), (0,)), ((), ())), preferred_element_type=f32,
    ).astype(bf16)

    for copy in lws:
        copy.wait()
    largest = jnp.max(lw_all[...], (0, 1), keepdims=True)[0]
    mass = jnp.sum(jnp.exp(lw_all[...] - largest[None]), (0, 1), keepdims=True)[0]
    out_lw[...] = mine - (largest + jnp.log(mass))

    done(2, 0)
    relay_d0 = [piece(7, sib, which, 0, dn, False) for which in range(2)]
    done(6, 1)
    relay_d1 = [piece(7, sib, which, 1, dn, False) for which in range(2)]
    for kind in (3, 4, 5):
        for h in range(2):
            done(kind, h)
    for copy in moves.values():
        copy.wait_send()
    for copy in relay_d0 + relay_d1:
        copy.wait()
    put_k.wait()
    put_v.wait()


def select_kernel(
    parts, anc, fresh_sel, attn, lw, all_k, all_v,
    out_attn, new_k, new_v, chosen, out_lw, sem,
):
    copies = []
    for i in range(parts):
        a = anc[0, i]
        d, n = a // parts, a % parts
        for which, (src, dst) in enumerate(((all_k, new_k), (all_v, new_v))):
            copy = pltpu.make_async_copy(src.at[d, n], dst.at[i], sem.at[2 * i + which])
            copy.start()
            copies.append(copy)
    chosen[...] = fresh_sel[...]
    out_attn[...] = attn[...]
    row = lax.broadcasted_iota(jnp.int32, (parts, parts), 0)
    col = lax.broadcasted_iota(jnp.int32, (parts, parts), 1)
    out_lw[...] = jnp.sum(jnp.where(row == col, lw[:, :1], 0.0), 0, keepdims=True)
    for copy in copies:
        copy.wait()


def all_rows(
    steps, parts, act, gain, wq, wk, wv, wo, ck, cv, twist, aux, cosine, sine,
):
    f32, bf16 = jnp.float32, jnp.bfloat16
    rows, width = act.shape
    span = ck.shape[1]
    kvw = wk.shape[1]
    qw = wq.shape[1]
    groups = kvw // HD
    pack = steps * (qw // kvw)
    doms = lax.axis_size("dom")
    tps = lax.axis_size("tp")
    vmem = pl.BlockSpec(memory_space=pltpu.VMEM)
    hbm = pl.BlockSpec(memory_space=pl.ANY)
    block = jax.ShapeDtypeStruct((doms,) + ck.shape, bf16)
    attn, all_k, all_v, fresh_sel, out_lw, anc = pl.pallas_call(
        functools.partial(layer_kernel, steps, parts, doms, tps),
        out_shape=(
            jax.ShapeDtypeStruct((rows, width), bf16), block, block,
            jax.ShapeDtypeStruct((HD, 2 * kvw), bf16),
            jax.ShapeDtypeStruct((parts, HD), f32),
            jax.ShapeDtypeStruct((8, HD), jnp.int32),
        ),
        in_specs=[hbm, vmem] + [hbm] * 6 + [vmem] * 4,
        out_specs=(vmem, hbm, hbm, vmem, vmem, vmem),
        scratch_shapes=[
            pltpu.VMEM((tps, rows, width), bf16),
            pltpu.VMEM(wq.shape, bf16),
            pltpu.VMEM(wk.shape, bf16),
            pltpu.VMEM(wv.shape, bf16),
            pltpu.VMEM(wo.shape, bf16),
            pltpu.VMEM(ck.shape, bf16),
            pltpu.VMEM(cv.shape, bf16),
            pltpu.VMEM((groups, parts, pack, HD), f32),
            pltpu.VMEM((groups, parts, pack, HD), f32),
            pltpu.VMEM((groups, parts * pack, span), f32),
            pltpu.VMEM((rows, qw), bf16),
            pltpu.VMEM((rows, 2 * kvw), bf16),
            pltpu.VMEM((doms, rows, 2 * kvw), bf16),
            pltpu.VMEM((tps - 1, rows, width), f32),
            pltpu.VMEM((tps - 1, rows, width), f32),
            pltpu.VMEM((tps, rows, HD), f32),
            pltpu.VMEM((doms, parts, HD), f32),
            pltpu.VMEM((doms, parts, HD), f32),
            pltpu.SemaphoreType.DMA((9,)),
            pltpu.SemaphoreType.DMA((3 * (tps - 1),)),
            pltpu.SemaphoreType.DMA((3 * (tps - 1),)),
            pltpu.SemaphoreType.DMA((3 * (doms - 1),)),
            pltpu.SemaphoreType.DMA((3 * (doms - 1),)),
            pltpu.SemaphoreType.DMA((32,)),
            pltpu.SemaphoreType.DMA((32,)),
        ],
        compiler_params=pltpu.CompilerParams(
            collective_id=4, has_side_effects=True, vmem_limit_bytes=52 << 20
        ),
        name="layer",
    )(act, gain, wq, wk, wv, wo, ck, cv, twist, aux, cosine, sine)
    result = jax.ShapeDtypeStruct((parts, span, kvw), bf16)
    return pl.pallas_call(
        functools.partial(select_kernel, parts),
        out_shape=(
            jax.ShapeDtypeStruct((rows, width), bf16), result, result,
            jax.ShapeDtypeStruct((HD, 2 * kvw), bf16),
            jax.ShapeDtypeStruct((1, parts), f32),
        ),
        in_specs=[pl.BlockSpec(memory_space=pltpu.SMEM), vmem, vmem, vmem, hbm, hbm],
        out_specs=(vmem,) * 5,
        scratch_shapes=[pltpu.SemaphoreType.DMA((2 * parts,))],
        compiler_params=pltpu.CompilerParams(vmem_limit_bytes=8 << 20),
        name="select",
    )(anc, fresh_sel, attn, out_lw, all_k, all_v)


def plan_kernel(
    parts, doms, tps, cap, hot_cap, steps, rows,
    cnt, act, ck, cv, tab, chip_k, chip_v, act_part,
    cnt_all, send, recv, loc, sib_send, sib_recv, tp_send, tp_recv,
):
    f32, bf16, i32 = jnp.float32, jnp.bfloat16, jnp.int32
    me_d = lax.axis_index("dom")
    me_t = lax.axis_index("tp")
    core = me_d % 2
    x = (me_d // 2) % 2
    y = me_d // 4
    chip = me_d // 2
    barrier = pltpu.get_barrier_semaphore()
    for k in range(1, tps):
        pl.semaphore_signal(
            barrier, inc=1, device_id=(me_d, (me_t + k) % tps), device_id_type=MESH
        )
    for k in range(1, doms):
        pl.semaphore_signal(
            barrier, inc=1, device_id=((me_d + k) % doms, me_t), device_id_type=MESH
        )
    owns = []
    for i, (src, dst) in enumerate(((ck, chip_k), (cv, chip_v))):
        copy = pltpu.make_async_copy(src, dst.at[pl.ds(0, parts)], loc.at[i])
        copy.start()
        owns.append(copy)
    early = act.at[pl.ds(0, act_part.shape[1])]
    copy = pltpu.make_async_copy(early, act_part.at[me_t], loc.at[2])
    copy.start()
    owns.append(copy)
    cnt_all[me_d] = jnp.zeros(cnt_all.shape[1:], f32)
    cnt_all[me_d, :, :parts] = jnp.broadcast_to(cnt[...].astype(f32), (8, parts))
    pl.semaphore_wait(barrier, tps + doms - 2)
    copies = []
    for k in range(1, doms):
        copy = pltpu.make_async_remote_copy(
            src_ref=cnt_all.at[me_d], dst_ref=cnt_all.at[me_d],
            send_sem=send.at[k - 1], recv_sem=recv.at[k - 1],
            device_id=((me_d + k) % doms, me_t), device_id_type=MESH,
        )
        copy.start()
        copies.append(copy)
    swaps = []
    for k in range(1, tps):
        copy = pltpu.make_async_remote_copy(
            src_ref=early, dst_ref=act_part.at[me_t],
            send_sem=tp_send.at[k - 1], recv_sem=tp_recv.at[k - 1],
            device_id=(me_d, (me_t + k) % tps), device_id_type=MESH,
        )
        copy.start()
        swaps.append(copy)
    for i, (src, dst) in enumerate(((ck, chip_k), (cv, chip_v))):
        copy = pltpu.make_async_remote_copy(
            src_ref=src, dst_ref=dst.at[pl.ds(parts, parts)],
            send_sem=sib_send.at[i], recv_sem=sib_recv.at[i],
            device_id=(me_d + 1 - 2 * core, me_t), device_id_type=MESH,
        )
        copy.start()
        swaps.append(copy)
    for copy in copies:
        copy.wait()
    whole = parts * doms
    j = lax.broadcasted_iota(i32, (whole, HD), 0)
    lane = lax.broadcasted_iota(i32, (whole, HD), 1)
    spread = jnp.concatenate([cnt_all[d] for d in range(doms) for _ in range(parts // 8)], 0)
    column = jnp.sum(jnp.where(lane == j % parts, spread, 0.0), -1, keepdims=True)
    number = jnp.broadcast_to(column, (whole, HD))
    first = lax.broadcasted_iota(i32, (whole, whole), 0)
    second = lax.broadcasted_iota(i32, (whole, whole), 1)

    def total(mask, values):
        return jnp.dot(
            mask.astype(f32).astype(bf16), values.astype(bf16), preferred_element_type=f32
        )

    ends = total(second <= first, number)
    loads = total(second // parts == first // parts, number)
    number = number.astype(i32)
    ends = ends.astype(i32)
    starts = ends - number
    top = jnp.max(loads, (0, 1), keepdims=True)
    owner = j // parts
    heavy = jnp.min(jnp.where(loads == top, owner, doms).astype(f32), (0, 1), keepdims=True)
    heavy = heavy.astype(i32)
    light = owner != heavy
    home = j // (2 * parts)

    def needs(to):
        hit = None
        for m in range(4):
            one = (m < number) & (((starts + m) % doms) // 2 == to)
            hit = one if hit is None else hit | one
        return hit & light & (home != to)

    kind = (lane // cap) % 4
    there_x = x + kind % 2 - 2 * x * (kind % 2)
    there_y = y + kind // 2 - 2 * y * (kind // 2)
    need_send = needs(2 * there_y + there_x)
    kind = jnp.minimum(lane // 16, 2) + 1
    there_x = x + kind % 2 - 2 * x * (kind % 2)
    there_y = y + kind // 2 - 2 * y * (kind // 2)
    need_fresh = needs(2 * there_y + there_x)
    need_here = needs(jnp.broadcast_to(chip, (whole, HD)))
    need_any = needs(lane % 4)
    before = (second < first) & (second // (2 * parts) == first // (2 * parts))
    places = total(
        before,
        jnp.concatenate([u.astype(f32) for u in (need_send, need_here, need_any, need_fresh)], 1),
    ).astype(i32)
    place_send = places[:, :HD]
    place_here = places[:, HD : 2 * HD]
    place_any = places[:, 2 * HD : 3 * HD]
    place_fresh = places[:, 3 * HD :]
    local_row = j % parts + parts * (owner % 2 + core - 2 * core * (owner % 2))
    half = cap // 2
    entry = lane % cap
    picked = need_send & (place_send == 2 * (entry % half) + entry // half) & (home == chip)
    sources = jnp.sum(jnp.where(picked, local_row, 0).astype(f32), 0, keepdims=True)
    hx, hy = home % 2, home // 2
    away = (hx + x - 2 * x * hx) + 2 * (hy + y - 2 * y * hy)
    value = jnp.where(
        away == 0,
        local_row,
        jnp.where(
            light,
            3 * parts + (away - 1) * cap + place_here % 2 * half + place_here // 2,
            2 * parts + j % parts,
        ),
    )
    rank = lane * doms + me_d
    mine = (starts <= rank) & (rank < ends)
    index = jnp.sum(jnp.where(mine, value, 0).astype(f32), 0, keepdims=True)
    deep = lane % 16 // steps
    hit = need_fresh & (place_fresh == 2 * deep + core) & (lane < 48) & (deep < half)
    hot = (owner == heavy) & (lane >= 64)
    hot = hot & (j % parts == parts // 2 * core + (lane - 64) // steps)
    hot = hot & (lane < 64 + parts // 2 * steps)
    spot = local_row // parts * rows + j % parts
    hit = (hit | hot) & (home == chip)
    picks = jnp.where(hit, spot + lane % steps * parts + 1, 0).astype(f32)
    picks = jnp.sum(picks, 0, keepdims=True).astype(i32) - 1
    wide = (lane // 8) * doms + me_d
    step = lane % 8
    spot = jnp.where(
        away == 0,
        spot + step * parts,
        jnp.where(
            light,
            3 * rows + (away - 1) * 32 + place_here % 2 * 16 + place_here // 2 * steps + step,
            2 * rows + j % parts * steps + step,
        ),
    )
    chosen = (starts <= wide) & (wide < ends) & (step < steps)
    target = jnp.where(chosen, spot + 1, 0).astype(f32)
    target = jnp.sum(target, 0, keepdims=True).astype(i32) - 1
    room = jnp.where(home == heavy // 2, hot_cap, cap)
    over = jnp.max(
        (need_any & (place_any >= room)).astype(f32), (0, 1), keepdims=True
    ).astype(i32)
    base = parts * (heavy % 2 + core - 2 * core * (heavy % 2))
    branch = jnp.where(over == 0, heavy // 2, 4)
    tab[0:1, :] = sources.astype(i32)
    tab[1:2, :] = index.astype(i32)
    tab[2:3, :] = jnp.broadcast_to(base, (1, HD))
    tab[3:4, :] = target
    tab[4:5, :] = jnp.broadcast_to(branch, (1, HD))
    tab[5:6, :] = picks
    tab[6:8, :] = jnp.zeros((2, HD), i32)
    for copy in owns + swaps:
        copy.wait()


def main_kernel(
    steps, parts, doms, tps, cap, hot_cap, hot,
    act, act_part, gain, wq, wk, wv, wo, chip_k, chip_v, twist, tokens, table, prev,
    cosine, sine, tab, tabv,
    attn_out, new_k, new_v, chosen, out_lw,
    act_all, wq_v, wk_v, wv_v, wo_v, all_k, all_v, send_k, send_v,
    qs, cx, sc1, ctx_b, pair_f, hot_f, light_f, send_f, rs_send, rs_recv, sc_all, lw_all,
    loc, tp_send, tp_recv, lw_send, lw_recv,
    hv_send, hv_recv, li_send, li_recv, fr_send, fr_recv,
):
    f32, bf16 = jnp.float32, jnp.bfloat16
    me_d = lax.axis_index("dom")
    me_t = lax.axis_index("tp")
    rows, width = act.shape
    kvw = wk.shape[1]
    groups = kvw // HD
    per = wq.shape[1] // kvw
    pack = steps * per
    span = chip_k.shape[1]
    c = me_d % 2
    x = (me_d // 2) % 2
    y = me_d // 4
    sib = me_d + 1 - 2 * c
    xn = me_d + 2 - 4 * x
    yn = me_d + 4 - 8 * y
    dn = xn + 4 - 8 * y
    rx = x if hot % 2 == 0 else 1 - x
    ry = y if hot // 2 == 0 else 1 - y
    pos = (1 - c) * (3 * ry + rx * (1 - 2 * ry)) + c * (3 * rx + ry * (1 - 2 * rx))
    turn_y = (pos + c) % 2
    onward = xn + turn_y * (yn - xn)

    barrier = pltpu.get_barrier_semaphore()
    for k in range(1, tps):
        pl.semaphore_signal(
            barrier, inc=1, device_id=(me_d, (me_t + k) % tps), device_id_type=MESH
        )
    for k in range(1, doms):
        pl.semaphore_signal(
            barrier, inc=1, device_id=((me_d + k) % doms, me_t), device_id_type=MESH
        )

    def fetch(i, src, dst):
        copy = pltpu.make_async_copy(src, dst, loc.at[i])
        copy.start()
        return copy

    first = act_part.shape[1]
    later = act.at[pl.ds(first, rows - first)]
    own_act = fetch(0, later, act_all.at[me_t])
    load_k = fetch(2, wk, wk_v)
    load_v = fetch(3, wv, wv_v)
    load_q = fetch(1, wq, wq_v)
    load_o = fetch(6, wo, wo_v)
    pl.semaphore_wait(barrier, tps + doms - 2)

    def push(src, dst, ssem, rsem, to_d, to_t):
        return pltpu.make_async_remote_copy(
            src_ref=src, dst_ref=dst, send_sem=ssem, recv_sem=rsem,
            device_id=(to_d, to_t), device_id_type=MESH,
        )

    def tp_push(base, k, src, dst):
        copy = push(
            src, dst, tp_send.at[base + k - 1], tp_recv.at[base + k - 1],
            me_d, (me_t + k) % tps,
        )
        copy.start()
        return copy

    acts = [tp_push(0, k, later, act_all.at[me_t]) for k in range(1, tps)]
    lane_rows = cap // 2
    hot_lane = hot_cap // 2
    rel = rx + 2 * ry
    hot_rows = parts // 2
    chunk = hot_rows // 4

    def hot_copy(q, which, to, base):
        ref = (all_k, all_v)[which]
        area = ref.at[pl.ds(2 * parts + hot_rows * c + q * chunk, chunk)]
        i = base + q * 2 + which
        return push(area, area, hv_send.at[i], hv_recv.at[i], to, me_t)

    def forward(q, which):
        return hot_copy(q, which, onward, 0)

    def mirror(q, which):
        return hot_copy(q, which, sib, 8)

    def light_part(ref, base, piece):
        if piece == 0:
            return ref.at[pl.ds(base, hot_lane)]
        return ref.at[pl.ds(base + hot_lane, lane_rows - hot_lane)]

    def light_area(which, k, piece):
        base = 3 * parts + (k - 1) * cap + lane_rows * c
        return light_part((all_k, all_v)[which], base, piece)

    def light(k, which, piece):
        i = ((k - 1) * 2 + which) * 2 + piece
        return push(
            light_part((send_k, send_v)[which].at[k - 1], 0, piece),
            light_area(which, k, piece),
            li_send.at[i], li_recv.at[i], (xn, yn, dn)[k - 1], me_t,
        )

    def light_mirror(k, which, piece):
        i = 12 + ((k - 1) * 2 + which) * 2 + piece
        area = light_area(which, k, piece)
        return push(area, area, li_send.at[i], li_recv.at[i], sib, me_t)

    def send_lights(when, kinds, pieces):
        @pl.when(when)
        def _():
            for k in kinds:
                for piece in range(pieces):
                    for which in range(2):
                        light(k, which, piece).start()

    def arrived(k):
        for which in range(2):
            light(k, which, 0).wait_recv()
            light_mirror(k, which, 0).start()

        @pl.when(rel != k)
        def _():
            for which in range(2):
                light(k, which, 1).wait_recv()
                light_mirror(k, which, 1).start()

    @pl.when(pos == 0)
    def _():
        for i in range(hot_rows):
            at = tab[2, 0] + hot_rows * c + i
            all_k[2 * parts + hot_rows * c + i] = chip_k[at]
            all_v[2 * parts + hot_rows * c + i] = chip_v[at]
            if i % chunk == chunk - 1:
                for which in range(2):
                    forward(i // chunk, which).start()

    def gather(i, carry):
        at = tab[0, (i // lane_rows + 1) * cap + lane_rows * c + i % lane_rows]
        send_k[i // lane_rows, i % lane_rows] = chip_k[at]
        send_v[i // lane_rows, i % lane_rows] = chip_v[at]
        return carry

    lax.fori_loop(0, 3 * lane_rows, gather, 0)
    send_lights((pos == 1) & (rel == 1), (1,), 2)
    send_lights((pos == 1) & (rel == 2), (2,), 2)
    send_lights((pos == 3) & (rel == 1), (2, 1), 2)
    send_lights((pos == 3) & (rel == 2), (1, 2), 2)
    send_lights(pos == 2, (3, 2, 1), 2)
    send_lights((pos == 0) & (c == 0), (3, 1), 1)
    send_lights((pos == 0) & (c == 1), (2,), 1)
    both_k = fetch(7, chip_k, all_k.at[pl.ds(0, 2 * parts)])
    both_v = fetch(8, chip_v, all_v.at[pl.ds(0, 2 * parts)])

    def relay(*list_of):
        for where, q in list_of:

            @pl.when(pos == where)
            def _():
                for which in range(2):
                    forward(q, which).wait_recv()
                    if where < 3:
                        forward(q, which).start()
                    mirror(q, which).start()

    relay((1, 0))
    relay((1, 1))
    own_act.wait()
    for copy in acts:
        copy.wait()

    def features(t):
        return jnp.concatenate([act_part[t], act_all[t]], 0).astype(f32)

    square = jnp.zeros((rows, 1), f32)
    for t in range(tps):
        u = features(t)
        square = square + jnp.sum(u * u, -1, keepdims=True)
    inv = lax.rsqrt(square / (width * tps) + 1e-05)
    normed = []
    for t in range(tps):
        u = features(t)
        normed.append((u * inv * gain[:, t * width : (t + 1) * width]).astype(bf16))

    def project(w):
        total = None
        for t in range(tps):
            part = jnp.dot(
                normed[t], w[t * width : (t + 1) * width, :], preferred_element_type=f32
            )
            total = part if total is None else total + part
        return total

    cos_t, sin_t = cosine[...], sine[...]

    def turn(u):
        return u * cos_t + pltpu.roll(u, HD // 2, 1) * sin_t

    load_k.wait()
    load_v.wait()
    keys = project(wk_v)
    fresh = pair_f.at[0]
    for g in range(groups):
        fresh[:, g * HD : (g + 1) * HD] = turn(keys[:, g * HD : (g + 1) * HD]).astype(bf16)
    fresh[:, kvw:] = project(wv_v).astype(bf16)

    swap_f = push(fresh, pair_f.at[1], fr_send.at[0], fr_recv.at[0], sib, me_t)
    swap_f.start()

    def light_fresh(k):
        return push(
            send_f.at[k - 1], light_f.at[k - 1, c], fr_send.at[k], fr_recv.at[k],
            (xn, yn, dn)[k - 1], me_t,
        )

    def hot_fresh(k):
        return push(
            send_f.at[pl.ds(4, 2)], hot_f.at[c], fr_send.at[3 + k], fr_recv.at[3 + k],
            (xn, yn, dn)[k - 1], me_t,
        )

    def light_fresh_mirror(k):
        area = light_f.at[k - 1, c]
        return push(area, area, fr_send.at[6 + k], fr_recv.at[6 + k], sib, me_t)

    def hot_fresh_mirror():
        return push(hot_f.at[c], hot_f.at[c], fr_send.at[10], fr_recv.at[10], sib, me_t)

    load_q.wait()
    query = project(wq_v)
    for h in range(groups * per):
        g, j = h // per, h % per
        turned = turn(query[:, h * HD : (h + 1) * HD])
        for s in range(steps):
            qs[g, :, s * per + j, :] = turned[s * parts : (s + 1) * parts]
    relay((1, 2), (2, 0))

    lines = parts * pack
    row = lax.broadcasted_iota(jnp.int32, (lines, rows), 0)
    col = lax.broadcasted_iota(jnp.int32, (lines, rows), 1)
    allowed = (row // pack == col % parts) & (col // parts <= (row % pack) // per)
    scale = HD**0.5
    for g in range(groups):
        lanes = slice(g * HD, (g + 1) * HD)
        qg = qs[g].reshape(lines, HD).astype(bf16)
        for n in range(parts):
            sc1[g, n * pack : (n + 1) * pack, :] = lax.dot_general(
                qg[n * pack : (n + 1) * pack], chip_k[n, :, lanes],
                (((1,), (1,)), ((), ())), preferred_element_type=f32,
            )
        near = lax.dot_general(
            qg, fresh[:, lanes], (((1,), (1,)), ((), ())), preferred_element_type=f32
        )
        near = jnp.where(allowed, near / scale, -jnp.inf)
        far = sc1[g] / scale
        top = jnp.maximum(
            jnp.max(far, -1, keepdims=True), jnp.max(near, -1, keepdims=True)
        )
        far = jnp.exp(far - top)
        near = jnp.exp(near - top)
        mass = jnp.sum(far, -1, keepdims=True) + jnp.sum(near, -1, keepdims=True)
        far = (far / mass).astype(bf16)
        near = (near / mass).astype(bf16)
        extra = jnp.dot(
            near, fresh[:, kvw + g * HD : kvw + (g + 1) * HD], preferred_element_type=f32
        )
        for n in range(parts):
            part = slice(n * pack, (n + 1) * pack)
            cx[g, n] = extra[part] + jnp.dot(
                far[part], chip_v[n, :, lanes], preferred_element_type=f32
            )
    for h in range(groups * per):
        g, j = h // per, h % per
        for s in range(steps):
            ctx_b[s * parts : (s + 1) * parts, h * HD : (h + 1) * HD] = cx[
                g, :, s * per + j, :
            ].astype(bf16)
    load_o.wait()

    def mix(p):
        return jnp.dot(
            ctx_b[...], wo_v[:, pl.ds(pl.multiple_of(p * width, HD), width)],
            preferred_element_type=f32,
        )

    lane = lax.broadcasted_iota(jnp.int32, (rows, HD), 1)
    line = lax.broadcasted_iota(jnp.int32, (rows, HD), 0)

    def flat(column, start=0):
        return jnp.sum(jnp.where(lane == line + start, column, 0.0), 0, keepdims=True)

    count = table.shape[0]
    deep = lax.broadcasted_iota(jnp.int32, (rows, parts), 0) % parts
    broad = lax.broadcasted_iota(jnp.int32, (rows, parts), 1)
    names = jnp.concatenate(
        [jnp.broadcast_to(tokens[s : s + 1, :], (parts, parts)) for s in range(steps)], 0
    )
    name = jnp.sum(jnp.where(deep == broad, names, 0).astype(f32), -1, keepdims=True)
    name = name.astype(jnp.int32)
    entry = lax.broadcasted_iota(jnp.int32, (rows, count), 1)
    found = jnp.dot(
        (entry == name // HD).astype(f32).astype(bf16), table[...], preferred_element_type=f32
    )
    gift = flat(jnp.sum(jnp.where(lane == name % HD, found, 0.0), -1, keepdims=True))
    lw_all[me_d] = jnp.full((8, HD), -jnp.inf, f32)

    sums = []
    for k in (2, 1, 3)[: tps - 1]:
        rs_send[k - 1] = mix((me_t + k) % tps).astype(bf16)
        sums.append(tp_push(tps - 1, k, rs_send.at[k - 1], rs_recv.at[k - 1]))
    head = mix(me_t)
    swap_f.wait_recv()
    pair = pair_f[...].reshape(2 * rows, 2 * kvw)
    index = lax.broadcasted_iota(jnp.int32, (2 * rows, HD), 0)
    pick = (index == tabv[5:6, :]).astype(f32).astype(bf16)
    send_f[...] = lax.dot_general(
        pick, pair, (((0,), (0,)), ((), ())), preferred_element_type=f32
    ).astype(bf16).reshape(send_f.shape)
    for k in (3, 1, 2):
        light_fresh(k).start()

    @pl.when(pos == 0)
    def _():
        hot_f[...] = jnp.zeros(hot_f.shape, bf16)
        for k in (3, 1, 2):
            hot_fresh(k).start()

    relay((1, 3), (2, 1))
    send_lights((pos == 0) & (c == 0), (2,), 1)
    send_lights((pos == 0) & (c == 1), (3, 1), 1)
    send_lights((pos == 1) & (rel == 1), (3, 2), 2)
    send_lights((pos == 1) & (rel == 2), (3, 1), 2)
    send_lights(pos == 3, (3,), 2)
    relay((2, 2))
    relay((2, 3), (3, 0))
    for copy in sums:
        copy.wait()
    for k in range(1, tps):
        head = head + rs_recv[k - 1].astype(f32)
    attn_out[...] = head.astype(bf16)
    summed = features(me_t) + head
    along = jnp.sum(summed * twist[...], -1, keepdims=True)
    energy = jnp.sum(summed * summed, -1, keepdims=True)
    sc_all[me_t] = jnp.broadcast_to(flat(along) + flat(energy, HD // 2), (8, HD))
    scores = [
        tp_push(2 * (tps - 1), k, sc_all.at[me_t], sc_all.at[me_t]) for k in range(1, tps)
    ]
    relay((3, 1))
    for copy in scores:
        copy.wait()
    both = sc_all[0]
    for t in range(1, tps):
        both = both + sc_all[t]
    power = pltpu.roll(both, HD // 2, 1)
    score = both / jnp.sqrt(power / (width * tps) + 1e-06)
    score = jnp.where(lane[:8] < rows, score + gift, 0.0)
    total = score
    for s in range(1, steps):
        total = total + pltpu.roll(score, HD - s * parts, 1)
    mine = total[:, :parts] + jnp.broadcast_to(prev[...], (8, parts))
    lw_all[me_d, :, :parts] = mine
    lws = []
    for k in range(1, doms):
        copy = push(
            lw_all.at[me_d], lw_all.at[me_d], lw_send.at[k - 1], lw_recv.at[k - 1],
            (me_d + k) % doms, me_t,
        )
        copy.start()
        lws.append(copy)

    arrived(2)
    arrived(1)
    relay((3, 2))
    for k in (1, 2, 3):
        light_fresh(k).wait_recv()
        light_fresh_mirror(k).start()

        @pl.when(rel == k)
        def _():
            hot_fresh(k).wait_recv()
            hot_fresh_mirror().start()

    arrived(3)
    relay((3, 3))
    for k in (1, 2, 3):
        light_fresh_mirror(k).wait()

    @pl.when(pos > 0)
    def _():
        hot_fresh_mirror().wait()

    pool = jnp.concatenate(
        [
            pair_f[...].reshape(2 * rows, 2 * kvw),
            hot_f[...].reshape(rows, 2 * kvw),
            light_f[...].reshape(96, 2 * kvw),
        ],
        0,
    )
    index = lax.broadcasted_iota(jnp.int32, (3 * rows + 96, HD), 0)
    pick = (index == tabv[3:4, :]).astype(f32).astype(bf16)
    chosen[...] = lax.dot_general(
        pick, pool, (((0,), (0,)), ((), ())), preferred_element_type=f32
    ).astype(bf16)

    both_k.wait()
    both_v.wait()
    for k in (1, 2, 3):
        for which in range(2):
            light_mirror(k, which, 0).wait()

        @pl.when(rel != k)
        def _():
            for which in range(2):
                light_mirror(k, which, 1).wait()

    @pl.when(pos > 0)
    def _():
        for q in range(4):
            for which in range(2):
                mirror(q, which).wait()

    def place(i, carry):
        at = tab[1, i]
        new_k[i] = all_k[at]
        new_v[i] = all_v[at]
        return carry

    lax.fori_loop(0, parts, place, 0)

    for copy in lws:
        copy.wait()
    every_lw = lw_all[:, 0, :]
    largest = jnp.max(every_lw, (0, 1), keepdims=True)
    mass = jnp.sum(jnp.exp(every_lw - largest), (0, 1), keepdims=True)
    out_lw[...] = mine[:1] - (largest + jnp.log(mass))

    @pl.when(pos < 3)
    def _():
        for q in range(4):
            for which in range(2):
                forward(q, which).wait_send()

    for k in (1, 2, 3):
        for which in range(2):
            light(k, which, 0).wait_send()

    @pl.when(pos > 0)
    def _():
        for k in (1, 2, 3):
            for which in range(2):
                light(k, which, 1).wait_send()

    for k in (1, 2, 3):
        light_fresh(k).wait_send()
    swap_f.wait_send()

    @pl.when(pos == 0)
    def _():
        for k in (1, 2, 3):
            hot_fresh(k).wait_send()


def finish_kernel(
    parts, steps, rows_k, rows_v, chosen, attn, lw,
    out_k, out_v, out_attn, out_lw, buf_k, buf_v, sem,
):
    span, width = rows_k.shape[1:]
    group = 32
    copies = [pltpu.make_async_copy(attn, out_attn, sem.at[0])]
    copies[0].start()

    def send(buf, out, start, size):
        copy = pltpu.make_async_copy(
            buf.at[pl.ds(start, size)], out.at[pl.ds(start, size)], sem.at[len(copies)]
        )
        copy.start()
        copies.append(copy)

    for which, (src, buf, out) in enumerate(((rows_k, buf_k, out_k), (rows_v, buf_v, out_v))):
        for g in range(0, span, group):
            buf[g : g + group] = jnp.transpose(src[:, g : g + group, :], (1, 0, 2))
            send(buf, out, g, group)
        tail = chosen[:, which * width : (which + 1) * width].reshape(parts, 8, width)
        buf[span:] = jnp.transpose(tail, (1, 0, 2))[:steps]
        send(buf, out, span, steps)
    out_lw[...] = lw[...]
    for copy in copies:
        copy.wait()


def adaptive(
    activations, norm_gain, w_query, w_key, value_weight, w_output, cache_keys, cache_values,
    tokens, twisting_table, twist_vec, previous_log_weights, copy_counts,
):
    f32, bf16 = jnp.float32, jnp.bfloat16
    steps, parts, width = activations.shape
    rows = steps * parts
    span = cache_keys.shape[1]
    kvw = w_key.shape[1]
    qw = w_query.shape[1]
    groups = kvw // HD
    pack = steps * (qw // kvw)
    doms = lax.axis_size("dom")
    tps = lax.axis_size("tp")
    middle = HD // 2
    cap = CAP
    angles = (span + np.arange(rows) // parts)[:, None] * (
        500000.0 ** (-2.0 * np.arange(middle) / HD)
    )
    cosine = np.concatenate([np.cos(angles)] * 2, 1).astype(np.float32)
    sine = np.concatenate([-np.sin(angles), np.sin(angles)], 1).astype(np.float32)
    vmem = pl.BlockSpec(memory_space=pltpu.VMEM)
    smem = pl.BlockSpec(memory_space=pltpu.SMEM)
    hbm = pl.BlockSpec(memory_space=pl.ANY)
    dma = pltpu.SemaphoreType.DMA
    both = jax.ShapeDtypeStruct((2 * parts, span, kvw), bf16)
    tab, chip_k, chip_v, act_part = pl.pallas_call(
        functools.partial(plan_kernel, parts, doms, tps, cap, HOT_CAP, steps, rows),
        out_shape=(
            jax.ShapeDtypeStruct((8, HD), jnp.int32), both, both,
            jax.ShapeDtypeStruct((tps, EARLY * parts, width), bf16),
        ),
        in_specs=[vmem, hbm, hbm, hbm],
        out_specs=(vmem,) * 4,
        scratch_shapes=[
            pltpu.VMEM((doms, 8, HD), f32),
            dma((doms - 1,)), dma((doms - 1,)), dma((3,)), dma((2,)), dma((2,)),
            dma((tps - 1,)), dma((tps - 1,)),
        ],
        compiler_params=pltpu.CompilerParams(
            collective_id=5, has_side_effects=True, vmem_limit_bytes=16 << 20
        ),
        name="plan",
    )(copy_counts.reshape(1, parts), activations.reshape(rows, width), cache_keys, cache_values)

    def hot_branch(hot):
        result = jax.ShapeDtypeStruct((parts, span, kvw), bf16)
        call = pl.pallas_call(
            functools.partial(main_kernel, steps, parts, doms, tps, cap, HOT_CAP, hot),
            out_shape=(
                jax.ShapeDtypeStruct((rows, width), bf16), result, result,
                jax.ShapeDtypeStruct((HD, 2 * kvw), bf16),
                jax.ShapeDtypeStruct((1, parts), f32),
            ),
            in_specs=[hbm, vmem, vmem] + [hbm] * 4 + [vmem] * 8 + [smem, vmem],
            out_specs=(vmem,) * 5,
            scratch_shapes=[
                pltpu.VMEM((tps, rows - EARLY * parts, width), bf16),
                pltpu.VMEM(w_query.shape, bf16),
                pltpu.VMEM(w_key.shape, bf16),
                pltpu.VMEM(value_weight.shape, bf16),
                pltpu.VMEM(w_output.shape, bf16),
                pltpu.VMEM((3 * parts + 3 * cap, span, kvw), bf16),
                pltpu.VMEM((3 * parts + 3 * cap, span, kvw), bf16),
                pltpu.VMEM((3, cap // 2, span, kvw), bf16),
                pltpu.VMEM((3, cap // 2, span, kvw), bf16),
                pltpu.VMEM((groups, parts, pack, HD), f32),
                pltpu.VMEM((groups, parts, pack, HD), f32),
                pltpu.VMEM((groups, parts * pack, span), f32),
                pltpu.VMEM((rows, qw), bf16),
                pltpu.VMEM((2, rows, 2 * kvw), bf16),
                pltpu.VMEM((2, 2, 16, 2 * kvw), bf16),
                pltpu.VMEM((3, 2, 16, 2 * kvw), bf16),
                pltpu.VMEM((8, 16, 2 * kvw), bf16),
                pltpu.VMEM((tps - 1, rows, width), bf16),
                pltpu.VMEM((tps - 1, rows, width), bf16),
                pltpu.VMEM((tps, 8, HD), f32),
                pltpu.VMEM((doms, 8, HD), f32),
                dma((9,)),
                dma((3 * (tps - 1),)), dma((3 * (tps - 1),)),
                dma((doms - 1,)), dma((doms - 1,)),
                dma((16,)), dma((16,)),
                dma((24,)), dma((24,)),
                dma((11,)), dma((11,)),
            ],
            compiler_params=pltpu.CompilerParams(
                collective_id=hot, has_side_effects=True, vmem_limit_bytes=40 << 20
            ),
            name=f"main{hot}",
        )

        def run(
            act, act_part, gain, wq, wk, wv, wo, chip_k, chip_v, twist, tokens, table, prev,
            cosine, sine, tab, ck, cv, counts,
        ):
            attn, new_k, new_v, chosen, out_lw = call(
                act, act_part, gain, wq, wk, wv, wo, chip_k, chip_v, twist, tokens, table,
                prev, cosine, sine, tab, tab,
            )
            return new_k, new_v, attn, chosen, out_lw

        return run

    def every(
        act, act_part, gain, wq, wk, wv, wo, chip_k, chip_v, twist, tokens, table, prev,
        cosine, sine, tab, ck, cv, counts,
    ):
        reward = jnp.sum(table.reshape(-1)[tokens].astype(f32), 0)
        aux = jnp.stack([prev[0] + reward, counts.astype(f32)], 1)
        attn, new_k, new_v, chosen, out_lw = all_rows(
            steps, parts, act, gain, wq, wk, wv, wo, ck, cv, twist, aux, cosine, sine
        )
        return new_k, new_v, attn, chosen, out_lw

    rows_k, rows_v, attn, chosen, out_lw = lax.switch(
        tab[4, 0],
        [hot_branch(hot) for hot in range(4)] + [every],
        activations.reshape(rows, width), act_part, norm_gain.reshape(1, -1), w_query, w_key,
        value_weight, w_output, chip_k, chip_v, twist_vec.reshape(1, -1), tokens,
        twisting_table.reshape(-1, HD), previous_log_weights.reshape(1, parts),
        jnp.asarray(cosine), jnp.asarray(sine), tab, cache_keys, cache_values, copy_counts,
    )
    result = jax.ShapeDtypeStruct((span + steps, parts, kvw), bf16)
    new_k, new_v, attn, out_lw = pl.pallas_call(
        functools.partial(finish_kernel, parts, steps),
        out_shape=(
            result, result, jax.ShapeDtypeStruct((rows, width), bf16),
            jax.ShapeDtypeStruct((1, parts), f32),
        ),
        in_specs=[vmem] * 5,
        out_specs=(hbm, hbm, hbm, vmem),
        scratch_shapes=[
            pltpu.VMEM(result.shape, bf16), pltpu.VMEM(result.shape, bf16), dma((11,)),
        ],
        compiler_params=pltpu.CompilerParams(vmem_limit_bytes=8 << 20),
        name="finish",
    )(rows_k, rows_v, chosen, attn, out_lw)
    return (
        attn.reshape(steps, parts, width), jnp.transpose(new_k, (1, 0, 2)),
        jnp.transpose(new_v, (1, 0, 2)), out_lw.reshape(parts),
    )


def solution(mesh):
    body = adaptive if (mesh.shape["dom"], mesh.shape["tp"]) == (8, 4) else local
    return jax.shard_map(
        body,
        mesh=mesh,
        in_specs=(
            P(None, "dom", "tp"),
            P(),
            P(None, "tp"),
            P(None, "tp"),
            P(None, "tp"),
            P("tp", None),
            P("dom", None, "tp"),
            P("dom", None, "tp"),
            P(None, "dom"),
            P(),
            P("tp"),
            P("dom"),
            P("dom"),
        ),
        out_specs=(P(None, "dom", "tp"), P("dom", None, "tp"), P("dom", None, "tp"), P("dom")),
        check_vma=False,
    )
```

```python
import functools

import jax
import jax.numpy as jnp
import numpy as np
from jax import lax
from jax.experimental import pallas as pl
from jax.experimental.pallas import tpu as pltpu
from jax.sharding import PartitionSpec as P

D = 4096
HD = 128
CAP = 6
HOT_CAP = 4
EARLY = 1


def rotate(tensor, positions):
    middle = tensor.shape[-1] // 2
    frequency = 500000.0 ** (-2.0 * jnp.arange(middle, dtype=jnp.float32) / tensor.shape[-1])
    angles = positions[:, None] * frequency[None, :]
    cosine = jnp.cos(angles)[:, None, None, :]
    sine_part = jnp.sin(angles)[:, None, None, :]
    lower_half = tensor[..., :middle]
    upper_half = tensor[..., middle:]
    return jnp.concatenate(
        [
            lower_half * cosine - upper_half * sine_part,
            upper_half * cosine + lower_half * sine_part,
        ],
        -1,
    )


def local(
    activations,
    norm_gain,
    w_query,
    w_key,
    value_weight,
    w_output,
    cache_keys,
    cache_values,
    tokens,
    twisting_table,
    twist_vec,
    previous_log_weights,
    copy_counts,
):
    step_count = activations.shape[0]
    particle_count = activations.shape[1]
    span_old = cache_keys.shape[1]
    dom_size = lax.axis_size("dom")
    kv_local = w_key.shape[1] // HD
    q_local = w_query.shape[1] // HD
    group_size = q_local // kv_local
    all_counts = lax.all_gather(copy_counts, "dom", axis=0, tiled=True)
    copy_ends = jnp.cumsum(all_counts)
    ranks = jnp.arange(particle_count, dtype=jnp.int32) * dom_size + lax.axis_index("dom")
    ancestor = jnp.sum((copy_ends[None, :] <= ranks[:, None]).astype(jnp.int32), 1)
    all_keys = lax.all_gather(cache_keys, "dom", axis=0, tiled=True)
    all_values = lax.all_gather(cache_values, "dom", axis=0, tiled=True)

    gathered = lax.all_gather(activations, "tp", axis=2, tiled=True)
    inputs = gathered.astype(jnp.float32)
    normed = (
        inputs * lax.rsqrt(jnp.mean(inputs * inputs, -1, keepdims=True) + 1e-05) * norm_gain
    ).astype(jnp.bfloat16)
    flat_rows = normed.reshape(step_count * particle_count, D)
    positions = (span_old + jnp.arange(step_count, dtype=jnp.int32)).astype(jnp.float32)
    queries = jnp.dot(flat_rows, w_query, preferred_element_type=jnp.float32).reshape(
        step_count, particle_count, q_local, HD
    )
    queries = rotate(queries, positions).astype(jnp.bfloat16)
    fresh_keys = jnp.dot(flat_rows, w_key, preferred_element_type=jnp.float32).reshape(
        step_count, particle_count, kv_local, HD
    )
    fresh_keys = (
        rotate(fresh_keys, positions)
        .astype(jnp.bfloat16)
        .reshape(step_count, particle_count, kv_local * HD)
    )
    fresh_values = jnp.dot(flat_rows, value_weight, preferred_element_type=jnp.float32).astype(
        jnp.bfloat16
    )
    fresh_values = fresh_values.reshape(step_count, particle_count, kv_local * HD)
    fresh_keys = jnp.transpose(fresh_keys, (1, 0, 2))
    fresh_values = jnp.transpose(fresh_values, (1, 0, 2))
    key_rows = jnp.concatenate([cache_keys, fresh_keys], 1)
    value_rows = jnp.concatenate([cache_values, fresh_values], 1)
    key_span = span_old + step_count
    query_heads = queries.reshape(step_count, particle_count, kv_local, group_size, HD)
    key_heads = key_rows.reshape(particle_count, key_span, kv_local, HD)
    value_heads = value_rows.reshape(particle_count, key_span, kv_local, HD)
    scores = (
        jnp.einsum("snkgd,nlkd->snkgl", query_heads, key_heads, preferred_element_type=jnp.float32)
        / HD**0.5
    )
    allowed = (
        jnp.arange(key_span, dtype=jnp.int32)[None, :]
        <= (span_old + jnp.arange(step_count, dtype=jnp.int32))[:, None]
    )
    allowed = allowed[:, None, None, None, :]
    masked = jnp.where(allowed, scores, -jnp.inf)
    highest = jnp.max(masked, -1, keepdims=True)
    exponent = jnp.exp(masked - highest)
    weights = (exponent / jnp.sum(exponent, -1, keepdims=True)).astype(jnp.bfloat16)
    context = jnp.einsum(
        "snkgl,nlkd->snkgd", weights, value_heads, preferred_element_type=jnp.float32
    ).astype(jnp.bfloat16)
    context = context.reshape(step_count * particle_count, q_local * HD)
    partial_value = jnp.dot(context, w_output, preferred_element_type=jnp.float32).reshape(
        step_count, particle_count, D
    )
    head_mix = lax.psum_scatter(partial_value, "tp", scatter_dimension=2, tiled=True)
    attn_out = head_mix.astype(jnp.bfloat16)
    summed = activations.astype(jnp.float32) + head_mix
    aligned, energy = lax.psum(
        (jnp.sum(summed * twist_vec, -1), jnp.sum(summed * summed, -1)), "tp"
    )
    twisting_score = aligned / jnp.sqrt(energy / D + 1e-06)
    token_reward = twisting_table[tokens].astype(jnp.float32)
    particle_log_weight = previous_log_weights + jnp.sum(token_reward + twisting_score, 0)
    largest = lax.pmax(jnp.max(particle_log_weight), "dom")
    mass_total = lax.psum(jnp.sum(jnp.exp(particle_log_weight - largest)), "dom")
    out_logw = particle_log_weight - (largest + jnp.log(mass_total))
    fresh = lax.all_gather(
        jnp.concatenate([fresh_keys, fresh_values], 2), "dom", axis=0, tiled=True
    )[ancestor]
    width = fresh_keys.shape[2]
    new_keys = jnp.concatenate([all_keys[ancestor], fresh[..., :width]], 1)
    new_values = jnp.concatenate([all_values[ancestor], fresh[..., width:]], 1)
    return (attn_out, new_keys, new_values, out_logw)


MESH = pl.DeviceIdType.MESH


def layer_kernel(
    steps, parts, doms, tps,
    act, gain, wq, wk, wv, wo, ck, cv, twist, aux, cosine, sine,
    attn_out, all_k, all_v, fresh_sel, out_lw, anc_out,
    act_all, wq_v, wk_v, wv_v, wo_v, ck_v, cv_v, qs, cx, sc1, ctx_b, fresh, fresh_all,
    rs_send, rs_recv, sc_all, lw_all, cnt_all,
    loc, tp_send, tp_recv, dom_send, dom_recv, blk_send, blk_recv,
):
    f32, bf16 = jnp.float32, jnp.bfloat16
    me_d = lax.axis_index("dom")
    me_t = lax.axis_index("tp")
    rows, width = act.shape
    half = parts // 2
    kvw = wk.shape[1]
    groups = kvw // HD
    per = wq.shape[1] // kvw
    pack = steps * per
    c = me_d % 2
    x = (me_d // 2) % 2
    y = me_d // 4
    sib = me_d + 1 - 2 * c
    xn = me_d + 2 - 4 * x
    yn = me_d + 4 - 8 * y
    dn = xn + 4 - 8 * y

    barrier = pltpu.get_barrier_semaphore()
    for k in range(1, tps):
        pl.semaphore_signal(
            barrier, inc=1, device_id=(me_d, (me_t + k) % tps), device_id_type=MESH
        )
    for k in range(1, doms):
        pl.semaphore_signal(
            barrier, inc=1, device_id=((me_d + k) % doms, me_t), device_id_type=MESH
        )

    def fetch(i, src, dst):
        copy = pltpu.make_async_copy(src, dst, loc.at[i])
        copy.start()
        return copy

    own_act = fetch(0, act, act_all.at[me_t])
    load_q = fetch(1, wq, wq_v)
    load_k = fetch(2, wk, wk_v)
    load_v = fetch(3, wv, wv_v)
    load_ck = fetch(4, ck, ck_v)
    load_cv = fetch(5, cv, cv_v)
    load_o = fetch(6, wo, wo_v)

    cnt_all[me_d] = jnp.broadcast_to(aux[:, 1:], cnt_all.shape[1:])
    pl.semaphore_wait(barrier, tps + doms - 2)

    def tp_push(base, k, src, dst):
        copy = pltpu.make_async_remote_copy(
            src_ref=src, dst_ref=dst, send_sem=tp_send.at[base + k - 1],
            recv_sem=tp_recv.at[base + k - 1],
            device_id=(me_d, (me_t + k) % tps), device_id_type=MESH,
        )
        copy.start()
        return copy

    def dom_push(base, k, src, dst):
        copy = pltpu.make_async_remote_copy(
            src_ref=src, dst_ref=dst, send_sem=dom_send.at[base + k - 1],
            recv_sem=dom_recv.at[base + k - 1],
            device_id=((me_d + k) % doms, me_t), device_id_type=MESH,
        )
        copy.start()
        return copy

    acts = [tp_push(0, k, act, act_all.at[me_t]) for k in range(1, tps)]

    def piece(kind, to, which, h, slot, own):
        dst = (all_k, all_v)[which].at[slot, pl.ds(h * half, half)]
        src = (ck, cv)[which].at[pl.ds(h * half, half)] if own else dst
        i = kind * 4 + h * 2 + which
        copy = pltpu.make_async_remote_copy(
            src_ref=src, dst_ref=dst, send_sem=blk_send.at[i], recv_sem=blk_recv.at[i],
            device_id=(to, me_t), device_id_type=MESH,
        )
        copy.start()
        return copy

    moves = {}
    for h, kind, to in ((0, 0, xn), (1, 1, yn), (1, 0, xn), (0, 1, yn)):
        for which in range(2):
            moves[kind, h, which] = piece(kind, to, which, h, me_d, True)
    cnts = [dom_push(0, k, cnt_all.at[me_d], cnt_all.at[me_d]) for k in range(1, doms)]
    for h in range(2):
        for which in range(2):
            moves[3, h, which] = piece(3, sib, which, h, me_d, True)

    own_act.wait()
    for copy in acts:
        copy.wait()
    square = jnp.zeros((rows, 1), f32)
    for t in range(tps):
        u = act_all[t].astype(f32)
        square = square + jnp.sum(u * u, -1, keepdims=True)
    inv = lax.rsqrt(square / (width * tps) + 1e-05)
    normed = []
    for t in range(tps):
        u = act_all[t].astype(f32)
        normed.append((u * inv * gain[:, t * width : (t + 1) * width]).astype(bf16))

    def project(w):
        total = None
        for t in range(tps):
            part = jnp.dot(
                normed[t], w[t * width : (t + 1) * width, :], preferred_element_type=f32
            )
            total = part if total is None else total + part
        return total

    cos_t, sin_t = cosine[...], sine[...]

    def turn(u):
        return u * cos_t + pltpu.roll(u, HD // 2, 1) * sin_t

    load_k.wait()
    load_v.wait()
    keys = project(wk_v)
    for g in range(groups):
        fresh[:, g * HD : (g + 1) * HD] = turn(keys[:, g * HD : (g + 1) * HD]).astype(bf16)
    fresh[:, kvw:] = project(wv_v).astype(bf16)
    fresh_all[me_d] = fresh[...]
    news = [dom_push(doms - 1, k, fresh, fresh_all.at[me_d]) for k in range(1, doms)]
    load_q.wait()
    query = project(wq_v)
    for h in range(groups * per):
        g, j = h // per, h % per
        turned = turn(query[:, h * HD : (h + 1) * HD])
        for s in range(steps):
            qs[g, :, s * per + j, :] = turned[s * parts : (s + 1) * parts]
    load_ck.wait()
    load_cv.wait()
    put_k = fetch(7, ck_v, all_k.at[me_d])
    put_v = fetch(8, cv_v, all_v.at[me_d])

    lines = parts * pack
    row = lax.broadcasted_iota(jnp.int32, (lines, rows), 0)
    col = lax.broadcasted_iota(jnp.int32, (lines, rows), 1)
    allowed = (row // pack == col % parts) & (col // parts <= (row % pack) // per)
    scale = HD**0.5
    for g in range(groups):
        lanes = slice(g * HD, (g + 1) * HD)
        qg = qs[g].reshape(lines, HD).astype(bf16)
        for n in range(parts):
            sc1[g, n * pack : (n + 1) * pack, :] = lax.dot_general(
                qg[n * pack : (n + 1) * pack], ck_v[n, :, lanes],
                (((1,), (1,)), ((), ())), preferred_element_type=f32,
            )
        near = lax.dot_general(
            qg, fresh[:, lanes], (((1,), (1,)), ((), ())), preferred_element_type=f32
        )
        near = jnp.where(allowed, near / scale, -jnp.inf)
        far = sc1[g] / scale
        top = jnp.maximum(
            jnp.max(far, -1, keepdims=True), jnp.max(near, -1, keepdims=True)
        )
        far = jnp.exp(far - top)
        near = jnp.exp(near - top)
        mass = jnp.sum(far, -1, keepdims=True) + jnp.sum(near, -1, keepdims=True)
        far = (far / mass).astype(bf16)
        near = (near / mass).astype(bf16)
        extra = jnp.dot(
            near, fresh[:, kvw + g * HD : kvw + (g + 1) * HD], preferred_element_type=f32
        )
        for n in range(parts):
            span = slice(n * pack, (n + 1) * pack)
            cx[g, n] = extra[span] + jnp.dot(
                far[span], cv_v[n, :, lanes], preferred_element_type=f32
            )
    for h in range(groups * per):
        g, j = h // per, h % per
        for s in range(steps):
            ctx_b[s * parts : (s + 1) * parts, h * HD : (h + 1) * HD] = cx[
                g, :, s * per + j, :
            ].astype(bf16)
    load_o.wait()

    def mix(p):
        return jnp.dot(
            ctx_b[...], wo_v[:, pl.ds(pl.multiple_of(p * width, HD), width)],
            preferred_element_type=f32,
        )

    sums = []
    for k in range(1, tps):
        rs_send[k - 1] = mix((me_t + k) % tps)
        sums.append(tp_push(tps - 1, k, rs_send.at[k - 1], rs_recv.at[k - 1]))
    head = mix(me_t)

    def done(kind, h):
        for which in range(2):
            moves[kind, h, which].wait_recv()

    def relay(kind, to, h, slot):
        for which in range(2):
            moves[kind, h, which] = piece(kind, to, which, h, slot, False)

    done(0, 0)
    relay(2, yn, 0, xn)
    relay(4, sib, 0, xn)
    done(1, 1)
    relay(6, xn, 1, yn)
    relay(5, sib, 1, yn)
    for k in range(1, tps):
        sums[k - 1].wait()
        head = head + rs_recv[k - 1]
    attn_out[...] = head.astype(bf16)
    summed = act_all[me_t].astype(f32) + head
    along = jnp.sum(summed * twist[...], -1, keepdims=True)
    energy = jnp.sum(summed * summed, -1, keepdims=True)
    lane = lax.broadcasted_iota(jnp.int32, (rows, HD), 1)
    sc_all[me_t] = jnp.where(lane < HD // 2, along, energy)
    scores = [
        tp_push(2 * (tps - 1), k, sc_all.at[me_t], sc_all.at[me_t]) for k in range(1, tps)
    ]
    for copy in scores:
        copy.wait()
    both = sc_all[0]
    for t in range(1, tps):
        both = both + sc_all[t]
    score = both[:, :1] / jnp.sqrt(both[:, HD - 1 :] / (width * tps) + 1e-06)
    total = score[:parts]
    for s in range(1, steps):
        total = total + score[s * parts : (s + 1) * parts]
    mine = jnp.broadcast_to(aux[:, :1] + total, (parts, HD))
    lw_all[me_d] = mine
    lws = [
        dom_push(2 * (doms - 1), k, lw_all.at[me_d], lw_all.at[me_d]) for k in range(1, doms)
    ]

    done(0, 1)
    relay(4, sib, 1, xn)
    done(1, 0)
    relay(5, sib, 0, yn)

    for copy in cnts:
        copy.wait()
    for copy in news:
        copy.wait()
    whole = parts * doms
    number = cnt_all[...].reshape(whole, HD).astype(bf16)
    lower = lax.broadcasted_iota(jnp.int32, (whole, whole), 0)
    upper = lax.broadcasted_iota(jnp.int32, (whole, whole), 1)
    ends = jnp.dot(
        (upper <= lower).astype(f32).astype(bf16), number, preferred_element_type=f32
    )
    slot = lax.broadcasted_iota(jnp.int32, (whole, HD), 1)

    def ancestor(place):
        rank = (place * doms + me_d).astype(f32)
        return jnp.sum((ends <= rank).astype(f32), 0, keepdims=True).astype(jnp.int32)

    anc_out[...] = jnp.broadcast_to(ancestor(slot), anc_out.shape)
    lanes = lax.broadcasted_iota(jnp.int32, (1, HD), 1)
    wide = ancestor(slot // 8)
    target = (wide // parts) * rows + (lanes % 8) * parts + wide % parts
    target = jnp.where(lanes % 8 < steps, target, -1)
    index = lax.broadcasted_iota(jnp.int32, (doms * rows, HD), 0)
    pick = (index == target).astype(f32).astype(bf16)
    fresh_sel[...] = lax.dot_general(
        pick, fresh_all[...].reshape(doms * rows, 2 * kvw),
        (((0,), (0,)), ((), ())), preferred_element_type=f32,
    ).astype(bf16)

    for copy in lws:
        copy.wait()
    largest = jnp.max(lw_all[...], (0, 1), keepdims=True)[0]
    mass = jnp.sum(jnp.exp(lw_all[...] - largest[None]), (0, 1), keepdims=True)[0]
    out_lw[...] = mine - (largest + jnp.log(mass))

    done(2, 0)
    relay_d0 = [piece(7, sib, which, 0, dn, False) for which in range(2)]
    done(6, 1)
    relay_d1 = [piece(7, sib, which, 1, dn, False) for which in range(2)]
    for kind in (3, 4, 5):
        for h in range(2):
            done(kind, h)
    for copy in moves.values():
        copy.wait_send()
    for copy in relay_d0 + relay_d1:
        copy.wait()
    put_k.wait()
    put_v.wait()


def select_kernel(
    parts, anc, fresh_sel, attn, lw, all_k, all_v,
    out_attn, new_k, new_v, chosen, out_lw, sem,
):
    copies = []
    for i in range(parts):
        a = anc[0, i]
        d, n = a // parts, a % parts
        for which, (src, dst) in enumerate(((all_k, new_k), (all_v, new_v))):
            copy = pltpu.make_async_copy(src.at[d, n], dst.at[i], sem.at[2 * i + which])
            copy.start()
            copies.append(copy)
    chosen[...] = fresh_sel[...]
    out_attn[...] = attn[...]
    row = lax.broadcasted_iota(jnp.int32, (parts, parts), 0)
    col = lax.broadcasted_iota(jnp.int32, (parts, parts), 1)
    out_lw[...] = jnp.sum(jnp.where(row == col, lw[:, :1], 0.0), 0, keepdims=True)
    for copy in copies:
        copy.wait()


def all_rows(
    steps, parts, act, gain, wq, wk, wv, wo, ck, cv, twist, aux, cosine, sine,
):
    f32, bf16 = jnp.float32, jnp.bfloat16
    rows, width = act.shape
    span = ck.shape[1]
    kvw = wk.shape[1]
    qw = wq.shape[1]
    groups = kvw // HD
    pack = steps * (qw // kvw)
    doms = lax.axis_size("dom")
    tps = lax.axis_size("tp")
    vmem = pl.BlockSpec(memory_space=pltpu.VMEM)
    hbm = pl.BlockSpec(memory_space=pl.ANY)
    block = jax.ShapeDtypeStruct((doms,) + ck.shape, bf16)
    attn, all_k, all_v, fresh_sel, out_lw, anc = pl.pallas_call(
        functools.partial(layer_kernel, steps, parts, doms, tps),
        out_shape=(
            jax.ShapeDtypeStruct((rows, width), bf16), block, block,
            jax.ShapeDtypeStruct((HD, 2 * kvw), bf16),
            jax.ShapeDtypeStruct((parts, HD), f32),
            jax.ShapeDtypeStruct((8, HD), jnp.int32),
        ),
        in_specs=[hbm, vmem] + [hbm] * 6 + [vmem] * 4,
        out_specs=(vmem, hbm, hbm, vmem, vmem, vmem),
        scratch_shapes=[
            pltpu.VMEM((tps, rows, width), bf16),
            pltpu.VMEM(wq.shape, bf16),
            pltpu.VMEM(wk.shape, bf16),
            pltpu.VMEM(wv.shape, bf16),
            pltpu.VMEM(wo.shape, bf16),
            pltpu.VMEM(ck.shape, bf16),
            pltpu.VMEM(cv.shape, bf16),
            pltpu.VMEM((groups, parts, pack, HD), f32),
            pltpu.VMEM((groups, parts, pack, HD), f32),
            pltpu.VMEM((groups, parts * pack, span), f32),
            pltpu.VMEM((rows, qw), bf16),
            pltpu.VMEM((rows, 2 * kvw), bf16),
            pltpu.VMEM((doms, rows, 2 * kvw), bf16),
            pltpu.VMEM((tps - 1, rows, width), f32),
            pltpu.VMEM((tps - 1, rows, width), f32),
            pltpu.VMEM((tps, rows, HD), f32),
            pltpu.VMEM((doms, parts, HD), f32),
            pltpu.VMEM((doms, parts, HD), f32),
            pltpu.SemaphoreType.DMA((9,)),
            pltpu.SemaphoreType.DMA((3 * (tps - 1),)),
            pltpu.SemaphoreType.DMA((3 * (tps - 1),)),
            pltpu.SemaphoreType.DMA((3 * (doms - 1),)),
            pltpu.SemaphoreType.DMA((3 * (doms - 1),)),
            pltpu.SemaphoreType.DMA((32,)),
            pltpu.SemaphoreType.DMA((32,)),
        ],
        compiler_params=pltpu.CompilerParams(
            collective_id=4, has_side_effects=True, vmem_limit_bytes=52 << 20
        ),
        name="layer",
    )(act, gain, wq, wk, wv, wo, ck, cv, twist, aux, cosine, sine)
    result = jax.ShapeDtypeStruct((parts, span, kvw), bf16)
    return pl.pallas_call(
        functools.partial(select_kernel, parts),
        out_shape=(
            jax.ShapeDtypeStruct((rows, width), bf16), result, result,
            jax.ShapeDtypeStruct((HD, 2 * kvw), bf16),
            jax.ShapeDtypeStruct((1, parts), f32),
        ),
        in_specs=[pl.BlockSpec(memory_space=pltpu.SMEM), vmem, vmem, vmem, hbm, hbm],
        out_specs=(vmem,) * 5,
        scratch_shapes=[pltpu.SemaphoreType.DMA((2 * parts,))],
        compiler_params=pltpu.CompilerParams(vmem_limit_bytes=8 << 20),
        name="select",
    )(anc, fresh_sel, attn, out_lw, all_k, all_v)


def plan_kernel(
    parts, doms, tps, cap, hot_cap, steps, rows,
    cnt, act, ck, cv, tab, chip_k, chip_v, act_part,
    cnt_all, send, recv, loc, sib_send, sib_recv, tp_send, tp_recv,
):
    f32, bf16, i32 = jnp.float32, jnp.bfloat16, jnp.int32
    me_d = lax.axis_index("dom")
    me_t = lax.axis_index("tp")
    core = me_d % 2
    x = (me_d // 2) % 2
    y = me_d // 4
    chip = me_d // 2
    barrier = pltpu.get_barrier_semaphore()
    for k in range(1, tps):
        pl.semaphore_signal(
            barrier, inc=1, device_id=(me_d, (me_t + k) % tps), device_id_type=MESH
        )
    for k in range(1, doms):
        pl.semaphore_signal(
            barrier, inc=1, device_id=((me_d + k) % doms, me_t), device_id_type=MESH
        )
    owns = []
    for i, (src, dst) in enumerate(((ck, chip_k), (cv, chip_v))):
        copy = pltpu.make_async_copy(src, dst.at[pl.ds(0, parts)], loc.at[i])
        copy.start()
        owns.append(copy)
    early = act.at[pl.ds(0, act_part.shape[1])]
    copy = pltpu.make_async_copy(early, act_part.at[me_t], loc.at[2])
    copy.start()
    owns.append(copy)
    cnt_all[me_d] = jnp.zeros(cnt_all.shape[1:], f32)
    cnt_all[me_d, :, :parts] = jnp.broadcast_to(cnt[...].astype(f32), (8, parts))
    pl.semaphore_wait(barrier, tps + doms - 2)
    copies = []
    for k in range(1, doms):
        copy = pltpu.make_async_remote_copy(
            src_ref=cnt_all.at[me_d], dst_ref=cnt_all.at[me_d],
            send_sem=send.at[k - 1], recv_sem=recv.at[k - 1],
            device_id=((me_d + k) % doms, me_t), device_id_type=MESH,
        )
        copy.start()
        copies.append(copy)
    swaps = []
    for k in range(1, tps):
        copy = pltpu.make_async_remote_copy(
            src_ref=early, dst_ref=act_part.at[me_t],
            send_sem=tp_send.at[k - 1], recv_sem=tp_recv.at[k - 1],
            device_id=(me_d, (me_t + k) % tps), device_id_type=MESH,
        )
        copy.start()
        swaps.append(copy)
    for i, (src, dst) in enumerate(((ck, chip_k), (cv, chip_v))):
        copy = pltpu.make_async_remote_copy(
            src_ref=src, dst_ref=dst.at[pl.ds(parts, parts)],
            send_sem=sib_send.at[i], recv_sem=sib_recv.at[i],
            device_id=(me_d + 1 - 2 * core, me_t), device_id_type=MESH,
        )
        copy.start()
        swaps.append(copy)
    for copy in copies:
        copy.wait()
    whole = parts * doms
    j = lax.broadcasted_iota(i32, (whole, HD), 0)
    lane = lax.broadcasted_iota(i32, (whole, HD), 1)
    spread = jnp.concatenate([cnt_all[d] for d in range(doms) for _ in range(parts // 8)], 0)
    column = jnp.sum(jnp.where(lane == j % parts, spread, 0.0), -1, keepdims=True)
    number = jnp.broadcast_to(column, (whole, HD))
    first = lax.broadcasted_iota(i32, (whole, whole), 0)
    second = lax.broadcasted_iota(i32, (whole, whole), 1)

    def total(mask, values):
        return jnp.dot(
            mask.astype(f32).astype(bf16), values.astype(bf16), preferred_element_type=f32
        )

    ends = total(second <= first, number)
    loads = total(second // parts == first // parts, number)
    number = number.astype(i32)
    ends = ends.astype(i32)
    starts = ends - number
    top = jnp.max(loads, (0, 1), keepdims=True)
    owner = j // parts
    heavy = jnp.min(jnp.where(loads == top, owner, doms).astype(f32), (0, 1), keepdims=True)
    heavy = heavy.astype(i32)
    light = owner != heavy
    home = j // (2 * parts)

    def needs(to):
        hit = None
        for m in range(4):
            one = (m < number) & (((starts + m) % doms) // 2 == to)
            hit = one if hit is None else hit | one
        return hit & light & (home != to)

    kind = (lane // cap) % 4
    there_x = x + kind % 2 - 2 * x * (kind % 2)
    there_y = y + kind // 2 - 2 * y * (kind // 2)
    need_send = needs(2 * there_y + there_x)
    kind = jnp.minimum(lane // 16, 2) + 1
    there_x = x + kind % 2 - 2 * x * (kind % 2)
    there_y = y + kind // 2 - 2 * y * (kind // 2)
    need_fresh = needs(2 * there_y + there_x)
    need_here = needs(jnp.broadcast_to(chip, (whole, HD)))
    need_any = needs(lane % 4)
    before = (second < first) & (second // (2 * parts) == first // (2 * parts))
    places = total(
        before,
        jnp.concatenate([u.astype(f32) for u in (need_send, need_here, need_any, need_fresh)], 1),
    ).astype(i32)
    place_send = places[:, :HD]
    place_here = places[:, HD : 2 * HD]
    place_any = places[:, 2 * HD : 3 * HD]
    place_fresh = places[:, 3 * HD :]
    local_row = j % parts + parts * (owner % 2 + core - 2 * core * (owner % 2))
    half = cap // 2
    entry = lane % cap
    picked = need_send & (place_send == 2 * (entry % half) + entry // half) & (home == chip)
    sources = jnp.sum(jnp.where(picked, local_row, 0).astype(f32), 0, keepdims=True)
    hx, hy = home % 2, home // 2
    away = (hx + x - 2 * x * hx) + 2 * (hy + y - 2 * y * hy)
    value = jnp.where(
        away == 0,
        local_row,
        jnp.where(
            light,
            3 * parts + (away - 1) * cap + place_here % 2 * half + place_here // 2,
            2 * parts + j % parts,
        ),
    )
    rank = lane * doms + me_d
    mine = (starts <= rank) & (rank < ends)
    index = jnp.sum(jnp.where(mine, value, 0).astype(f32), 0, keepdims=True)
    deep = lane % 16 // steps
    hit = need_fresh & (place_fresh == 2 * deep + core) & (lane < 48) & (deep < half)
    hot = (owner == heavy) & (lane >= 64)
    hot = hot & (j % parts == parts // 2 * core + (lane - 64) // steps)
    hot = hot & (lane < 64 + parts // 2 * steps)
    spot = local_row // parts * rows + j % parts
    hit = (hit | hot) & (home == chip)
    picks = jnp.where(hit, spot + lane % steps * parts + 1, 0).astype(f32)
    picks = jnp.sum(picks, 0, keepdims=True).astype(i32) - 1
    wide = (lane // 8) * doms + me_d
    step = lane % 8
    spot = jnp.where(
        away == 0,
        spot + step * parts,
        jnp.where(
            light,
            3 * rows + (away - 1) * 32 + place_here % 2 * 16 + place_here // 2 * steps + step,
            2 * rows + j % parts * steps + step,
        ),
    )
    chosen = (starts <= wide) & (wide < ends) & (step < steps)
    target = jnp.where(chosen, spot + 1, 0).astype(f32)
    target = jnp.sum(target, 0, keepdims=True).astype(i32) - 1
    room = jnp.where(home == heavy // 2, hot_cap, cap)
    over = jnp.max(
        (need_any & (place_any >= room)).astype(f32), (0, 1), keepdims=True
    ).astype(i32)
    base = parts * (heavy % 2 + core - 2 * core * (heavy % 2))
    branch = jnp.where(over == 0, heavy // 2, 4)
    tab[0:1, :] = sources.astype(i32)
    tab[1:2, :] = index.astype(i32)
    tab[2:3, :] = jnp.broadcast_to(base, (1, HD))
    tab[3:4, :] = target
    tab[4:5, :] = jnp.broadcast_to(branch, (1, HD))
    tab[5:6, :] = picks
    tab[6:8, :] = jnp.zeros((2, HD), i32)
    for copy in owns + swaps:
        copy.wait()


def main_kernel(
    steps, parts, doms, tps, cap, hot_cap, hot,
    act, act_part, gain, wq, wk, wv, wo, chip_k, chip_v, twist, tokens, table, prev,
    cosine, sine, tab, tabv,
    attn_out, new_k, new_v, chosen, out_lw,
    act_all, wq_v, wk_v, wv_v, wo_v, all_k, all_v, send_k, send_v,
    qs, cx, sc1, ctx_b, pair_f, hot_f, light_f, send_f, rs_send, rs_recv, sc_all, lw_all,
    loc, tp_send, tp_recv, lw_send, lw_recv,
    hv_send, hv_recv, li_send, li_recv, fr_send, fr_recv,
):
    f32, bf16 = jnp.float32, jnp.bfloat16
    me_d = lax.axis_index("dom")
    me_t = lax.axis_index("tp")
    rows, width = act.shape
    kvw = wk.shape[1]
    groups = kvw // HD
    per = wq.shape[1] // kvw
    pack = steps * per
    span = chip_k.shape[1]
    c = me_d % 2
    x = (me_d // 2) % 2
    y = me_d // 4
    sib = me_d + 1 - 2 * c
    xn = me_d + 2 - 4 * x
    yn = me_d + 4 - 8 * y
    dn = xn + 4 - 8 * y
    rx = x if hot % 2 == 0 else 1 - x
    ry = y if hot // 2 == 0 else 1 - y
    pos = (1 - c) * (3 * ry + rx * (1 - 2 * ry)) + c * (3 * rx + ry * (1 - 2 * rx))
    turn_y = (pos + c) % 2
    onward = xn + turn_y * (yn - xn)

    barrier = pltpu.get_barrier_semaphore()
    for k in range(1, tps):
        pl.semaphore_signal(
            barrier, inc=1, device_id=(me_d, (me_t + k) % tps), device_id_type=MESH
        )
    for k in range(1, doms):
        pl.semaphore_signal(
            barrier, inc=1, device_id=((me_d + k) % doms, me_t), device_id_type=MESH
        )

    def fetch(i, src, dst):
        copy = pltpu.make_async_copy(src, dst, loc.at[i])
        copy.start()
        return copy

    first = act_part.shape[1]
    later = act.at[pl.ds(first, rows - first)]
    own_act = fetch(0, later, act_all.at[me_t])
    load_k = fetch(2, wk, wk_v)
    load_v = fetch(3, wv, wv_v)
    load_q = fetch(1, wq, wq_v)
    load_o = fetch(6, wo, wo_v)
    pl.semaphore_wait(barrier, tps + doms - 2)

    def push(src, dst, ssem, rsem, to_d, to_t):
        return pltpu.make_async_remote_copy(
            src_ref=src, dst_ref=dst, send_sem=ssem, recv_sem=rsem,
            device_id=(to_d, to_t), device_id_type=MESH,
        )

    def tp_push(base, k, src, dst):
        copy = push(
            src, dst, tp_send.at[base + k - 1], tp_recv.at[base + k - 1],
            me_d, (me_t + k) % tps,
        )
        copy.start()
        return copy

    acts = [tp_push(0, k, later, act_all.at[me_t]) for k in range(1, tps)]
    lane_rows = cap // 2
    hot_lane = hot_cap // 2
    rel = rx + 2 * ry
    hot_rows = parts // 2
    chunk = hot_rows // 4

    def hot_copy(q, which, to, base):
        ref = (all_k, all_v)[which]
        area = ref.at[pl.ds(2 * parts + hot_rows * c + q * chunk, chunk)]
        i = base + q * 2 + which
        return push(area, area, hv_send.at[i], hv_recv.at[i], to, me_t)

    def forward(q, which):
        return hot_copy(q, which, onward, 0)

    def mirror(q, which):
        return hot_copy(q, which, sib, 8)

    def light_part(ref, base, piece):
        if piece == 0:
            return ref.at[pl.ds(base, hot_lane)]
        return ref.at[pl.ds(base + hot_lane, lane_rows - hot_lane)]

    def light_area(which, k, piece):
        base = 3 * parts + (k - 1) * cap + lane_rows * c
        return light_part((all_k, all_v)[which], base, piece)

    def light(k, which, piece):
        i = ((k - 1) * 2 + which) * 2 + piece
        return push(
            light_part((send_k, send_v)[which].at[k - 1], 0, piece),
            light_area(which, k, piece),
            li_send.at[i], li_recv.at[i], (xn, yn, dn)[k - 1], me_t,
        )

    def light_mirror(k, which, piece):
        i = 12 + ((k - 1) * 2 + which) * 2 + piece
        area = light_area(which, k, piece)
        return push(area, area, li_send.at[i], li_recv.at[i], sib, me_t)

    def send_lights(when, kinds, pieces):
        @pl.when(when)
        def _():
            for k in kinds:
                for piece in range(pieces):
                    for which in range(2):
                        light(k, which, piece).start()

    def arrived(k):
        for which in range(2):
            light(k, which, 0).wait_recv()
            light_mirror(k, which, 0).start()

        @pl.when(rel != k)
        def _():
            for which in range(2):
                light(k, which, 1).wait_recv()
                light_mirror(k, which, 1).start()

    @pl.when(pos == 0)
    def _():
        for i in range(hot_rows):
            at = tab[2, 0] + hot_rows * c + i
            all_k[2 * parts + hot_rows * c + i] = chip_k[at]
            all_v[2 * parts + hot_rows * c + i] = chip_v[at]
            if i % chunk == chunk - 1:
                for which in range(2):
                    forward(i // chunk, which).start()

    def gather(i, carry):
        at = tab[0, (i // lane_rows + 1) * cap + lane_rows * c + i % lane_rows]
        send_k[i // lane_rows, i % lane_rows] = chip_k[at]
        send_v[i // lane_rows, i % lane_rows] = chip_v[at]
        return carry

    lax.fori_loop(0, 3 * lane_rows, gather, 0)
    send_lights((pos == 1) & (rel == 1), (1,), 2)
    send_lights((pos == 1) & (rel == 2), (2,), 2)
    send_lights((pos == 3) & (rel == 1), (2, 1), 2)
    send_lights((pos == 3) & (rel == 2), (1, 2), 2)
    send_lights(pos == 2, (3, 2, 1), 2)
    send_lights((pos == 0) & (c == 0), (3, 1), 1)
    send_lights((pos == 0) & (c == 1), (2,), 1)
    both_k = fetch(7, chip_k, all_k.at[pl.ds(0, 2 * parts)])
    both_v = fetch(8, chip_v, all_v.at[pl.ds(0, 2 * parts)])

    def relay(*list_of):
        for where, q in list_of:

            @pl.when(pos == where)
            def _():
                for which in range(2):
                    forward(q, which).wait_recv()
                    if where < 3:
                        forward(q, which).start()
                    mirror(q, which).start()

    relay((1, 0))
    relay((1, 1))
    own_act.wait()
    for copy in acts:
        copy.wait()

    def features(t):
        return jnp.concatenate([act_part[t], act_all[t]], 0).astype(f32)

    square = jnp.zeros((rows, 1), f32)
    for t in range(tps):
        u = features(t)
        square = square + jnp.sum(u * u, -1, keepdims=True)
    inv = lax.rsqrt(square / (width * tps) + 1e-05)
    normed = []
    for t in range(tps):
        u = features(t)
        normed.append((u * inv * gain[:, t * width : (t + 1) * width]).astype(bf16))

    def project(w):
        total = None
        for t in range(tps):
            part = jnp.dot(
                normed[t], w[t * width : (t + 1) * width, :], preferred_element_type=f32
            )
            total = part if total is None else total + part
        return total

    cos_t, sin_t = cosine[...], sine[...]

    def turn(u):
        return u * cos_t + pltpu.roll(u, HD // 2, 1) * sin_t

    load_k.wait()
    load_v.wait()
    keys = project(wk_v)
    fresh = pair_f.at[0]
    for g in range(groups):
        fresh[:, g * HD : (g + 1) * HD] = turn(keys[:, g * HD : (g + 1) * HD]).astype(bf16)
    fresh[:, kvw:] = project(wv_v).astype(bf16)

    swap_f = push(fresh, pair_f.at[1], fr_send.at[0], fr_recv.at[0], sib, me_t)
    swap_f.start()

    def light_fresh(k):
        return push(
            send_f.at[k - 1], light_f.at[k - 1, c], fr_send.at[k], fr_recv.at[k],
            (xn, yn, dn)[k - 1], me_t,
        )

    def hot_fresh(k):
        return push(
            send_f.at[pl.ds(4, 2)], hot_f.at[c], fr_send.at[3 + k], fr_recv.at[3 + k],
            (xn, yn, dn)[k - 1], me_t,
        )

    def light_fresh_mirror(k):
        area = light_f.at[k - 1, c]
        return push(area, area, fr_send.at[6 + k], fr_recv.at[6 + k], sib, me_t)

    def hot_fresh_mirror():
        return push(hot_f.at[c], hot_f.at[c], fr_send.at[10], fr_recv.at[10], sib, me_t)

    load_q.wait()
    query = project(wq_v)
    for h in range(groups * per):
        g, j = h // per, h % per
        turned = turn(query[:, h * HD : (h + 1) * HD])
        for s in range(steps):
            qs[g, :, s * per + j, :] = turned[s * parts : (s + 1) * parts]
    relay((1, 2), (2, 0))
    send_lights((pos == 0) & (c == 0), (2,), 1)
    send_lights((pos == 0) & (c == 1), (3, 1), 1)
    send_lights(pos == 3, (3,), 2)

    lines = parts * pack
    row = lax.broadcasted_iota(jnp.int32, (lines, rows), 0)
    col = lax.broadcasted_iota(jnp.int32, (lines, rows), 1)
    allowed = (row // pack == col % parts) & (col // parts <= (row % pack) // per)
    scale = HD**0.5
    for g in range(groups):
        lanes = slice(g * HD, (g + 1) * HD)
        qg = qs[g].reshape(lines, HD).astype(bf16)
        for n in range(parts):
            sc1[g, n * pack : (n + 1) * pack, :] = lax.dot_general(
                qg[n * pack : (n + 1) * pack], chip_k[n, :, lanes],
                (((1,), (1,)), ((), ())), preferred_element_type=f32,
            )
        near = lax.dot_general(
            qg, fresh[:, lanes], (((1,), (1,)), ((), ())), preferred_element_type=f32
        )
        near = jnp.where(allowed, near / scale, -jnp.inf)
        far = sc1[g] / scale
        top = jnp.maximum(
            jnp.max(far, -1, keepdims=True), jnp.max(near, -1, keepdims=True)
        )
        far = jnp.exp(far - top)
        near = jnp.exp(near - top)
        mass = jnp.sum(far, -1, keepdims=True) + jnp.sum(near, -1, keepdims=True)
        far = (far / mass).astype(bf16)
        near = (near / mass).astype(bf16)
        extra = jnp.dot(
            near, fresh[:, kvw + g * HD : kvw + (g + 1) * HD], preferred_element_type=f32
        )
        for n in range(parts):
            part = slice(n * pack, (n + 1) * pack)
            cx[g, n] = extra[part] + jnp.dot(
                far[part], chip_v[n, :, lanes], preferred_element_type=f32
            )
    for h in range(groups * per):
        g, j = h // per, h % per
        for s in range(steps):
            ctx_b[s * parts : (s + 1) * parts, h * HD : (h + 1) * HD] = cx[
                g, :, s * per + j, :
            ].astype(bf16)
    load_o.wait()

    def mix(p):
        return jnp.dot(
            ctx_b[...], wo_v[:, pl.ds(pl.multiple_of(p * width, HD), width)],
            preferred_element_type=f32,
        )

    lane = lax.broadcasted_iota(jnp.int32, (rows, HD), 1)
    line = lax.broadcasted_iota(jnp.int32, (rows, HD), 0)

    def flat(column, start=0):
        return jnp.sum(jnp.where(lane == line + start, column, 0.0), 0, keepdims=True)

    count = table.shape[0]
    deep = lax.broadcasted_iota(jnp.int32, (rows, parts), 0) % parts
    broad = lax.broadcasted_iota(jnp.int32, (rows, parts), 1)
    names = jnp.concatenate(
        [jnp.broadcast_to(tokens[s : s + 1, :], (parts, parts)) for s in range(steps)], 0
    )
    name = jnp.sum(jnp.where(deep == broad, names, 0).astype(f32), -1, keepdims=True)
    name = name.astype(jnp.int32)
    entry = lax.broadcasted_iota(jnp.int32, (rows, count), 1)
    found = jnp.dot(
        (entry == name // HD).astype(f32).astype(bf16), table[...], preferred_element_type=f32
    )
    gift = flat(jnp.sum(jnp.where(lane == name % HD, found, 0.0), -1, keepdims=True))
    lw_all[me_d] = jnp.full((8, HD), -jnp.inf, f32)

    sums = []
    for k in (2, 1, 3)[: tps - 1]:
        rs_send[k - 1] = mix((me_t + k) % tps).astype(bf16)
        sums.append(tp_push(tps - 1, k, rs_send.at[k - 1], rs_recv.at[k - 1]))
    head = mix(me_t)
    swap_f.wait_recv()
    pair = pair_f[...].reshape(2 * rows, 2 * kvw)
    index = lax.broadcasted_iota(jnp.int32, (2 * rows, HD), 0)
    pick = (index == tabv[5:6, :]).astype(f32).astype(bf16)
    send_f[...] = lax.dot_general(
        pick, pair, (((0,), (0,)), ((), ())), preferred_element_type=f32
    ).astype(bf16).reshape(send_f.shape)
    for k in (3, 1, 2):
        light_fresh(k).start()

    @pl.when(pos == 0)
    def _():
        hot_f[...] = jnp.zeros(hot_f.shape, bf16)
        for k in (3, 1, 2):
            hot_fresh(k).start()

    relay((1, 3), (2, 1))
    send_lights((pos == 1) & (rel == 1), (3, 2), 2)
    send_lights((pos == 1) & (rel == 2), (3, 1), 2)
    relay((2, 2))
    relay((2, 3), (3, 0))
    for copy in sums:
        copy.wait()
    for k in range(1, tps):
        head = head + rs_recv[k - 1].astype(f32)
    attn_out[...] = head.astype(bf16)
    summed = features(me_t) + head
    along = jnp.sum(summed * twist[...], -1, keepdims=True)
    energy = jnp.sum(summed * summed, -1, keepdims=True)
    sc_all[me_t] = jnp.broadcast_to(flat(along) + flat(energy, HD // 2), (8, HD))
    scores = [
        tp_push(2 * (tps - 1), k, sc_all.at[me_t], sc_all.at[me_t]) for k in range(1, tps)
    ]
    relay((3, 1))
    for copy in scores:
        copy.wait()
    both = sc_all[0]
    for t in range(1, tps):
        both = both + sc_all[t]
    power = pltpu.roll(both, HD // 2, 1)
    score = both / jnp.sqrt(power / (width * tps) + 1e-06)
    score = jnp.where(lane[:8] < rows, score + gift, 0.0)
    total = score
    for s in range(1, steps):
        total = total + pltpu.roll(score, HD - s * parts, 1)
    mine = total[:, :parts] + jnp.broadcast_to(prev[...], (8, parts))
    lw_all[me_d, :, :parts] = mine
    lws = []
    for k in range(1, doms):
        copy = push(
            lw_all.at[me_d], lw_all.at[me_d], lw_send.at[k - 1], lw_recv.at[k - 1],
            (me_d + k) % doms, me_t,
        )
        copy.start()
        lws.append(copy)

    arrived(2)
    arrived(1)
    relay((3, 2))
    for k in (1, 2, 3):
        light_fresh(k).wait_recv()
        light_fresh_mirror(k).start()

        @pl.when(rel == k)
        def _():
            hot_fresh(k).wait_recv()
            hot_fresh_mirror().start()

    arrived(3)
    relay((3, 3))
    for k in (1, 2, 3):
        light_fresh_mirror(k).wait()

    @pl.when(pos > 0)
    def _():
        hot_fresh_mirror().wait()

    pool = jnp.concatenate(
        [
            pair_f[...].reshape(2 * rows, 2 * kvw),
            hot_f[...].reshape(rows, 2 * kvw),
            light_f[...].reshape(96, 2 * kvw),
        ],
        0,
    )
    index = lax.broadcasted_iota(jnp.int32, (3 * rows + 96, HD), 0)
    pick = (index == tabv[3:4, :]).astype(f32).astype(bf16)
    chosen[...] = lax.dot_general(
        pick, pool, (((0,), (0,)), ((), ())), preferred_element_type=f32
    ).astype(bf16)

    both_k.wait()
    both_v.wait()
    for k in (1, 2, 3):
        for which in range(2):
            light_mirror(k, which, 0).wait()

        @pl.when(rel != k)
        def _():
            for which in range(2):
                light_mirror(k, which, 1).wait()

    @pl.when(pos > 0)
    def _():
        for q in range(4):
            for which in range(2):
                mirror(q, which).wait()

    def place(i, carry):
        at = tab[1, i]
        new_k[i] = all_k[at]
        new_v[i] = all_v[at]
        return carry

    lax.fori_loop(0, parts, place, 0)

    for copy in lws:
        copy.wait()
    every_lw = lw_all[:, 0, :]
    largest = jnp.max(every_lw, (0, 1), keepdims=True)
    mass = jnp.sum(jnp.exp(every_lw - largest), (0, 1), keepdims=True)
    out_lw[...] = mine[:1] - (largest + jnp.log(mass))

    @pl.when(pos < 3)
    def _():
        for q in range(4):
            for which in range(2):
                forward(q, which).wait_send()

    for k in (1, 2, 3):
        for which in range(2):
            light(k, which, 0).wait_send()

    @pl.when(pos > 0)
    def _():
        for k in (1, 2, 3):
            for which in range(2):
                light(k, which, 1).wait_send()

    for k in (1, 2, 3):
        light_fresh(k).wait_send()
    swap_f.wait_send()

    @pl.when(pos == 0)
    def _():
        for k in (1, 2, 3):
            hot_fresh(k).wait_send()


def finish_kernel(
    parts, steps, rows_k, rows_v, chosen, attn, lw,
    out_k, out_v, out_attn, out_lw, buf_k, buf_v, sem,
):
    span, width = rows_k.shape[1:]
    group = 32
    copies = [pltpu.make_async_copy(attn, out_attn, sem.at[0])]
    copies[0].start()

    def send(buf, out, start, size):
        copy = pltpu.make_async_copy(
            buf.at[pl.ds(start, size)], out.at[pl.ds(start, size)], sem.at[len(copies)]
        )
        copy.start()
        copies.append(copy)

    for which, (src, buf, out) in enumerate(((rows_k, buf_k, out_k), (rows_v, buf_v, out_v))):
        for g in range(0, span, group):
            buf[g : g + group] = jnp.transpose(src[:, g : g + group, :], (1, 0, 2))
            send(buf, out, g, group)
        tail = chosen[:, which * width : (which + 1) * width].reshape(parts, 8, width)
        buf[span:] = jnp.transpose(tail, (1, 0, 2))[:steps]
        send(buf, out, span, steps)
    out_lw[...] = lw[...]
    for copy in copies:
        copy.wait()


def adaptive(
    activations, norm_gain, w_query, w_key, value_weight, w_output, cache_keys, cache_values,
    tokens, twisting_table, twist_vec, previous_log_weights, copy_counts,
):
    f32, bf16 = jnp.float32, jnp.bfloat16
    steps, parts, width = activations.shape
    rows = steps * parts
    span = cache_keys.shape[1]
    kvw = w_key.shape[1]
    qw = w_query.shape[1]
    groups = kvw // HD
    pack = steps * (qw // kvw)
    doms = lax.axis_size("dom")
    tps = lax.axis_size("tp")
    middle = HD // 2
    cap = CAP
    angles = (span + np.arange(rows) // parts)[:, None] * (
        500000.0 ** (-2.0 * np.arange(middle) / HD)
    )
    cosine = np.concatenate([np.cos(angles)] * 2, 1).astype(np.float32)
    sine = np.concatenate([-np.sin(angles), np.sin(angles)], 1).astype(np.float32)
    vmem = pl.BlockSpec(memory_space=pltpu.VMEM)
    smem = pl.BlockSpec(memory_space=pltpu.SMEM)
    hbm = pl.BlockSpec(memory_space=pl.ANY)
    dma = pltpu.SemaphoreType.DMA
    both = jax.ShapeDtypeStruct((2 * parts, span, kvw), bf16)
    tab, chip_k, chip_v, act_part = pl.pallas_call(
        functools.partial(plan_kernel, parts, doms, tps, cap, HOT_CAP, steps, rows),
        out_shape=(
            jax.ShapeDtypeStruct((8, HD), jnp.int32), both, both,
            jax.ShapeDtypeStruct((tps, EARLY * parts, width), bf16),
        ),
        in_specs=[vmem, hbm, hbm, hbm],
        out_specs=(vmem,) * 4,
        scratch_shapes=[
            pltpu.VMEM((doms, 8, HD), f32),
            dma((doms - 1,)), dma((doms - 1,)), dma((3,)), dma((2,)), dma((2,)),
            dma((tps - 1,)), dma((tps - 1,)),
        ],
        compiler_params=pltpu.CompilerParams(
            collective_id=5, has_side_effects=True, vmem_limit_bytes=16 << 20
        ),
        name="plan",
    )(copy_counts.reshape(1, parts), activations.reshape(rows, width), cache_keys, cache_values)

    def hot_branch(hot):
        result = jax.ShapeDtypeStruct((parts, span, kvw), bf16)
        call = pl.pallas_call(
            functools.partial(main_kernel, steps, parts, doms, tps, cap, HOT_CAP, hot),
            out_shape=(
                jax.ShapeDtypeStruct((rows, width), bf16), result, result,
                jax.ShapeDtypeStruct((HD, 2 * kvw), bf16),
                jax.ShapeDtypeStruct((1, parts), f32),
            ),
            in_specs=[hbm, vmem, vmem] + [hbm] * 4 + [vmem] * 8 + [smem, vmem],
            out_specs=(vmem,) * 5,
            scratch_shapes=[
                pltpu.VMEM((tps, rows - EARLY * parts, width), bf16),
                pltpu.VMEM(w_query.shape, bf16),
                pltpu.VMEM(w_key.shape, bf16),
                pltpu.VMEM(value_weight.shape, bf16),
                pltpu.VMEM(w_output.shape, bf16),
                pltpu.VMEM((3 * parts + 3 * cap, span, kvw), bf16),
                pltpu.VMEM((3 * parts + 3 * cap, span, kvw), bf16),
                pltpu.VMEM((3, cap // 2, span, kvw), bf16),
                pltpu.VMEM((3, cap // 2, span, kvw), bf16),
                pltpu.VMEM((groups, parts, pack, HD), f32),
                pltpu.VMEM((groups, parts, pack, HD), f32),
                pltpu.VMEM((groups, parts * pack, span), f32),
                pltpu.VMEM((rows, qw), bf16),
                pltpu.VMEM((2, rows, 2 * kvw), bf16),
                pltpu.VMEM((2, 2, 16, 2 * kvw), bf16),
                pltpu.VMEM((3, 2, 16, 2 * kvw), bf16),
                pltpu.VMEM((8, 16, 2 * kvw), bf16),
                pltpu.VMEM((tps - 1, rows, width), bf16),
                pltpu.VMEM((tps - 1, rows, width), bf16),
                pltpu.VMEM((tps, 8, HD), f32),
                pltpu.VMEM((doms, 8, HD), f32),
                dma((9,)),
                dma((3 * (tps - 1),)), dma((3 * (tps - 1),)),
                dma((doms - 1,)), dma((doms - 1,)),
                dma((16,)), dma((16,)),
                dma((24,)), dma((24,)),
                dma((11,)), dma((11,)),
            ],
            compiler_params=pltpu.CompilerParams(
                collective_id=hot, has_side_effects=True, vmem_limit_bytes=40 << 20
            ),
            name=f"main{hot}",
        )

        def run(
            act, act_part, gain, wq, wk, wv, wo, chip_k, chip_v, twist, tokens, table, prev,
            cosine, sine, tab, ck, cv, counts,
        ):
            attn, new_k, new_v, chosen, out_lw = call(
                act, act_part, gain, wq, wk, wv, wo, chip_k, chip_v, twist, tokens, table,
                prev, cosine, sine, tab, tab,
            )
            return new_k, new_v, attn, chosen, out_lw

        return run

    def every(
        act, act_part, gain, wq, wk, wv, wo, chip_k, chip_v, twist, tokens, table, prev,
        cosine, sine, tab, ck, cv, counts,
    ):
        reward = jnp.sum(table.reshape(-1)[tokens].astype(f32), 0)
        aux = jnp.stack([prev[0] + reward, counts.astype(f32)], 1)
        attn, new_k, new_v, chosen, out_lw = all_rows(
            steps, parts, act, gain, wq, wk, wv, wo, ck, cv, twist, aux, cosine, sine
        )
        return new_k, new_v, attn, chosen, out_lw

    rows_k, rows_v, attn, chosen, out_lw = lax.switch(
        tab[4, 0],
        [hot_branch(hot) for hot in range(4)] + [every],
        activations.reshape(rows, width), act_part, norm_gain.reshape(1, -1), w_query, w_key,
        value_weight, w_output, chip_k, chip_v, twist_vec.reshape(1, -1), tokens,
        twisting_table.reshape(-1, HD), previous_log_weights.reshape(1, parts),
        jnp.asarray(cosine), jnp.asarray(sine), tab, cache_keys, cache_values, copy_counts,
    )
    result = jax.ShapeDtypeStruct((span + steps, parts, kvw), bf16)
    new_k, new_v, attn, out_lw = pl.pallas_call(
        functools.partial(finish_kernel, parts, steps),
        out_shape=(
            result, result, jax.ShapeDtypeStruct((rows, width), bf16),
            jax.ShapeDtypeStruct((1, parts), f32),
        ),
        in_specs=[vmem] * 5,
        out_specs=(hbm, hbm, hbm, vmem),
        scratch_shapes=[
            pltpu.VMEM(result.shape, bf16), pltpu.VMEM(result.shape, bf16), dma((11,)),
        ],
        compiler_params=pltpu.CompilerParams(vmem_limit_bytes=8 << 20),
        name="finish",
    )(rows_k, rows_v, chosen, attn, out_lw)
    return (
        attn.reshape(steps, parts, width), jnp.transpose(new_k, (1, 0, 2)),
        jnp.transpose(new_v, (1, 0, 2)), out_lw.reshape(parts),
    )


def solution(mesh):
    body = adaptive if (mesh.shape["dom"], mesh.shape["tp"]) == (8, 4) else local
    return jax.shard_map(
        body,
        mesh=mesh,
        in_specs=(
            P(None, "dom", "tp"),
            P(),
            P(None, "tp"),
            P(None, "tp"),
            P(None, "tp"),
            P("tp", None),
            P("dom", None, "tp"),
            P("dom", None, "tp"),
            P(None, "dom"),
            P(),
            P("tp"),
            P("dom"),
            P("dom"),
        ),
        out_specs=(P(None, "dom", "tp"), P("dom", None, "tp"), P("dom", None, "tp"), P("dom")),
        check_vma=False,
    )
```

```python
import functools

import jax
import jax.numpy as jnp
import numpy as np
from jax import lax
from jax.experimental import pallas as pl
from jax.experimental.pallas import tpu as pltpu
from jax.sharding import PartitionSpec as P

D = 4096
HD = 128
CAP = 6
HOT_CAP = 4
EARLY = 1


def rotate(tensor, positions):
    middle = tensor.shape[-1] // 2
    frequency = 500000.0 ** (-2.0 * jnp.arange(middle, dtype=jnp.float32) / tensor.shape[-1])
    angles = positions[:, None] * frequency[None, :]
    cosine = jnp.cos(angles)[:, None, None, :]
    sine_part = jnp.sin(angles)[:, None, None, :]
    lower_half = tensor[..., :middle]
    upper_half = tensor[..., middle:]
    return jnp.concatenate(
        [
            lower_half * cosine - upper_half * sine_part,
            upper_half * cosine + lower_half * sine_part,
        ],
        -1,
    )


def local(
    activations,
    norm_gain,
    w_query,
    w_key,
    value_weight,
    w_output,
    cache_keys,
    cache_values,
    tokens,
    twisting_table,
    twist_vec,
    previous_log_weights,
    copy_counts,
):
    step_count = activations.shape[0]
    particle_count = activations.shape[1]
    span_old = cache_keys.shape[1]
    dom_size = lax.axis_size("dom")
    kv_local = w_key.shape[1] // HD
    q_local = w_query.shape[1] // HD
    group_size = q_local // kv_local
    all_counts = lax.all_gather(copy_counts, "dom", axis=0, tiled=True)
    copy_ends = jnp.cumsum(all_counts)
    ranks = jnp.arange(particle_count, dtype=jnp.int32) * dom_size + lax.axis_index("dom")
    ancestor = jnp.sum((copy_ends[None, :] <= ranks[:, None]).astype(jnp.int32), 1)
    all_keys = lax.all_gather(cache_keys, "dom", axis=0, tiled=True)
    all_values = lax.all_gather(cache_values, "dom", axis=0, tiled=True)

    gathered = lax.all_gather(activations, "tp", axis=2, tiled=True)
    inputs = gathered.astype(jnp.float32)
    normed = (
        inputs * lax.rsqrt(jnp.mean(inputs * inputs, -1, keepdims=True) + 1e-05) * norm_gain
    ).astype(jnp.bfloat16)
    flat_rows = normed.reshape(step_count * particle_count, D)
    positions = (span_old + jnp.arange(step_count, dtype=jnp.int32)).astype(jnp.float32)
    queries = jnp.dot(flat_rows, w_query, preferred_element_type=jnp.float32).reshape(
        step_count, particle_count, q_local, HD
    )
    queries = rotate(queries, positions).astype(jnp.bfloat16)
    fresh_keys = jnp.dot(flat_rows, w_key, preferred_element_type=jnp.float32).reshape(
        step_count, particle_count, kv_local, HD
    )
    fresh_keys = (
        rotate(fresh_keys, positions)
        .astype(jnp.bfloat16)
        .reshape(step_count, particle_count, kv_local * HD)
    )
    fresh_values = jnp.dot(flat_rows, value_weight, preferred_element_type=jnp.float32).astype(
        jnp.bfloat16
    )
    fresh_values = fresh_values.reshape(step_count, particle_count, kv_local * HD)
    fresh_keys = jnp.transpose(fresh_keys, (1, 0, 2))
    fresh_values = jnp.transpose(fresh_values, (1, 0, 2))
    key_rows = jnp.concatenate([cache_keys, fresh_keys], 1)
    value_rows = jnp.concatenate([cache_values, fresh_values], 1)
    key_span = span_old + step_count
    query_heads = queries.reshape(step_count, particle_count, kv_local, group_size, HD)
    key_heads = key_rows.reshape(particle_count, key_span, kv_local, HD)
    value_heads = value_rows.reshape(particle_count, key_span, kv_local, HD)
    scores = (
        jnp.einsum("snkgd,nlkd->snkgl", query_heads, key_heads, preferred_element_type=jnp.float32)
        / HD**0.5
    )
    allowed = (
        jnp.arange(key_span, dtype=jnp.int32)[None, :]
        <= (span_old + jnp.arange(step_count, dtype=jnp.int32))[:, None]
    )
    allowed = allowed[:, None, None, None, :]
    masked = jnp.where(allowed, scores, -jnp.inf)
    highest = jnp.max(masked, -1, keepdims=True)
    exponent = jnp.exp(masked - highest)
    weights = (exponent / jnp.sum(exponent, -1, keepdims=True)).astype(jnp.bfloat16)
    context = jnp.einsum(
        "snkgl,nlkd->snkgd", weights, value_heads, preferred_element_type=jnp.float32
    ).astype(jnp.bfloat16)
    context = context.reshape(step_count * particle_count, q_local * HD)
    partial_value = jnp.dot(context, w_output, preferred_element_type=jnp.float32).reshape(
        step_count, particle_count, D
    )
    head_mix = lax.psum_scatter(partial_value, "tp", scatter_dimension=2, tiled=True)
    attn_out = head_mix.astype(jnp.bfloat16)
    summed = activations.astype(jnp.float32) + head_mix
    aligned, energy = lax.psum(
        (jnp.sum(summed * twist_vec, -1), jnp.sum(summed * summed, -1)), "tp"
    )
    twisting_score = aligned / jnp.sqrt(energy / D + 1e-06)
    token_reward = twisting_table[tokens].astype(jnp.float32)
    particle_log_weight = previous_log_weights + jnp.sum(token_reward + twisting_score, 0)
    largest = lax.pmax(jnp.max(particle_log_weight), "dom")
    mass_total = lax.psum(jnp.sum(jnp.exp(particle_log_weight - largest)), "dom")
    out_logw = particle_log_weight - (largest + jnp.log(mass_total))
    fresh = lax.all_gather(
        jnp.concatenate([fresh_keys, fresh_values], 2), "dom", axis=0, tiled=True
    )[ancestor]
    width = fresh_keys.shape[2]
    new_keys = jnp.concatenate([all_keys[ancestor], fresh[..., :width]], 1)
    new_values = jnp.concatenate([all_values[ancestor], fresh[..., width:]], 1)
    return (attn_out, new_keys, new_values, out_logw)


MESH = pl.DeviceIdType.MESH


def layer_kernel(
    steps, parts, doms, tps,
    act, gain, wq, wk, wv, wo, ck, cv, twist, aux, cosine, sine,
    attn_out, all_k, all_v, fresh_sel, out_lw, anc_out,
    act_all, wq_v, wk_v, wv_v, wo_v, ck_v, cv_v, qs, cx, sc1, ctx_b, fresh, fresh_all,
    rs_send, rs_recv, sc_all, lw_all, cnt_all,
    loc, tp_send, tp_recv, dom_send, dom_recv, blk_send, blk_recv,
):
    f32, bf16 = jnp.float32, jnp.bfloat16
    me_d = lax.axis_index("dom")
    me_t = lax.axis_index("tp")
    rows, width = act.shape
    half = parts // 2
    kvw = wk.shape[1]
    groups = kvw // HD
    per = wq.shape[1] // kvw
    pack = steps * per
    c = me_d % 2
    x = (me_d // 2) % 2
    y = me_d // 4
    sib = me_d + 1 - 2 * c
    xn = me_d + 2 - 4 * x
    yn = me_d + 4 - 8 * y
    dn = xn + 4 - 8 * y

    barrier = pltpu.get_barrier_semaphore()
    for k in range(1, tps):
        pl.semaphore_signal(
            barrier, inc=1, device_id=(me_d, (me_t + k) % tps), device_id_type=MESH
        )
    for k in range(1, doms):
        pl.semaphore_signal(
            barrier, inc=1, device_id=((me_d + k) % doms, me_t), device_id_type=MESH
        )

    def fetch(i, src, dst):
        copy = pltpu.make_async_copy(src, dst, loc.at[i])
        copy.start()
        return copy

    own_act = fetch(0, act, act_all.at[me_t])
    load_q = fetch(1, wq, wq_v)
    load_k = fetch(2, wk, wk_v)
    load_v = fetch(3, wv, wv_v)
    load_ck = fetch(4, ck, ck_v)
    load_cv = fetch(5, cv, cv_v)
    load_o = fetch(6, wo, wo_v)

    cnt_all[me_d] = jnp.broadcast_to(aux[:, 1:], cnt_all.shape[1:])
    pl.semaphore_wait(barrier, tps + doms - 2)

    def tp_push(base, k, src, dst):
        copy = pltpu.make_async_remote_copy(
            src_ref=src, dst_ref=dst, send_sem=tp_send.at[base + k - 1],
            recv_sem=tp_recv.at[base + k - 1],
            device_id=(me_d, (me_t + k) % tps), device_id_type=MESH,
        )
        copy.start()
        return copy

    def dom_push(base, k, src, dst):
        copy = pltpu.make_async_remote_copy(
            src_ref=src, dst_ref=dst, send_sem=dom_send.at[base + k - 1],
            recv_sem=dom_recv.at[base + k - 1],
            device_id=((me_d + k) % doms, me_t), device_id_type=MESH,
        )
        copy.start()
        return copy

    acts = [tp_push(0, k, act, act_all.at[me_t]) for k in range(1, tps)]

    def piece(kind, to, which, h, slot, own):
        dst = (all_k, all_v)[which].at[slot, pl.ds(h * half, half)]
        src = (ck, cv)[which].at[pl.ds(h * half, half)] if own else dst
        i = kind * 4 + h * 2 + which
        copy = pltpu.make_async_remote_copy(
            src_ref=src, dst_ref=dst, send_sem=blk_send.at[i], recv_sem=blk_recv.at[i],
            device_id=(to, me_t), device_id_type=MESH,
        )
        copy.start()
        return copy

    moves = {}
    for h, kind, to in ((0, 0, xn), (1, 1, yn), (1, 0, xn), (0, 1, yn)):
        for which in range(2):
            moves[kind, h, which] = piece(kind, to, which, h, me_d, True)
    cnts = [dom_push(0, k, cnt_all.at[me_d], cnt_all.at[me_d]) for k in range(1, doms)]
    for h in range(2):
        for which in range(2):
            moves[3, h, which] = piece(3, sib, which, h, me_d, True)

    own_act.wait()
    for copy in acts:
        copy.wait()
    square = jnp.zeros((rows, 1), f32)
    for t in range(tps):
        u = act_all[t].astype(f32)
        square = square + jnp.sum(u * u, -1, keepdims=True)
    inv = lax.rsqrt(square / (width * tps) + 1e-05)
    normed = []
    for t in range(tps):
        u = act_all[t].astype(f32)
        normed.append((u * inv * gain[:, t * width : (t + 1) * width]).astype(bf16))

    def project(w):
        total = None
        for t in range(tps):
            part = jnp.dot(
                normed[t], w[t * width : (t + 1) * width, :], preferred_element_type=f32
            )
            total = part if total is None else total + part
        return total

    cos_t, sin_t = cosine[...], sine[...]

    def turn(u):
        return u * cos_t + pltpu.roll(u, HD // 2, 1) * sin_t

    load_k.wait()
    load_v.wait()
    keys = project(wk_v)
    for g in range(groups):
        fresh[:, g * HD : (g + 1) * HD] = turn(keys[:, g * HD : (g + 1) * HD]).astype(bf16)
    fresh[:, kvw:] = project(wv_v).astype(bf16)
    fresh_all[me_d] = fresh[...]
    news = [dom_push(doms - 1, k, fresh, fresh_all.at[me_d]) for k in range(1, doms)]
    load_q.wait()
    query = project(wq_v)
    for h in range(groups * per):
        g, j = h // per, h % per
        turned = turn(query[:, h * HD : (h + 1) * HD])
        for s in range(steps):
            qs[g, :, s * per + j, :] = turned[s * parts : (s + 1) * parts]
    load_ck.wait()
    load_cv.wait()
    put_k = fetch(7, ck_v, all_k.at[me_d])
    put_v = fetch(8, cv_v, all_v.at[me_d])

    lines = parts * pack
    row = lax.broadcasted_iota(jnp.int32, (lines, rows), 0)
    col = lax.broadcasted_iota(jnp.int32, (lines, rows), 1)
    allowed = (row // pack == col % parts) & (col // parts <= (row % pack) // per)
    scale = HD**0.5
    for g in range(groups):
        lanes = slice(g * HD, (g + 1) * HD)
        qg = qs[g].reshape(lines, HD).astype(bf16)
        for n in range(parts):
            sc1[g, n * pack : (n + 1) * pack, :] = lax.dot_general(
                qg[n * pack : (n + 1) * pack], ck_v[n, :, lanes],
                (((1,), (1,)), ((), ())), preferred_element_type=f32,
            )
        near = lax.dot_general(
            qg, fresh[:, lanes], (((1,), (1,)), ((), ())), preferred_element_type=f32
        )
        near = jnp.where(allowed, near / scale, -jnp.inf)
        far = sc1[g] / scale
        top = jnp.maximum(
            jnp.max(far, -1, keepdims=True), jnp.max(near, -1, keepdims=True)
        )
        far = jnp.exp(far - top)
        near = jnp.exp(near - top)
        mass = jnp.sum(far, -1, keepdims=True) + jnp.sum(near, -1, keepdims=True)
        far = (far / mass).astype(bf16)
        near = (near / mass).astype(bf16)
        extra = jnp.dot(
            near, fresh[:, kvw + g * HD : kvw + (g + 1) * HD], preferred_element_type=f32
        )
        for n in range(parts):
            span = slice(n * pack, (n + 1) * pack)
            cx[g, n] = extra[span] + jnp.dot(
                far[span], cv_v[n, :, lanes], preferred_element_type=f32
            )
    for h in range(groups * per):
        g, j = h // per, h % per
        for s in range(steps):
            ctx_b[s * parts : (s + 1) * parts, h * HD : (h + 1) * HD] = cx[
                g, :, s * per + j, :
            ].astype(bf16)
    load_o.wait()

    def mix(p):
        return jnp.dot(
            ctx_b[...], wo_v[:, pl.ds(pl.multiple_of(p * width, HD), width)],
            preferred_element_type=f32,
        )

    sums = []
    for k in range(1, tps):
        rs_send[k - 1] = mix((me_t + k) % tps)
        sums.append(tp_push(tps - 1, k, rs_send.at[k - 1], rs_recv.at[k - 1]))
    head = mix(me_t)

    def done(kind, h):
        for which in range(2):
            moves[kind, h, which].wait_recv()

    def relay(kind, to, h, slot):
        for which in range(2):
            moves[kind, h, which] = piece(kind, to, which, h, slot, False)

    done(0, 0)
    relay(2, yn, 0, xn)
    relay(4, sib, 0, xn)
    done(1, 1)
    relay(6, xn, 1, yn)
    relay(5, sib, 1, yn)
    for k in range(1, tps):
        sums[k - 1].wait()
        head = head + rs_recv[k - 1]
    attn_out[...] = head.astype(bf16)
    summed = act_all[me_t].astype(f32) + head
    along = jnp.sum(summed * twist[...], -1, keepdims=True)
    energy = jnp.sum(summed * summed, -1, keepdims=True)
    lane = lax.broadcasted_iota(jnp.int32, (rows, HD), 1)
    sc_all[me_t] = jnp.where(lane < HD // 2, along, energy)
    scores = [
        tp_push(2 * (tps - 1), k, sc_all.at[me_t], sc_all.at[me_t]) for k in range(1, tps)
    ]
    for copy in scores:
        copy.wait()
    both = sc_all[0]
    for t in range(1, tps):
        both = both + sc_all[t]
    score = both[:, :1] / jnp.sqrt(both[:, HD - 1 :] / (width * tps) + 1e-06)
    total = score[:parts]
    for s in range(1, steps):
        total = total + score[s * parts : (s + 1) * parts]
    mine = jnp.broadcast_to(aux[:, :1] + total, (parts, HD))
    lw_all[me_d] = mine
    lws = [
        dom_push(2 * (doms - 1), k, lw_all.at[me_d], lw_all.at[me_d]) for k in range(1, doms)
    ]

    done(0, 1)
    relay(4, sib, 1, xn)
    done(1, 0)
    relay(5, sib, 0, yn)

    for copy in cnts:
        copy.wait()
    for copy in news:
        copy.wait()
    whole = parts * doms
    number = cnt_all[...].reshape(whole, HD).astype(bf16)
    lower = lax.broadcasted_iota(jnp.int32, (whole, whole), 0)
    upper = lax.broadcasted_iota(jnp.int32, (whole, whole), 1)
    ends = jnp.dot(
        (upper <= lower).astype(f32).astype(bf16), number, preferred_element_type=f32
    )
    slot = lax.broadcasted_iota(jnp.int32, (whole, HD), 1)

    def ancestor(place):
        rank = (place * doms + me_d).astype(f32)
        return jnp.sum((ends <= rank).astype(f32), 0, keepdims=True).astype(jnp.int32)

    anc_out[...] = jnp.broadcast_to(ancestor(slot), anc_out.shape)
    lanes = lax.broadcasted_iota(jnp.int32, (1, HD), 1)
    wide = ancestor(slot // 8)
    target = (wide // parts) * rows + (lanes % 8) * parts + wide % parts
    target = jnp.where(lanes % 8 < steps, target, -1)
    index = lax.broadcasted_iota(jnp.int32, (doms * rows, HD), 0)
    pick = (index == target).astype(f32).astype(bf16)
    fresh_sel[...] = lax.dot_general(
        pick, fresh_all[...].reshape(doms * rows, 2 * kvw),
        (((0,), (0,)), ((), ())), preferred_element_type=f32,
    ).astype(bf16)

    for copy in lws:
        copy.wait()
    largest = jnp.max(lw_all[...], (0, 1), keepdims=True)[0]
    mass = jnp.sum(jnp.exp(lw_all[...] - largest[None]), (0, 1), keepdims=True)[0]
    out_lw[...] = mine - (largest + jnp.log(mass))

    done(2, 0)
    relay_d0 = [piece(7, sib, which, 0, dn, False) for which in range(2)]
    done(6, 1)
    relay_d1 = [piece(7, sib, which, 1, dn, False) for which in range(2)]
    for kind in (3, 4, 5):
        for h in range(2):
            done(kind, h)
    for copy in moves.values():
        copy.wait_send()
    for copy in relay_d0 + relay_d1:
        copy.wait()
    put_k.wait()
    put_v.wait()


def select_kernel(
    parts, anc, fresh_sel, attn, lw, all_k, all_v,
    out_attn, new_k, new_v, chosen, out_lw, sem,
):
    copies = []
    for i in range(parts):
        a = anc[0, i]
        d, n = a // parts, a % parts
        for which, (src, dst) in enumerate(((all_k, new_k), (all_v, new_v))):
            copy = pltpu.make_async_copy(src.at[d, n], dst.at[i], sem.at[2 * i + which])
            copy.start()
            copies.append(copy)
    chosen[...] = fresh_sel[...]
    out_attn[...] = attn[...]
    row = lax.broadcasted_iota(jnp.int32, (parts, parts), 0)
    col = lax.broadcasted_iota(jnp.int32, (parts, parts), 1)
    out_lw[...] = jnp.sum(jnp.where(row == col, lw[:, :1], 0.0), 0, keepdims=True)
    for copy in copies:
        copy.wait()


def all_rows(
    steps, parts, act, gain, wq, wk, wv, wo, ck, cv, twist, aux, cosine, sine,
):
    f32, bf16 = jnp.float32, jnp.bfloat16
    rows, width = act.shape
    span = ck.shape[1]
    kvw = wk.shape[1]
    qw = wq.shape[1]
    groups = kvw // HD
    pack = steps * (qw // kvw)
    doms = lax.axis_size("dom")
    tps = lax.axis_size("tp")
    vmem = pl.BlockSpec(memory_space=pltpu.VMEM)
    hbm = pl.BlockSpec(memory_space=pl.ANY)
    block = jax.ShapeDtypeStruct((doms,) + ck.shape, bf16)
    attn, all_k, all_v, fresh_sel, out_lw, anc = pl.pallas_call(
        functools.partial(layer_kernel, steps, parts, doms, tps),
        out_shape=(
            jax.ShapeDtypeStruct((rows, width), bf16), block, block,
            jax.ShapeDtypeStruct((HD, 2 * kvw), bf16),
            jax.ShapeDtypeStruct((parts, HD), f32),
            jax.ShapeDtypeStruct((8, HD), jnp.int32),
        ),
        in_specs=[hbm, vmem] + [hbm] * 6 + [vmem] * 4,
        out_specs=(vmem, hbm, hbm, vmem, vmem, vmem),
        scratch_shapes=[
            pltpu.VMEM((tps, rows, width), bf16),
            pltpu.VMEM(wq.shape, bf16),
            pltpu.VMEM(wk.shape, bf16),
            pltpu.VMEM(wv.shape, bf16),
            pltpu.VMEM(wo.shape, bf16),
            pltpu.VMEM(ck.shape, bf16),
            pltpu.VMEM(cv.shape, bf16),
            pltpu.VMEM((groups, parts, pack, HD), f32),
            pltpu.VMEM((groups, parts, pack, HD), f32),
            pltpu.VMEM((groups, parts * pack, span), f32),
            pltpu.VMEM((rows, qw), bf16),
            pltpu.VMEM((rows, 2 * kvw), bf16),
            pltpu.VMEM((doms, rows, 2 * kvw), bf16),
            pltpu.VMEM((tps - 1, rows, width), f32),
            pltpu.VMEM((tps - 1, rows, width), f32),
            pltpu.VMEM((tps, rows, HD), f32),
            pltpu.VMEM((doms, parts, HD), f32),
            pltpu.VMEM((doms, parts, HD), f32),
            pltpu.SemaphoreType.DMA((9,)),
            pltpu.SemaphoreType.DMA((3 * (tps - 1),)),
            pltpu.SemaphoreType.DMA((3 * (tps - 1),)),
            pltpu.SemaphoreType.DMA((3 * (doms - 1),)),
            pltpu.SemaphoreType.DMA((3 * (doms - 1),)),
            pltpu.SemaphoreType.DMA((32,)),
            pltpu.SemaphoreType.DMA((32,)),
        ],
        compiler_params=pltpu.CompilerParams(
            collective_id=4, has_side_effects=True, vmem_limit_bytes=52 << 20
        ),
        name="layer",
    )(act, gain, wq, wk, wv, wo, ck, cv, twist, aux, cosine, sine)
    result = jax.ShapeDtypeStruct((parts, span, kvw), bf16)
    return pl.pallas_call(
        functools.partial(select_kernel, parts),
        out_shape=(
            jax.ShapeDtypeStruct((rows, width), bf16), result, result,
            jax.ShapeDtypeStruct((HD, 2 * kvw), bf16),
            jax.ShapeDtypeStruct((1, parts), f32),
        ),
        in_specs=[pl.BlockSpec(memory_space=pltpu.SMEM), vmem, vmem, vmem, hbm, hbm],
        out_specs=(vmem,) * 5,
        scratch_shapes=[pltpu.SemaphoreType.DMA((2 * parts,))],
        compiler_params=pltpu.CompilerParams(vmem_limit_bytes=8 << 20),
        name="select",
    )(anc, fresh_sel, attn, out_lw, all_k, all_v)


def plan_kernel(
    parts, doms, tps, cap, hot_cap, steps, rows,
    cnt, act, ck, cv, tab, chip_k, chip_v, act_part,
    cnt_all, send, recv, loc, sib_send, sib_recv, tp_send, tp_recv,
):
    f32, bf16, i32 = jnp.float32, jnp.bfloat16, jnp.int32
    me_d = lax.axis_index("dom")
    me_t = lax.axis_index("tp")
    core = me_d % 2
    x = (me_d // 2) % 2
    y = me_d // 4
    chip = me_d // 2
    barrier = pltpu.get_barrier_semaphore()
    for k in range(1, tps):
        pl.semaphore_signal(
            barrier, inc=1, device_id=(me_d, (me_t + k) % tps), device_id_type=MESH
        )
    for k in range(1, doms):
        pl.semaphore_signal(
            barrier, inc=1, device_id=((me_d + k) % doms, me_t), device_id_type=MESH
        )
    owns = []
    for i, (src, dst) in enumerate(((ck, chip_k), (cv, chip_v))):
        copy = pltpu.make_async_copy(src, dst.at[pl.ds(0, parts)], loc.at[i])
        copy.start()
        owns.append(copy)
    early = act.at[pl.ds(0, act_part.shape[1])]
    copy = pltpu.make_async_copy(early, act_part.at[me_t], loc.at[2])
    copy.start()
    owns.append(copy)
    cnt_all[me_d] = jnp.zeros(cnt_all.shape[1:], f32)
    cnt_all[me_d, :, :parts] = jnp.broadcast_to(cnt[...].astype(f32), (8, parts))
    pl.semaphore_wait(barrier, tps + doms - 2)
    copies = []
    for k in range(1, doms):
        copy = pltpu.make_async_remote_copy(
            src_ref=cnt_all.at[me_d], dst_ref=cnt_all.at[me_d],
            send_sem=send.at[k - 1], recv_sem=recv.at[k - 1],
            device_id=((me_d + k) % doms, me_t), device_id_type=MESH,
        )
        copy.start()
        copies.append(copy)
    swaps = []
    for k in range(1, tps):
        copy = pltpu.make_async_remote_copy(
            src_ref=early, dst_ref=act_part.at[me_t],
            send_sem=tp_send.at[k - 1], recv_sem=tp_recv.at[k - 1],
            device_id=(me_d, (me_t + k) % tps), device_id_type=MESH,
        )
        copy.start()
        swaps.append(copy)
    for i, (src, dst) in enumerate(((ck, chip_k), (cv, chip_v))):
        copy = pltpu.make_async_remote_copy(
            src_ref=src, dst_ref=dst.at[pl.ds(parts, parts)],
            send_sem=sib_send.at[i], recv_sem=sib_recv.at[i],
            device_id=(me_d + 1 - 2 * core, me_t), device_id_type=MESH,
        )
        copy.start()
        swaps.append(copy)
    for copy in copies:
        copy.wait()
    whole = parts * doms
    j = lax.broadcasted_iota(i32, (whole, HD), 0)
    lane = lax.broadcasted_iota(i32, (whole, HD), 1)
    spread = jnp.concatenate([cnt_all[d] for d in range(doms) for _ in range(parts // 8)], 0)
    column = jnp.sum(jnp.where(lane == j % parts, spread, 0.0), -1, keepdims=True)
    number = jnp.broadcast_to(column, (whole, HD))
    first = lax.broadcasted_iota(i32, (whole, whole), 0)
    second = lax.broadcasted_iota(i32, (whole, whole), 1)

    def total(mask, values):
        return jnp.dot(
            mask.astype(f32).astype(bf16), values.astype(bf16), preferred_element_type=f32
        )

    ends = total(second <= first, number)
    loads = total(second // parts == first // parts, number)
    number = number.astype(i32)
    ends = ends.astype(i32)
    starts = ends - number
    top = jnp.max(loads, (0, 1), keepdims=True)
    owner = j // parts
    heavy = jnp.min(jnp.where(loads == top, owner, doms).astype(f32), (0, 1), keepdims=True)
    heavy = heavy.astype(i32)
    light = owner != heavy
    home = j // (2 * parts)

    def needs(to):
        hit = None
        for m in range(4):
            one = (m < number) & (((starts + m) % doms) // 2 == to)
            hit = one if hit is None else hit | one
        return hit & light & (home != to)

    kind = (lane // cap) % 4
    there_x = x + kind % 2 - 2 * x * (kind % 2)
    there_y = y + kind // 2 - 2 * y * (kind // 2)
    need_send = needs(2 * there_y + there_x)
    kind = jnp.minimum(lane // 16, 2) + 1
    there_x = x + kind % 2 - 2 * x * (kind % 2)
    there_y = y + kind // 2 - 2 * y * (kind // 2)
    need_fresh = needs(2 * there_y + there_x)
    need_here = needs(jnp.broadcast_to(chip, (whole, HD)))
    need_any = needs(lane % 4)
    before = (second < first) & (second // (2 * parts) == first // (2 * parts))
    places = total(
        before,
        jnp.concatenate([u.astype(f32) for u in (need_send, need_here, need_any, need_fresh)], 1),
    ).astype(i32)
    place_send = places[:, :HD]
    place_here = places[:, HD : 2 * HD]
    place_any = places[:, 2 * HD : 3 * HD]
    place_fresh = places[:, 3 * HD :]
    local_row = j % parts + parts * (owner % 2 + core - 2 * core * (owner % 2))
    half = cap // 2
    entry = lane % cap
    picked = need_send & (place_send == 2 * (entry % half) + entry // half) & (home == chip)
    sources = jnp.sum(jnp.where(picked, local_row, 0).astype(f32), 0, keepdims=True)
    hx, hy = home % 2, home // 2
    away = (hx + x - 2 * x * hx) + 2 * (hy + y - 2 * y * hy)
    value = jnp.where(
        away == 0,
        local_row,
        jnp.where(
            light,
            3 * parts + (away - 1) * cap + place_here % 2 * half + place_here // 2,
            2 * parts + j % parts,
        ),
    )
    rank = lane * doms + me_d
    mine = (starts <= rank) & (rank < ends)
    index = jnp.sum(jnp.where(mine, value, 0).astype(f32), 0, keepdims=True)
    deep = lane % 16 // steps
    hit = need_fresh & (place_fresh == 2 * deep + core) & (lane < 48) & (deep < half)
    hot = (owner == heavy) & (lane >= 64)
    hot = hot & (j % parts == parts // 2 * core + (lane - 64) // steps)
    hot = hot & (lane < 64 + parts // 2 * steps)
    spot = local_row // parts * rows + j % parts
    hit = (hit | hot) & (home == chip)
    picks = jnp.where(hit, spot + lane % steps * parts + 1, 0).astype(f32)
    picks = jnp.sum(picks, 0, keepdims=True).astype(i32) - 1
    wide = (lane // 8) * doms + me_d
    step = lane % 8
    spot = jnp.where(
        away == 0,
        spot + step * parts,
        jnp.where(
            light,
            3 * rows + (away - 1) * 32 + place_here % 2 * 16 + place_here // 2 * steps + step,
            2 * rows + j % parts * steps + step,
        ),
    )
    chosen = (starts <= wide) & (wide < ends) & (step < steps)
    target = jnp.where(chosen, spot + 1, 0).astype(f32)
    target = jnp.sum(target, 0, keepdims=True).astype(i32) - 1
    room = jnp.where(home == heavy // 2, hot_cap, cap)
    over = jnp.max(
        (need_any & (place_any >= room)).astype(f32), (0, 1), keepdims=True
    ).astype(i32)
    base = parts * (heavy % 2 + core - 2 * core * (heavy % 2))
    branch = jnp.where(over == 0, heavy // 2, 4)
    tab[0:1, :] = sources.astype(i32)
    tab[1:2, :] = index.astype(i32)
    tab[2:3, :] = jnp.broadcast_to(base, (1, HD))
    tab[3:4, :] = target
    tab[4:5, :] = jnp.broadcast_to(branch, (1, HD))
    tab[5:6, :] = picks
    tab[6:8, :] = jnp.zeros((2, HD), i32)
    for copy in owns + swaps:
        copy.wait()


def main_kernel(
    steps, parts, doms, tps, cap, hot_cap, hot,
    act, act_part, gain, wq, wk, wv, wo, chip_k, chip_v, twist, tokens, table, prev,
    cosine, sine, tab, tabv,
    attn_out, new_k, new_v, chosen, out_lw,
    act_all, wq_v, wk_v, wv_v, wo_v, all_k, all_v, send_k, send_v,
    qs, cx, sc1, ctx_b, pair_f, hot_f, light_f, send_f, rs_send, rs_recv, sc_all, lw_all,
    loc, tp_send, tp_recv, lw_send, lw_recv,
    hv_send, hv_recv, li_send, li_recv, fr_send, fr_recv,
):
    f32, bf16 = jnp.float32, jnp.bfloat16
    me_d = lax.axis_index("dom")
    me_t = lax.axis_index("tp")
    rows, width = act.shape
    kvw = wk.shape[1]
    groups = kvw // HD
    per = wq.shape[1] // kvw
    pack = steps * per
    span = chip_k.shape[1]
    c = me_d % 2
    x = (me_d // 2) % 2
    y = me_d // 4
    sib = me_d + 1 - 2 * c
    xn = me_d + 2 - 4 * x
    yn = me_d + 4 - 8 * y
    dn = xn + 4 - 8 * y
    rx = x if hot % 2 == 0 else 1 - x
    ry = y if hot // 2 == 0 else 1 - y
    pos = (1 - c) * (3 * ry + rx * (1 - 2 * ry)) + c * (3 * rx + ry * (1 - 2 * rx))
    turn_y = (pos + c) % 2
    onward = xn + turn_y * (yn - xn)

    barrier = pltpu.get_barrier_semaphore()
    for k in range(1, tps):
        pl.semaphore_signal(
            barrier, inc=1, device_id=(me_d, (me_t + k) % tps), device_id_type=MESH
        )
    for k in range(1, doms):
        pl.semaphore_signal(
            barrier, inc=1, device_id=((me_d + k) % doms, me_t), device_id_type=MESH
        )

    def fetch(i, src, dst):
        copy = pltpu.make_async_copy(src, dst, loc.at[i])
        copy.start()
        return copy

    first = act_part.shape[1]
    later = act.at[pl.ds(first, rows - first)]
    own_act = fetch(0, later, act_all.at[me_t])
    load_k = fetch(2, wk, wk_v)
    load_v = fetch(3, wv, wv_v)
    load_q = fetch(1, wq, wq_v)
    load_o = fetch(6, wo, wo_v)
    pl.semaphore_wait(barrier, tps + doms - 2)

    def push(src, dst, ssem, rsem, to_d, to_t):
        return pltpu.make_async_remote_copy(
            src_ref=src, dst_ref=dst, send_sem=ssem, recv_sem=rsem,
            device_id=(to_d, to_t), device_id_type=MESH,
        )

    def tp_push(base, k, src, dst):
        copy = push(
            src, dst, tp_send.at[base + k - 1], tp_recv.at[base + k - 1],
            me_d, (me_t + k) % tps,
        )
        copy.start()
        return copy

    acts = [tp_push(0, k, later, act_all.at[me_t]) for k in range(1, tps)]
    lane_rows = cap // 2
    hot_lane = hot_cap // 2
    rel = rx + 2 * ry
    hot_rows = parts // 2
    chunk = hot_rows // 4

    def hot_copy(q, which, to, base):
        ref = (all_k, all_v)[which]
        area = ref.at[pl.ds(2 * parts + hot_rows * c + q * chunk, chunk)]
        i = base + q * 2 + which
        return push(area, area, hv_send.at[i], hv_recv.at[i], to, me_t)

    def forward(q, which):
        return hot_copy(q, which, onward, 0)

    def mirror(q, which):
        return hot_copy(q, which, sib, 8)

    def light_part(ref, base, piece):
        if piece == 0:
            return ref.at[pl.ds(base, hot_lane)]
        return ref.at[pl.ds(base + hot_lane, lane_rows - hot_lane)]

    def light_area(which, k, piece):
        base = 3 * parts + (k - 1) * cap + lane_rows * c
        return light_part((all_k, all_v)[which], base, piece)

    def light(k, which, piece):
        i = ((k - 1) * 2 + which) * 2 + piece
        return push(
            light_part((send_k, send_v)[which].at[k - 1], 0, piece),
            light_area(which, k, piece),
            li_send.at[i], li_recv.at[i], (xn, yn, dn)[k - 1], me_t,
        )

    def light_mirror(k, which, piece):
        i = 12 + ((k - 1) * 2 + which) * 2 + piece
        area = light_area(which, k, piece)
        return push(area, area, li_send.at[i], li_recv.at[i], sib, me_t)

    def send_lights(when, kinds, pieces):
        @pl.when(when)
        def _():
            for k in kinds:
                for piece in range(pieces):
                    for which in range(2):
                        light(k, which, piece).start()

    def arrived(k):
        for which in range(2):
            light(k, which, 0).wait_recv()
            light_mirror(k, which, 0).start()

        @pl.when(rel != k)
        def _():
            for which in range(2):
                light(k, which, 1).wait_recv()
                light_mirror(k, which, 1).start()

    @pl.when(pos == 0)
    def _():
        for i in range(hot_rows):
            at = tab[2, 0] + hot_rows * c + i
            all_k[2 * parts + hot_rows * c + i] = chip_k[at]
            all_v[2 * parts + hot_rows * c + i] = chip_v[at]
            if i % chunk == chunk - 1:
                for which in range(2):
                    forward(i // chunk, which).start()

    def gather(i, carry):
        at = tab[0, (i // lane_rows + 1) * cap + lane_rows * c + i % lane_rows]
        send_k[i // lane_rows, i % lane_rows] = chip_k[at]
        send_v[i // lane_rows, i % lane_rows] = chip_v[at]
        return carry

    lax.fori_loop(0, 3 * lane_rows, gather, 0)
    send_lights((pos == 1) & (rel == 1), (1,), 2)
    send_lights((pos == 1) & (rel == 2), (2,), 2)
    send_lights((pos == 3) & (rel == 1), (2, 1), 2)
    send_lights((pos == 3) & (rel == 2), (1, 2), 2)
    send_lights(pos == 2, (3, 2, 1), 2)
    send_lights((pos == 0) & (c == 0), (3, 1), 1)
    send_lights((pos == 0) & (c == 1), (2,), 1)
    both_k = fetch(7, chip_k, all_k.at[pl.ds(0, 2 * parts)])
    both_v = fetch(8, chip_v, all_v.at[pl.ds(0, 2 * parts)])

    def relay(*list_of):
        for where, q in list_of:

            @pl.when(pos == where)
            def _():
                for which in range(2):
                    forward(q, which).wait_recv()
                    if where < 3:
                        forward(q, which).start()
                    mirror(q, which).start()

    relay((1, 0))
    relay((1, 1))
    own_act.wait()
    for copy in acts:
        copy.wait()

    def features(t):
        return jnp.concatenate([act_part[t], act_all[t]], 0).astype(f32)

    square = jnp.zeros((rows, 1), f32)
    for t in range(tps):
        u = features(t)
        square = square + jnp.sum(u * u, -1, keepdims=True)
    inv = lax.rsqrt(square / (width * tps) + 1e-05)
    normed = []
    for t in range(tps):
        u = features(t)
        normed.append((u * inv * gain[:, t * width : (t + 1) * width]).astype(bf16))

    def project(w):
        total = None
        for t in range(tps):
            part = jnp.dot(
                normed[t], w[t * width : (t + 1) * width, :], preferred_element_type=f32
            )
            total = part if total is None else total + part
        return total

    cos_t, sin_t = cosine[...], sine[...]

    def turn(u):
        return u * cos_t + pltpu.roll(u, HD // 2, 1) * sin_t

    load_k.wait()
    load_v.wait()
    keys = project(wk_v)
    fresh = pair_f.at[0]
    for g in range(groups):
        fresh[:, g * HD : (g + 1) * HD] = turn(keys[:, g * HD : (g + 1) * HD]).astype(bf16)
    fresh[:, kvw:] = project(wv_v).astype(bf16)

    swap_f = push(fresh, pair_f.at[1], fr_send.at[0], fr_recv.at[0], sib, me_t)
    swap_f.start()

    def light_fresh(k):
        return push(
            send_f.at[k - 1], light_f.at[k - 1, c], fr_send.at[k], fr_recv.at[k],
            (xn, yn, dn)[k - 1], me_t,
        )

    def hot_fresh(k):
        return push(
            send_f.at[pl.ds(4, 2)], hot_f.at[c], fr_send.at[3 + k], fr_recv.at[3 + k],
            (xn, yn, dn)[k - 1], me_t,
        )

    def light_fresh_mirror(k):
        area = light_f.at[k - 1, c]
        return push(area, area, fr_send.at[6 + k], fr_recv.at[6 + k], sib, me_t)

    def hot_fresh_mirror():
        return push(hot_f.at[c], hot_f.at[c], fr_send.at[10], fr_recv.at[10], sib, me_t)

    load_q.wait()
    query = project(wq_v)
    for h in range(groups * per):
        g, j = h // per, h % per
        turned = turn(query[:, h * HD : (h + 1) * HD])
        for s in range(steps):
            qs[g, :, s * per + j, :] = turned[s * parts : (s + 1) * parts]
    relay((1, 2), (2, 0))
    send_lights((pos == 1) & (rel == 1), (3,), 2)
    send_lights((pos == 0) & (c == 0), (2,), 1)
    send_lights((pos == 0) & (c == 1), (3, 1), 1)
    send_lights(pos == 3, (3,), 2)

    lines = parts * pack
    row = lax.broadcasted_iota(jnp.int32, (lines, rows), 0)
    col = lax.broadcasted_iota(jnp.int32, (lines, rows), 1)
    allowed = (row // pack == col % parts) & (col // parts <= (row % pack) // per)
    scale = HD**0.5
    for g in range(groups):
        lanes = slice(g * HD, (g + 1) * HD)
        qg = qs[g].reshape(lines, HD).astype(bf16)
        for n in range(parts):
            sc1[g, n * pack : (n + 1) * pack, :] = lax.dot_general(
                qg[n * pack : (n + 1) * pack], chip_k[n, :, lanes],
                (((1,), (1,)), ((), ())), preferred_element_type=f32,
            )
        near = lax.dot_general(
            qg, fresh[:, lanes], (((1,), (1,)), ((), ())), preferred_element_type=f32
        )
        near = jnp.where(allowed, near / scale, -jnp.inf)
        far = sc1[g] / scale
        top = jnp.maximum(
            jnp.max(far, -1, keepdims=True), jnp.max(near, -1, keepdims=True)
        )
        far = jnp.exp(far - top)
        near = jnp.exp(near - top)
        mass = jnp.sum(far, -1, keepdims=True) + jnp.sum(near, -1, keepdims=True)
        far = (far / mass).astype(bf16)
        near = (near / mass).astype(bf16)
        extra = jnp.dot(
            near, fresh[:, kvw + g * HD : kvw + (g + 1) * HD], preferred_element_type=f32
        )
        for n in range(parts):
            part = slice(n * pack, (n + 1) * pack)
            cx[g, n] = extra[part] + jnp.dot(
                far[part], chip_v[n, :, lanes], preferred_element_type=f32
            )
    for h in range(groups * per):
        g, j = h // per, h % per
        for s in range(steps):
            ctx_b[s * parts : (s + 1) * parts, h * HD : (h + 1) * HD] = cx[
                g, :, s * per + j, :
            ].astype(bf16)
    load_o.wait()

    def mix(p):
        return jnp.dot(
            ctx_b[...], wo_v[:, pl.ds(pl.multiple_of(p * width, HD), width)],
            preferred_element_type=f32,
        )

    lane = lax.broadcasted_iota(jnp.int32, (rows, HD), 1)
    line = lax.broadcasted_iota(jnp.int32, (rows, HD), 0)

    def flat(column, start=0):
        return jnp.sum(jnp.where(lane == line + start, column, 0.0), 0, keepdims=True)

    count = table.shape[0]
    deep = lax.broadcasted_iota(jnp.int32, (rows, parts), 0) % parts
    broad = lax.broadcasted_iota(jnp.int32, (rows, parts), 1)
    names = jnp.concatenate(
        [jnp.broadcast_to(tokens[s : s + 1, :], (parts, parts)) for s in range(steps)], 0
    )
    name = jnp.sum(jnp.where(deep == broad, names, 0).astype(f32), -1, keepdims=True)
    name = name.astype(jnp.int32)
    entry = lax.broadcasted_iota(jnp.int32, (rows, count), 1)
    found = jnp.dot(
        (entry == name // HD).astype(f32).astype(bf16), table[...], preferred_element_type=f32
    )
    gift = flat(jnp.sum(jnp.where(lane == name % HD, found, 0.0), -1, keepdims=True))
    lw_all[me_d] = jnp.full((8, HD), -jnp.inf, f32)

    sums = []
    for k in (2, 1, 3)[: tps - 1]:
        rs_send[k - 1] = mix((me_t + k) % tps).astype(bf16)
        sums.append(tp_push(tps - 1, k, rs_send.at[k - 1], rs_recv.at[k - 1]))
    head = mix(me_t)
    swap_f.wait_recv()
    pair = pair_f[...].reshape(2 * rows, 2 * kvw)
    index = lax.broadcasted_iota(jnp.int32, (2 * rows, HD), 0)
    pick = (index == tabv[5:6, :]).astype(f32).astype(bf16)
    send_f[...] = lax.dot_general(
        pick, pair, (((0,), (0,)), ((), ())), preferred_element_type=f32
    ).astype(bf16).reshape(send_f.shape)
    for k in (3, 1, 2):
        light_fresh(k).start()

    @pl.when(pos == 0)
    def _():
        hot_f[...] = jnp.zeros(hot_f.shape, bf16)
        for k in (3, 1, 2):
            hot_fresh(k).start()

    relay((1, 3), (2, 1))
    send_lights((pos == 1) & (rel == 1), (2,), 2)
    send_lights((pos == 1) & (rel == 2), (3, 1), 2)
    relay((2, 2))
    relay((2, 3), (3, 0))
    for copy in sums:
        copy.wait()
    for k in range(1, tps):
        head = head + rs_recv[k - 1].astype(f32)
    attn_out[...] = head.astype(bf16)
    summed = features(me_t) + head
    along = jnp.sum(summed * twist[...], -1, keepdims=True)
    energy = jnp.sum(summed * summed, -1, keepdims=True)
    sc_all[me_t] = jnp.broadcast_to(flat(along) + flat(energy, HD // 2), (8, HD))
    scores = [
        tp_push(2 * (tps - 1), k, sc_all.at[me_t], sc_all.at[me_t]) for k in range(1, tps)
    ]
    relay((3, 1))
    for copy in scores:
        copy.wait()
    both = sc_all[0]
    for t in range(1, tps):
        both = both + sc_all[t]
    power = pltpu.roll(both, HD // 2, 1)
    score = both / jnp.sqrt(power / (width * tps) + 1e-06)
    score = jnp.where(lane[:8] < rows, score + gift, 0.0)
    total = score
    for s in range(1, steps):
        total = total + pltpu.roll(score, HD - s * parts, 1)
    mine = total[:, :parts] + jnp.broadcast_to(prev[...], (8, parts))
    lw_all[me_d, :, :parts] = mine
    lws = []
    for k in range(1, doms):
        copy = push(
            lw_all.at[me_d], lw_all.at[me_d], lw_send.at[k - 1], lw_recv.at[k - 1],
            (me_d + k) % doms, me_t,
        )
        copy.start()
        lws.append(copy)

    arrived(2)
    arrived(1)
    relay((3, 2))
    for k in (1, 2, 3):
        light_fresh(k).wait_recv()
        light_fresh_mirror(k).start()

        @pl.when(rel == k)
        def _():
            hot_fresh(k).wait_recv()
            hot_fresh_mirror().start()

    arrived(3)
    relay((3, 3))
    for k in (1, 2, 3):
        light_fresh_mirror(k).wait()

    @pl.when(pos > 0)
    def _():
        hot_fresh_mirror().wait()

    pool = jnp.concatenate(
        [
            pair_f[...].reshape(2 * rows, 2 * kvw),
            hot_f[...].reshape(rows, 2 * kvw),
            light_f[...].reshape(96, 2 * kvw),
        ],
        0,
    )
    index = lax.broadcasted_iota(jnp.int32, (3 * rows + 96, HD), 0)
    pick = (index == tabv[3:4, :]).astype(f32).astype(bf16)
    chosen[...] = lax.dot_general(
        pick, pool, (((0,), (0,)), ((), ())), preferred_element_type=f32
    ).astype(bf16)

    both_k.wait()
    both_v.wait()
    for k in (1, 2, 3):
        for which in range(2):
            light_mirror(k, which, 0).wait()

        @pl.when(rel != k)
        def _():
            for which in range(2):
                light_mirror(k, which, 1).wait()

    @pl.when(pos > 0)
    def _():
        for q in range(4):
            for which in range(2):
                mirror(q, which).wait()

    def place(i, carry):
        at = tab[1, i]
        new_k[i] = all_k[at]
        new_v[i] = all_v[at]
        return carry

    lax.fori_loop(0, parts, place, 0)

    for copy in lws:
        copy.wait()
    every_lw = lw_all[:, 0, :]
    largest = jnp.max(every_lw, (0, 1), keepdims=True)
    mass = jnp.sum(jnp.exp(every_lw - largest), (0, 1), keepdims=True)
    out_lw[...] = mine[:1] - (largest + jnp.log(mass))

    @pl.when(pos < 3)
    def _():
        for q in range(4):
            for which in range(2):
                forward(q, which).wait_send()

    for k in (1, 2, 3):
        for which in range(2):
            light(k, which, 0).wait_send()

    @pl.when(pos > 0)
    def _():
        for k in (1, 2, 3):
            for which in range(2):
                light(k, which, 1).wait_send()

    for k in (1, 2, 3):
        light_fresh(k).wait_send()
    swap_f.wait_send()

    @pl.when(pos == 0)
    def _():
        for k in (1, 2, 3):
            hot_fresh(k).wait_send()


def finish_kernel(
    parts, steps, rows_k, rows_v, chosen, attn, lw,
    out_k, out_v, out_attn, out_lw, buf_k, buf_v, sem,
):
    span, width = rows_k.shape[1:]
    group = 32
    copies = [pltpu.make_async_copy(attn, out_attn, sem.at[0])]
    copies[0].start()

    def send(buf, out, start, size):
        copy = pltpu.make_async_copy(
            buf.at[pl.ds(start, size)], out.at[pl.ds(start, size)], sem.at[len(copies)]
        )
        copy.start()
        copies.append(copy)

    for which, (src, buf, out) in enumerate(((rows_k, buf_k, out_k), (rows_v, buf_v, out_v))):
        for g in range(0, span, group):
            buf[g : g + group] = jnp.transpose(src[:, g : g + group, :], (1, 0, 2))
            send(buf, out, g, group)
        tail = chosen[:, which * width : (which + 1) * width].reshape(parts, 8, width)
        buf[span:] = jnp.transpose(tail, (1, 0, 2))[:steps]
        send(buf, out, span, steps)
    out_lw[...] = lw[...]
    for copy in copies:
        copy.wait()


def adaptive(
    activations, norm_gain, w_query, w_key, value_weight, w_output, cache_keys, cache_values,
    tokens, twisting_table, twist_vec, previous_log_weights, copy_counts,
):
    f32, bf16 = jnp.float32, jnp.bfloat16
    steps, parts, width = activations.shape
    rows = steps * parts
    span = cache_keys.shape[1]
    kvw = w_key.shape[1]
    qw = w_query.shape[1]
    groups = kvw // HD
    pack = steps * (qw // kvw)
    doms = lax.axis_size("dom")
    tps = lax.axis_size("tp")
    middle = HD // 2
    cap = CAP
    angles = (span + np.arange(rows) // parts)[:, None] * (
        500000.0 ** (-2.0 * np.arange(middle) / HD)
    )
    cosine = np.concatenate([np.cos(angles)] * 2, 1).astype(np.float32)
    sine = np.concatenate([-np.sin(angles), np.sin(angles)], 1).astype(np.float32)
    vmem = pl.BlockSpec(memory_space=pltpu.VMEM)
    smem = pl.BlockSpec(memory_space=pltpu.SMEM)
    hbm = pl.BlockSpec(memory_space=pl.ANY)
    dma = pltpu.SemaphoreType.DMA
    both = jax.ShapeDtypeStruct((2 * parts, span, kvw), bf16)
    tab, chip_k, chip_v, act_part = pl.pallas_call(
        functools.partial(plan_kernel, parts, doms, tps, cap, HOT_CAP, steps, rows),
        out_shape=(
            jax.ShapeDtypeStruct((8, HD), jnp.int32), both, both,
            jax.ShapeDtypeStruct((tps, EARLY * parts, width), bf16),
        ),
        in_specs=[vmem, hbm, hbm, hbm],
        out_specs=(vmem,) * 4,
        scratch_shapes=[
            pltpu.VMEM((doms, 8, HD), f32),
            dma((doms - 1,)), dma((doms - 1,)), dma((3,)), dma((2,)), dma((2,)),
            dma((tps - 1,)), dma((tps - 1,)),
        ],
        compiler_params=pltpu.CompilerParams(
            collective_id=5, has_side_effects=True, vmem_limit_bytes=16 << 20
        ),
        name="plan",
    )(copy_counts.reshape(1, parts), activations.reshape(rows, width), cache_keys, cache_values)

    def hot_branch(hot):
        result = jax.ShapeDtypeStruct((parts, span, kvw), bf16)
        call = pl.pallas_call(
            functools.partial(main_kernel, steps, parts, doms, tps, cap, HOT_CAP, hot),
            out_shape=(
                jax.ShapeDtypeStruct((rows, width), bf16), result, result,
                jax.ShapeDtypeStruct((HD, 2 * kvw), bf16),
                jax.ShapeDtypeStruct((1, parts), f32),
            ),
            in_specs=[hbm, vmem, vmem] + [hbm] * 4 + [vmem] * 8 + [smem, vmem],
            out_specs=(vmem,) * 5,
            scratch_shapes=[
                pltpu.VMEM((tps, rows - EARLY * parts, width), bf16),
                pltpu.VMEM(w_query.shape, bf16),
                pltpu.VMEM(w_key.shape, bf16),
                pltpu.VMEM(value_weight.shape, bf16),
                pltpu.VMEM(w_output.shape, bf16),
                pltpu.VMEM((3 * parts + 3 * cap, span, kvw), bf16),
                pltpu.VMEM((3 * parts + 3 * cap, span, kvw), bf16),
                pltpu.VMEM((3, cap // 2, span, kvw), bf16),
                pltpu.VMEM((3, cap // 2, span, kvw), bf16),
                pltpu.VMEM((groups, parts, pack, HD), f32),
                pltpu.VMEM((groups, parts, pack, HD), f32),
                pltpu.VMEM((groups, parts * pack, span), f32),
                pltpu.VMEM((rows, qw), bf16),
                pltpu.VMEM((2, rows, 2 * kvw), bf16),
                pltpu.VMEM((2, 2, 16, 2 * kvw), bf16),
                pltpu.VMEM((3, 2, 16, 2 * kvw), bf16),
                pltpu.VMEM((8, 16, 2 * kvw), bf16),
                pltpu.VMEM((tps - 1, rows, width), bf16),
                pltpu.VMEM((tps - 1, rows, width), bf16),
                pltpu.VMEM((tps, 8, HD), f32),
                pltpu.VMEM((doms, 8, HD), f32),
                dma((9,)),
                dma((3 * (tps - 1),)), dma((3 * (tps - 1),)),
                dma((doms - 1,)), dma((doms - 1,)),
                dma((16,)), dma((16,)),
                dma((24,)), dma((24,)),
                dma((11,)), dma((11,)),
            ],
            compiler_params=pltpu.CompilerParams(
                collective_id=hot, has_side_effects=True, vmem_limit_bytes=40 << 20
            ),
            name=f"main{hot}",
        )

        def run(
            act, act_part, gain, wq, wk, wv, wo, chip_k, chip_v, twist, tokens, table, prev,
            cosine, sine, tab, ck, cv, counts,
        ):
            attn, new_k, new_v, chosen, out_lw = call(
                act, act_part, gain, wq, wk, wv, wo, chip_k, chip_v, twist, tokens, table,
                prev, cosine, sine, tab, tab,
            )
            return new_k, new_v, attn, chosen, out_lw

        return run

    def every(
        act, act_part, gain, wq, wk, wv, wo, chip_k, chip_v, twist, tokens, table, prev,
        cosine, sine, tab, ck, cv, counts,
    ):
        reward = jnp.sum(table.reshape(-1)[tokens].astype(f32), 0)
        aux = jnp.stack([prev[0] + reward, counts.astype(f32)], 1)
        attn, new_k, new_v, chosen, out_lw = all_rows(
            steps, parts, act, gain, wq, wk, wv, wo, ck, cv, twist, aux, cosine, sine
        )
        return new_k, new_v, attn, chosen, out_lw

    rows_k, rows_v, attn, chosen, out_lw = lax.switch(
        tab[4, 0],
        [hot_branch(hot) for hot in range(4)] + [every],
        activations.reshape(rows, width), act_part, norm_gain.reshape(1, -1), w_query, w_key,
        value_weight, w_output, chip_k, chip_v, twist_vec.reshape(1, -1), tokens,
        twisting_table.reshape(-1, HD), previous_log_weights.reshape(1, parts),
        jnp.asarray(cosine), jnp.asarray(sine), tab, cache_keys, cache_values, copy_counts,
    )
    result = jax.ShapeDtypeStruct((span + steps, parts, kvw), bf16)
    new_k, new_v, attn, out_lw = pl.pallas_call(
        functools.partial(finish_kernel, parts, steps),
        out_shape=(
            result, result, jax.ShapeDtypeStruct((rows, width), bf16),
            jax.ShapeDtypeStruct((1, parts), f32),
        ),
        in_specs=[vmem] * 5,
        out_specs=(hbm, hbm, hbm, vmem),
        scratch_shapes=[
            pltpu.VMEM(result.shape, bf16), pltpu.VMEM(result.shape, bf16), dma((11,)),
        ],
        compiler_params=pltpu.CompilerParams(vmem_limit_bytes=8 << 20),
        name="finish",
    )(rows_k, rows_v, chosen, attn, out_lw)
    return (
        attn.reshape(steps, parts, width), jnp.transpose(new_k, (1, 0, 2)),
        jnp.transpose(new_v, (1, 0, 2)), out_lw.reshape(parts),
    )


def solution(mesh):
    body = adaptive if (mesh.shape["dom"], mesh.shape["tp"]) == (8, 4) else local
    return jax.shard_map(
        body,
        mesh=mesh,
        in_specs=(
            P(None, "dom", "tp"),
            P(),
            P(None, "tp"),
            P(None, "tp"),
            P(None, "tp"),
            P("tp", None),
            P("dom", None, "tp"),
            P("dom", None, "tp"),
            P(None, "dom"),
            P(),
            P("tp"),
            P("dom"),
            P("dom"),
        ),
        out_specs=(P(None, "dom", "tp"), P("dom", None, "tp"), P("dom", None, "tp"), P("dom")),
        check_vma=False,
    )
```
